32 devices in a mesh: shard: 4 (over z), ctx: 2 (over x), tensor: 4 (over y, core).
Axes of the slice: x: 2, y: 2, z: 4, core: 2. Of those that a mesh axis runs over, the one named last changes fastest.
Arguments:
- dec_in: bfloat16 [4, 1024, 768], P('shard', 'ctx'), may hold values from -6 to 6
- memory: bfloat16 [4, 512, 768], P('shard', 'ctx'), may hold values from -6 to 6
- dec_segments: int32 [4, 1024], P('shard'), may hold values from 0 to 7, as said below
- mem_segments: int32 [4, 512], P('shard'), may hold values from 0 to 7, as said below
- gain_self: bfloat16 [768], P('shard'), may hold values from 0.25 to 1.75
- gain_cross: bfloat16 [768], P('shard'), may hold values from 0.25 to 1.75
- gain_ffn: bfloat16 [768], P('shard'), may hold values from 0.25 to 1.75
- self_q: bfloat16 [768, 768], P('shard', 'tensor'), may hold values from -0.0546875 to 0.0546875
- self_k: bfloat16 [768, 768], P('shard', 'tensor'), may hold values from -0.21875 to 0.21875
- self_v: bfloat16 [768, 768], P('shard', 'tensor'), may hold values from -0.21875 to 0.21875
- self_o: bfloat16 [768, 768], P('shard', 'tensor'), may hold values from -0.625 to 0.625
- cross_q: bfloat16 [768, 768], P('shard', 'tensor'), may hold values from -0.0546875 to 0.0546875
- cross_k: bfloat16 [768, 768], P('shard', 'tensor'), may hold values from -0.21875 to 0.21875
- cross_v: bfloat16 [768, 768], P('shard', 'tensor'), may hold values from -0.21875 to 0.21875
- cross_o: bfloat16 [768, 768], P('shard', 'tensor'), may hold values from -0.625 to 0.625
- ffn_gate: bfloat16 [768, 2048], P('shard', 'tensor'), may hold values from -0.21875 to 0.21875
- ffn_up: bfloat16 [768, 2048], P('shard', 'tensor'), may hold values from -0.21875 to 0.21875
- ffn_down: bfloat16 [768, 2048], P('shard', 'tensor'), may hold values from -0.1875 to 0.1875
- bias_table: bfloat16 [32, 12], P('shard', 'tensor'), may hold values from -4 to 4
- cotangent: bfloat16 [4, 1024, 768], P('shard', 'ctx'), may hold values from -6 to 6
Outputs:
- dec_out: bfloat16 [4, 1024, 768], P('shard', 'ctx')
- dec_grad: float32 [4, 1024, 768], P('shard', 'ctx')
- mem_grad: float32 [4, 512, 768], P('shard', 'ctx')
- grad_gain_self: float32 [768], P('shard')
- grad_gain_cross: float32 [768], P('shard')
- grad_gain_ffn: float32 [768], P('shard')
- grad_self_q: float32 [768, 768], P('shard', 'tensor')
- grad_self_k: float32 [768, 768], P('shard', 'tensor')
- grad_self_v: float32 [768, 768], P('shard', 'tensor')
- grad_self_o: float32 [768, 768], P('shard', 'tensor')
- grad_cross_q: float32 [768, 768], P('shard', 'tensor')
- grad_cross_k: float32 [768, 768], P('shard', 'tensor')
- grad_cross_v: float32 [768, 768], P('shard', 'tensor')
- grad_cross_o: float32 [768, 768], P('shard', 'tensor')
- grad_ffn_gate: float32 [768, 2048], P('shard', 'tensor')
- grad_ffn_up: float32 [768, 2048], P('shard', 'tensor')
- grad_ffn_down: float32 [768, 2048], P('shard', 'tensor')
- grad_bias_table: float32 [32, 12], P('shard', 'tensor')
The draws below stay inside these ranges and needn't reach their ends.
Inputs may be any that keep to these rules, and one draw needn't show every extreme that they name: `dec_segments`: in every sequence the ids never fall, start at 0 and end at 7; each of the 8 documents has one position or more. `mem_segments`: likewise for the memory; memory document s belongs to decoder document s of the same sequence.
All inputs are finite; a program needn't handle non-finite values.
Results may differ from the reference program's by a relative error of at most 0.039.
Values may be sent and summed in bfloat16 or wider, within the bound.
A program may use at most 192 MiB of HBM per device.

```python
import jax
import jax.numpy as jnp
import numpy as np
from jax import lax

D = 768
HEADS = 12
HEAD_DIM = 64
FF = 2048
BUCKETS = 32
MAX_DIST = 128
SEGS = 8
SEQUENCES = 4
LENGTH = 1024
MEM_LEN = 512


def document_ids(key, count_rows, length):
    first_key, second_key = jax.random.split(key)
    weights = 4096 // jax.random.randint(first_key, (count_rows, SEGS), 1, 65)
    longest = jax.random.randint(second_key, (count_rows, 1), 0, SEGS)
    chosen = jnp.arange(SEGS, dtype=jnp.int32)[None, :] == longest
    others = jnp.sum(jnp.where(chosen, 0, weights), axis=1, keepdims=True)
    weights = jnp.where(chosen, 2 * others, weights)
    spare = length - SEGS
    sizes = 1 + weights * spare // jnp.sum(weights, axis=1, keepdims=True)
    remainder = length - jnp.sum(sizes, axis=1, keepdims=True)
    sizes = sizes + jnp.where(jnp.arange(SEGS, dtype=jnp.int32)[None, :] == SEGS - 1, remainder, 0)
    bounds = jnp.cumsum(sizes, axis=1)[:, :SEGS - 1]
    places = jnp.arange(length, dtype=jnp.int32)
    return jnp.sum((places[None, :, None] >= bounds[:, None, :]).astype(jnp.int32), axis=2).astype(jnp.int32)


def draw_dec_segments(key, part):
    return document_ids(jax.random.fold_in(key, 11), SEQUENCES, LENGTH)


def draw_mem_segments(key, part):
    return document_ids(jax.random.fold_in(key, 23), SEQUENCES, MEM_LEN)


def level_of(own_key, extent, cuts, smallest, largest):
    def one(axis_at, shards_of):
        draws = jax.random.uniform(jax.random.fold_in(jax.random.fold_in(own_key, 6), axis_at), (shards_of,), jnp.float32, smallest / len(cuts), largest / len(cuts))
        return jnp.repeat(jnp.exp(draws), extent[axis_at] // shards_of).reshape((-1,) + (1,) * (len(extent) - axis_at - 1))

    factor_of = one(*cuts[0])
    for cut in cuts[1:]:
        factor_of = factor_of * one(*cut)
    return factor_of


def centred(stream_key, shape, scale, limit, cuts=(), held_as=jnp.bfloat16):
    level = level_of(stream_key, shape, cuts, -0.22, 0.18) if cuts else 1.0
    array = jax.random.normal(stream_key, shape, jnp.float32) * scale * level
    return jnp.minimum(jnp.maximum(array, -limit), limit).astype(held_as)


def setup_inputs(seed: int = 0) -> dict:
    streams_of = jax.random.split(jax.random.key(seed), 21)
    dec_in = centred(streams_of[0], (SEQUENCES, LENGTH, D), 1.0, 6.0, ((0, 4), (1, 2)))
    memory = centred(streams_of[1], (SEQUENCES, MEM_LEN, D), 1.0, 6.0, ((0, 4), (1, 2)))
    dec_segments = draw_dec_segments(jax.random.fold_in(streams_of[20], 71), 0)
    mem_segments = draw_mem_segments(jax.random.fold_in(streams_of[20], 71), 0)
    gain_self = jnp.clip(1.0 + 0.15 * jax.random.normal(streams_of[4], (D,), jnp.float32), 0.25, 1.75).astype(jnp.bfloat16)
    gain_cross = jnp.clip(1.0 + 0.15 * jax.random.normal(streams_of[5], (D,), jnp.float32), 0.25, 1.75).astype(jnp.bfloat16)
    gain_ffn = jnp.clip(1.0 + 0.15 * jax.random.normal(streams_of[6], (D,), jnp.float32), 0.25, 1.75).astype(jnp.bfloat16)
    self_q = centred(streams_of[7], (D, HEADS * HEAD_DIM), (16 * D) ** -0.5, 0.0546875, ((0, 4), (1, 4)))
    self_k = centred(streams_of[8], (D, HEADS * HEAD_DIM), D ** -0.5, 0.21875, ((0, 4), (1, 4)))
    self_v = centred(streams_of[9], (D, HEADS * HEAD_DIM), D ** -0.5, 0.21875, ((0, 4), (1, 4)))
    self_o = centred(streams_of[10], (D, HEADS * HEAD_DIM), (HEADS * HEAD_DIM // 8) ** -0.5, 0.625, ((0, 4), (1, 4)))
    cross_q = centred(streams_of[11], (D, HEADS * HEAD_DIM), (16 * D) ** -0.5, 0.0546875, ((0, 4), (1, 4)))
    cross_k = centred(streams_of[12], (D, HEADS * HEAD_DIM), D ** -0.5, 0.21875, ((0, 4), (1, 4)))
    cross_v = centred(streams_of[13], (D, HEADS * HEAD_DIM), D ** -0.5, 0.21875, ((0, 4), (1, 4)))
    cross_o = centred(streams_of[14], (D, HEADS * HEAD_DIM), (HEADS * HEAD_DIM // 8) ** -0.5, 0.625, ((0, 4), (1, 4)))
    ffn_gate = centred(streams_of[15], (D, FF), D ** -0.5, 0.21875, ((0, 4), (1, 4)))
    ffn_up = centred(streams_of[16], (D, FF), D ** -0.5, 0.21875, ((0, 4), (1, 4)))
    ffn_down = centred(streams_of[17], (D, FF), (FF // 2) ** -0.5, 0.1875, ((0, 4), (1, 4)))
    bias_table = centred(streams_of[18], (BUCKETS, HEADS), 1.0, 4.0, ((0, 4), (1, 4)))
    cotangent = centred(streams_of[19], (SEQUENCES, LENGTH, D), 1.0, 6.0, ((0, 4), (1, 2)))
    return {"dec_in": dec_in, "memory": memory, "dec_segments": dec_segments, "mem_segments": mem_segments, "gain_self": gain_self, "gain_cross": gain_cross, "gain_ffn": gain_ffn, "self_q": self_q, "self_k": self_k, "self_v": self_v, "self_o": self_o, "cross_q": cross_q, "cross_k": cross_k, "cross_v": cross_v, "cross_o": cross_o, "ffn_gate": ffn_gate, "ffn_up": ffn_up, "ffn_down": ffn_down, "bias_table": bias_table, "cotangent": cotangent}


@jax.custom_vjp
def low(v):
    return lax.optimization_barrier(v.astype(jnp.bfloat16)).astype(jnp.float32)

@jax.custom_vjp
def low_back(v):
    return v

def low_keep(v):
    return (low(v), None)

def low_pass(kept, grad):
    return (grad,)

def back_keep(v):
    return (v, None)

def back_low(kept, grad):
    return (low(grad),)
low.defvjp(low_keep, low_pass)
low_back.defvjp(back_keep, back_low)
highest = lax.Precision.HIGHEST
epsilon = 1e-06
negative = -1e+30

def thresholds():
    exact_part = BUCKETS // 2
    small_part = np.arange(1, exact_part + 1)
    steps_up = np.arange(exact_part + 1, BUCKETS)
    large_part = np.ceil(exact_part * (MAX_DIST / exact_part) ** ((steps_up - exact_part) / (BUCKETS - exact_part)))
    return np.concatenate([small_part, large_part]).astype(np.int32)

def bucket_of(distance):
    limits = jnp.asarray(thresholds())
    return lax.optimization_barrier(jnp.sum((distance[..., None] >= limits).astype(jnp.int32), axis=-1))

def rms_norm(values, gain):
    return values * lax.rsqrt(lax.optimization_barrier(jnp.mean(values * values, axis=-1, keepdims=True)) + epsilon) * gain

def matmul(left, right):
    return jnp.dot(left, right, precision=highest)

def matmul_t(left, right):
    return jnp.dot(left, right.T, precision=highest)

def attention(query, keys, values, query_pos, key_pos, query_seg, key_seg, table, causal):
    length = query.shape[0]
    heads = query.shape[1] // HEAD_DIM
    width = min(512, length)
    count = length // width
    query_blocks = query.reshape(count, width, heads, HEAD_DIM)
    key_heads = keys.reshape(keys.shape[0], heads, HEAD_DIM)
    value_heads = values.reshape(values.shape[0], heads, HEAD_DIM)

    def block(args):
        block_query, block_pos, block_seg = args
        mask = block_seg[:, None] == key_seg[None, :]
        raw = low_back(jnp.einsum('qhd,khd->hqk', block_query, key_heads, precision=highest))
        if causal:
            mask = mask & (block_pos[:, None] >= key_pos[None, :])
            bias = jnp.take(table, bucket_of(block_pos[:, None] - key_pos[None, :]), axis=0)
            raw = raw + jnp.moveaxis(bias, -1, 0)
        scores = jnp.where(mask[None], raw, negative)
        peak = lax.optimization_barrier(jnp.max(scores, axis=-1, keepdims=True))
        expo = jnp.where(mask[None], jnp.exp(scores - peak), 0.0)
        probs = expo / lax.optimization_barrier(jnp.sum(expo, axis=-1, keepdims=True))
        return jnp.einsum('hqk,khd->qhd', low(probs), value_heads, precision=highest)
    outs = lax.map(jax.checkpoint(block), (query_blocks, query_pos.reshape(count, width), query_seg.reshape(count, width)))
    return outs.reshape(length, heads * HEAD_DIM)

def layer(dec_rows, mem_rows, dec_seg, mem_seg, params):
    gain_self, gain_cross, gain_ffn, self_q, self_k, self_v, self_o, cross_q, cross_k, cross_v, cross_o, ffn_gate, ffn_up, ffn_down, bias_table = params
    positions = jnp.arange(dec_rows.shape[0], dtype=jnp.int32)
    mem_pos = jnp.arange(mem_rows.shape[0], dtype=jnp.int32)
    normed = low(rms_norm(dec_rows, gain_self))
    query = low(low_back(matmul(normed, self_q)))
    keys = low(low_back(matmul(normed, self_k)))
    values = low(low_back(matmul(normed, self_v)))
    mixed = attention(query, keys, values, positions, positions, dec_seg, dec_seg, bias_table, True)
    mixed = low(low_back(mixed))
    first = dec_rows + low_back(matmul_t(mixed, self_o))
    normed = low(rms_norm(first, gain_cross))
    query = low(low_back(matmul(normed, cross_q)))
    keys = low(low_back(matmul(mem_rows, cross_k)))
    values = low(low_back(matmul(mem_rows, cross_v)))
    mixed = attention(query, keys, values, positions, mem_pos, dec_seg, mem_seg, bias_table, False)
    mixed = low(low_back(mixed))
    second = first + low_back(matmul_t(mixed, cross_o))
    normed = low(rms_norm(second, gain_ffn))
    gate = low_back(matmul(normed, ffn_gate))
    upper = low_back(matmul(normed, ffn_up))
    hidden = low(jax.nn.gelu(gate, approximate=True) * upper)
    return second + low_back(matmul_t(hidden, ffn_down))

def reference(dec_in, memory, dec_segments, mem_segments, gain_self, gain_cross, gain_ffn, self_q, self_k, self_v, self_o, cross_q, cross_k, cross_v, cross_o, ffn_gate, ffn_up, ffn_down, bias_table, cotangent):
    params = tuple((weight.astype(jnp.float32) for weight in (gain_self, gain_cross, gain_ffn, self_q, self_k, self_v, self_o, cross_q, cross_k, cross_v, cross_o, ffn_gate, ffn_up, ffn_down, bias_table)))

    def one_sequence(totals, item):
        dec_rows, mem_rows, dec_seg, mem_seg, grad_rows = item

        def run(rows_in, mem_in, weights):
            return layer(rows_in, mem_in, dec_seg, mem_seg, weights)
        result, pull = jax.vjp(run, dec_rows.astype(jnp.float32), mem_rows.astype(jnp.float32), params)
        grad_dec, grad_mem, grad_params = pull(grad_rows.astype(jnp.float32))
        totals = tuple((total + part for total, part in zip(totals, grad_params)))
        return (totals, (result.astype(jnp.bfloat16), grad_dec, grad_mem))
    start = tuple((jnp.zeros_like(weight) for weight in params))
    totals, (outputs, grad_decs, grad_mems) = lax.scan(one_sequence, start, (dec_in, memory, dec_segments, mem_segments, cotangent))
    return (outputs, grad_decs, grad_mems, totals[0], totals[1], totals[2], totals[3], totals[4], totals[5], totals[6], totals[7], totals[8], totals[9], totals[10], totals[11], totals[12], totals[13], totals[14])
```

```python
import functools

import jax
import jax.numpy as jnp
import numpy as np
from jax import lax
from jax.experimental import pallas as pl
from jax.experimental.pallas import tpu as pltpu
from jax.sharding import PartitionSpec as P

HEAD_DIM = 64
BUCKETS = 32
MAX_DIST = 128


highest = lax.Precision.HIGHEST
epsilon = 1e-06
negative = -1e30


def thresholds():
    exact_part = BUCKETS // 2
    small_part = np.arange(1, exact_part + 1)
    steps_up = np.arange(exact_part + 1, BUCKETS)
    large_part = np.ceil(
        exact_part * (MAX_DIST / exact_part) ** ((steps_up - exact_part) / (BUCKETS - exact_part))
    )
    return np.concatenate([small_part, large_part]).astype(np.int32)


def bucket_of(distance):
    limits = jnp.asarray(thresholds())
    return jnp.sum((distance[..., None] >= limits).astype(jnp.int32), axis=-1)


def rms_norm(values, gain):
    return values * lax.rsqrt(jnp.mean(values * values, axis=-1, keepdims=True) + epsilon) * gain


def gated(gate, upper):
    return jax.nn.gelu(gate, approximate=True) * upper


def forward_mm(left, right):
    return jnp.dot(left, right, preferred_element_type=jnp.float32)


def backward_mm(left, right):
    return lax.dot_general(
        left, right, (((1,), (1,)), ((), ())), preferred_element_type=jnp.float32
    )


def weight_mm(left, right):
    return lax.dot_general(
        left, right, (((0,), (0,)), ((), ())), preferred_element_type=jnp.float32
    )


def toeplitz(vector, count_rows, count_cols):
    heads = vector.shape[0]
    span = count_rows + count_cols - 1
    tiled = jnp.pad(jnp.tile(vector, (1, count_rows)), ((0, 0), (0, count_rows)))
    grid = tiled.reshape(heads, count_rows, span + 1)[:, :, :count_cols]
    return grid[:, :, ::-1]


def diagonal_sums(block):
    heads, count_rows, count_cols = block.shape
    span = count_rows + count_cols - 1
    flipped = jnp.pad(block[:, :, ::-1], ((0, 0), (0, 0), (0, count_rows)))
    flat = flipped.reshape(heads, count_rows * (span + 1))[:, : count_rows * span]
    return jnp.sum(flat.reshape(heads, count_rows, span), axis=1)


def bias_block(table, offset, count_rows, count_cols):
    span = count_rows + count_cols - 1
    distance = jnp.arange(span, dtype=jnp.int32) - (count_cols - 1) + offset
    onehot = (
        bucket_of(distance)[:, None] == jnp.arange(table.shape[0], dtype=jnp.int32)[None, :]
    ).astype(jnp.float32)
    column = jnp.dot(onehot, table, precision=highest)
    return (toeplitz(column.T, count_rows, count_cols), onehot)


def key_blocks(pairs, key_pos, key_seg):
    length = pairs.shape[0]
    width = min(512, length)
    count = length // width
    heads = pairs.shape[1] // (2 * HEAD_DIM)
    blocks = pairs.reshape(count, width, 2, heads, HEAD_DIM)
    starts = jnp.arange(count, dtype=jnp.int32) * width
    return (blocks, key_pos.reshape(count, width), key_seg.reshape(count, width), starts)


def scores_of(query, block, block_pos, block_seg, start, query_pos, query_seg, table, causal):
    scores = jnp.einsum("qhd,khd->hqk", query, block[:, 0], preferred_element_type=jnp.float32)
    mask = query_seg[:, None] == block_seg[None, :]
    onehot = None
    if causal:
        mask = mask & (query_pos[:, None] >= block_pos[None, :])
        bias, onehot = bias_block(table, query_pos[0] - start, query.shape[0], block.shape[0])
        scores = scores + bias
    return (jnp.where(mask[None], scores, negative), mask, onehot)


def attend(query, pairs, key_pos, key_seg, query_pos, query_seg, table, causal):
    count_rows = query.shape[0]
    heads = query.shape[1] // HEAD_DIM
    query = query.reshape(count_rows, heads, HEAD_DIM)
    blocks = key_blocks(pairs, key_pos, key_seg)

    def stats(carry, item):
        peak, total = carry
        block, block_pos, block_seg, start = item
        scores, mask, _ = scores_of(
            query, block, block_pos, block_seg, start, query_pos, query_seg, table, causal
        )
        fresh = jnp.maximum(peak, jnp.max(scores, axis=-1))
        weights = jnp.where(mask[None], jnp.exp(scores - fresh[..., None]), 0.0)
        total = total * jnp.exp(peak - fresh) + jnp.sum(weights, axis=-1)
        return ((fresh, total), None)

    start_peak = jnp.full((heads, count_rows), negative, jnp.float32)
    start_total = jnp.zeros((heads, count_rows), jnp.float32)
    (peak, total), _ = lax.scan(stats, (start_peak, start_total), blocks)
    log_total = peak + jnp.log(total)

    def collect(accum, item):
        block, block_pos, block_seg, start = item
        scores, mask, _ = scores_of(
            query, block, block_pos, block_seg, start, query_pos, query_seg, table, causal
        )
        probs = jnp.where(mask[None], jnp.exp(scores - log_total[..., None]), 0.0).astype(
            jnp.bfloat16
        )
        accum = accum + jnp.einsum(
            "hqk,khd->qhd", probs, block[:, 1], preferred_element_type=jnp.float32
        )
        return (accum, None)

    mixed, _ = lax.scan(collect, jnp.zeros((count_rows, heads, HEAD_DIM), jnp.float32), blocks)
    return (mixed.reshape(count_rows, heads * HEAD_DIM), log_total)


def correction_of(grad_mixed, mixed):
    count_rows = mixed.shape[0]
    heads = mixed.shape[1] // HEAD_DIM
    return jnp.einsum(
        "qhd,qhd->hq",
        grad_mixed.reshape(count_rows, heads, HEAD_DIM).astype(jnp.float32),
        mixed.reshape(count_rows, heads, HEAD_DIM),
    )


def attend_back(
    query,
    pairs,
    key_pos,
    key_seg,
    query_pos,
    query_seg,
    table,
    causal,
    mixed,
    log_total,
    grad_mixed,
):
    count_rows = query.shape[0]
    heads = query.shape[1] // HEAD_DIM
    query = query.reshape(count_rows, heads, HEAD_DIM)
    grad_heads = grad_mixed.reshape(count_rows, heads, HEAD_DIM)
    correction = correction_of(grad_mixed, mixed)
    blocks = key_blocks(pairs, key_pos, key_seg)

    def step(carry, item):
        grad_query, grad_table = carry
        block, block_pos, block_seg, start = item
        scores, mask, onehot = scores_of(
            query, block, block_pos, block_seg, start, query_pos, query_seg, table, causal
        )
        probs = jnp.where(mask[None], jnp.exp(scores - log_total[..., None]), 0.0)
        grad_probs = jnp.einsum(
            "qhd,khd->hqk", grad_heads, block[:, 1], preferred_element_type=jnp.float32
        )
        grad_scores = probs * (grad_probs - correction[..., None])
        if causal:
            grad_table = grad_table + jnp.dot(
                onehot.T, diagonal_sums(grad_scores).T, precision=highest
            )
        low_scores = grad_scores.astype(jnp.bfloat16)
        grad_query = grad_query + jnp.einsum(
            "hqk,khd->qhd", low_scores, block[:, 0], preferred_element_type=jnp.float32
        )
        stacked = None
        grad_values = jnp.einsum(
            "hqk,qhd->khd",
            probs.astype(jnp.bfloat16),
            grad_heads,
            preferred_element_type=jnp.float32,
        )
        grad_keys = jnp.einsum(
            "hqk,qhd->khd", low_scores, query, preferred_element_type=jnp.float32
        )
        width = block.shape[0]
        stacked = jnp.concatenate(
            [
                grad_keys.reshape(width, heads * HEAD_DIM),
                grad_values.reshape(width, heads * HEAD_DIM),
            ],
            axis=1,
        )
        return ((grad_query, grad_table), stacked)

    start = (
        jnp.zeros((count_rows, heads, HEAD_DIM), jnp.float32),
        jnp.zeros(table.shape, jnp.float32),
    )
    (grad_query, grad_table), grad_pairs = lax.scan(step, start, blocks)
    grad_pairs = grad_pairs.reshape(pairs.shape[0], pairs.shape[1])
    return (grad_query.reshape(count_rows, heads * HEAD_DIM), grad_pairs, grad_table)


BLOCK = 128


def nt(left, right):
    return lax.dot_general(
        left, right, (((1,), (1,)), ((), ())), preferred_element_type=jnp.float32
    )


def tn(left, right):
    return lax.dot_general(
        left, right, (((0,), (0,)), ((), ())), preferred_element_type=jnp.float32
    )


def lane_buckets():
    lane = np.arange(BLOCK)
    distance = (BLOCK - lane) % BLOCK
    bucket = (distance[:, None] >= thresholds()[None, :]).sum(axis=1)
    return (bucket[None, :] == np.arange(BUCKETS)[:, None]).astype(np.float32)


def build_strip(near_ref, far_ref, strip_ref, tiles, heads):
    row = lax.broadcasted_iota(jnp.int32, (BLOCK, BLOCK), 0)
    col = lax.broadcasted_iota(jnp.int32, (BLOCK, BLOCK), 1)
    for h in range(heads):
        near = jnp.broadcast_to(near_ref[h : h + 1, :], (BLOCK, BLOCK))
        near = pltpu.roll(near, 0, 1, stride=1, stride_axis=0)
        far = jnp.broadcast_to(far_ref[h : h + 1, :], (BLOCK, BLOCK))
        for m in range(tiles - 2):
            strip_ref[h, :, m * BLOCK : (m + 1) * BLOCK] = far
        strip_ref[h, :, (tiles - 2) * BLOCK : (tiles - 1) * BLOCK] = jnp.where(
            row < col, near, far
        )
        strip_ref[h, :, (tiles - 1) * BLOCK : tiles * BLOCK] = near
        strip_ref[h, :, tiles * BLOCK :] = jnp.zeros((BLOCK, (tiles - 1) * BLOCK), jnp.float32)


def fold_diagonals(tile):
    rows = BLOCK
    while rows > 8:
        rows //= 2
        tile = tile[:rows] + pltpu.roll(tile[rows:], BLOCK - rows, 1)
    total = tile[0:1]
    for r in range(1, 8):
        total = total + pltpu.roll(tile[r : r + 1], BLOCK - r, 1)
    return total


def fwd_kernel(
    causal, heads, q_ref, kv_ref, rows_ref, cols_ref, near_ref, far_ref, a_ref, p_ref, strip_ref
):
    count, keys = q_ref.shape[0], kv_ref.shape[0]
    width = heads * HEAD_DIM
    tiles = keys // BLOCK
    place = lax.axis_index("ctx")
    if causal:
        build_strip(near_ref, far_ref, strip_ref, tiles, heads)

    def body(i, carry):
        base = pl.multiple_of(i * BLOCK, BLOCK)
        here = pl.ds(base, BLOCK)
        mask = rows_ref[here, :] == cols_ref[...]
        if causal:
            first = place * count + base
            row = lax.broadcasted_iota(jnp.int32, (BLOCK, keys), 0) + first
            col = lax.broadcasted_iota(jnp.int32, (BLOCK, keys), 1)
            mask = mask & (row >= col)
            start = pl.multiple_of((tiles - 1) * BLOCK - first, BLOCK)
        outs = []
        for h in range(heads):
            lanes = slice(h * HEAD_DIM, (h + 1) * HEAD_DIM)
            scores = nt(q_ref[here, lanes], kv_ref[:, lanes])
            if causal:
                scores = scores + strip_ref[h, :, pl.ds(start, keys)]
            scores = jnp.where(mask, scores, negative)
            peak = jnp.max(scores, axis=1, keepdims=True)
            weights = jnp.exp(scores - peak)
            probs = weights / jnp.sum(weights, axis=1, keepdims=True)
            p_ref[h, here, :] = probs
            outs.append(
                forward_mm(
                    probs.astype(jnp.bfloat16),
                    kv_ref[:, width + h * HEAD_DIM : width + (h + 1) * HEAD_DIM],
                )
            )
        a_ref[here, :] = jnp.concatenate(outs, axis=1).astype(jnp.bfloat16)
        return carry

    lax.fori_loop(0, count // BLOCK, body, 0)


def bwd_kernel(
    causal, heads, q_ref, kv_ref, p_ref, ga_ref, gq_ref, gkv_ref, dnear_ref, dfar_ref,
    ds_ref, pb_ref, dstrip_ref,
):
    count, keys = q_ref.shape[0], kv_ref.shape[0]
    width = heads * HEAD_DIM
    tiles = keys // BLOCK
    place = lax.axis_index("ctx")
    if causal:
        dstrip_ref[...] = jnp.zeros_like(dstrip_ref)

    def body(i, carry):
        base = pl.multiple_of(i * BLOCK, BLOCK)
        here = pl.ds(base, BLOCK)
        start = pl.multiple_of((tiles - 1) * BLOCK - place * count - base, BLOCK)
        outs = []
        for h in range(heads):
            lanes = slice(h * HEAD_DIM, (h + 1) * HEAD_DIM)
            probs = p_ref[h, here, :]
            grad_probs = nt(
                ga_ref[here, lanes],
                kv_ref[:, width + h * HEAD_DIM : width + (h + 1) * HEAD_DIM],
            )
            mean = jnp.sum(probs * grad_probs, axis=1, keepdims=True)
            grad_scores = probs * (grad_probs - mean)
            if causal:
                window = pl.ds(start, keys)
                dstrip_ref[h, :, window] = dstrip_ref[h, :, window] + grad_scores
            low = grad_scores.astype(jnp.bfloat16)
            ds_ref[h, here, :] = low
            pb_ref[h, here, :] = probs.astype(jnp.bfloat16)
            outs.append(forward_mm(low, kv_ref[:, lanes]))
        gq_ref[here, :] = jnp.concatenate(outs, axis=1).astype(jnp.bfloat16)
        return carry

    lax.fori_loop(0, count // BLOCK, body, 0)
    keys_t, values_t = [], []
    for h in range(heads):
        lanes = slice(h * HEAD_DIM, (h + 1) * HEAD_DIM)
        keys_t.append(tn(q_ref[:, lanes], ds_ref[h]))
        values_t.append(tn(ga_ref[:, lanes], pb_ref[h]))
    both = jnp.concatenate(keys_t + values_t, axis=0)
    gkv_ref[...] = both.T.astype(jnp.bfloat16)
    dnear_ref[...] = jnp.zeros_like(dnear_ref)
    dfar_ref[...] = jnp.zeros_like(dfar_ref)
    if causal:
        row = lax.broadcasted_iota(jnp.int32, (BLOCK, BLOCK), 0)
        col = lax.broadcasted_iota(jnp.int32, (BLOCK, BLOCK), 1)
        for h in range(heads):
            own = dstrip_ref[h, :, (tiles - 1) * BLOCK : tiles * BLOCK]
            last = dstrip_ref[h, :, (tiles - 2) * BLOCK : (tiles - 1) * BLOCK]
            dnear_ref[h : h + 1, :] = fold_diagonals(own + jnp.where(row < col, last, 0.0))
            far = jnp.where(row < col, 0.0, last)
            for m in range(tiles - 2):
                far = far + dstrip_ref[h, :, m * BLOCK : (m + 1) * BLOCK]
            dfar_ref[h : h + 1, :] = jnp.sum(far, axis=0, keepdims=True)


def attend_fast(query, pairs, row_ids, col_ids, near, far, causal):
    count, width = query.shape
    heads, keys = width // HEAD_DIM, pairs.shape[0]
    strip = (2 * (keys // BLOCK) - 1) * BLOCK if causal else BLOCK
    return pl.pallas_call(
        functools.partial(fwd_kernel, causal, heads),
        out_shape=(
            jax.ShapeDtypeStruct((count, width), jnp.bfloat16),
            jax.ShapeDtypeStruct((heads, count, keys), jnp.float32),
        ),
        scratch_shapes=[pltpu.VMEM((heads, BLOCK, strip), jnp.float32)],
        compiler_params=pltpu.CompilerParams(vmem_limit_bytes=48 * 1024 * 1024),
        name="attend_causal" if causal else "attend_cross",
    )(query, pairs, row_ids[:, None], col_ids[None, :], near, far)


def attend_back_fast(query, pairs, probs, grad_mixed, causal):
    count, width = query.shape
    heads, keys = width // HEAD_DIM, pairs.shape[0]
    strip = (2 * (keys // BLOCK) - 1) * BLOCK if causal else BLOCK
    return pl.pallas_call(
        functools.partial(bwd_kernel, causal, heads),
        out_shape=(
            jax.ShapeDtypeStruct((count, width), jnp.bfloat16),
            jax.ShapeDtypeStruct((keys, 2 * width), jnp.bfloat16),
            jax.ShapeDtypeStruct((8, BLOCK), jnp.float32),
            jax.ShapeDtypeStruct((8, BLOCK), jnp.float32),
        ),
        scratch_shapes=[
            pltpu.VMEM((heads, count, keys), jnp.bfloat16),
            pltpu.VMEM((heads, count, keys), jnp.bfloat16),
            pltpu.VMEM((heads, BLOCK, strip), jnp.float32),
        ],
        compiler_params=pltpu.CompilerParams(vmem_limit_bytes=56 * 1024 * 1024),
        name="attend_back_causal" if causal else "attend_back_cross",
    )(query, pairs, probs, grad_mixed)


def gather_rows(arrays):
    widths = [a.shape[1] for a in arrays]
    full = lax.all_gather(jnp.concatenate(arrays, axis=1), "shard", axis=0, tiled=True)
    return jnp.split(full, list(np.cumsum(widths)[:-1]), axis=1)


def local_fast(
    dec_in, memory, dec_segments, mem_segments, gain_self, gain_cross, gain_ffn,
    self_q, self_k, self_v, self_o, cross_q, cross_k, cross_v, cross_o,
    ffn_gate, ffn_up, ffn_down, bias_table, cotangent,
):
    shards = lax.axis_size("shard")
    part, buckets_part, heads = gain_self.shape[0], bias_table.shape[0], bias_table.shape[1]
    small = jnp.concatenate([gain_self, gain_cross, gain_ffn, bias_table.reshape(-1)])
    small = lax.all_gather(small, "shard", axis=0, tiled=False)
    gain_one = small[:, :part].reshape(-1).astype(jnp.float32)
    gain_two = small[:, part : 2 * part].reshape(-1).astype(jnp.float32)
    gain_three = small[:, 2 * part : 3 * part].reshape(-1).astype(jnp.float32)
    table = small[:, 3 * part :].reshape(shards * buckets_part, heads).astype(jnp.float32)
    query_self, key_self, value_self, out_self = gather_rows([self_q, self_k, self_v, self_o])
    query_cross, key_cross, value_cross, out_cross = gather_rows(
        [cross_q, cross_k, cross_v, cross_o]
    )
    gate_full, up_full, down_full = gather_rows([ffn_gate, ffn_up, ffn_down])
    lanes = jnp.asarray(lane_buckets())
    near = jnp.zeros((8, BLOCK), jnp.float32).at[:heads].set(
        jnp.dot(table.T, lanes, precision=highest)
    )
    far = jnp.zeros((8, BLOCK), jnp.float32).at[:heads].set(
        jnp.broadcast_to(table[-1][:, None], (heads, BLOCK))
    )
    width = query_self.shape[1]
    hidden_in = dec_in[0].astype(jnp.float32)
    mem_rows = memory[0]
    grad_out = cotangent[0].astype(jnp.float32)
    count_rows = hidden_in.shape[0]
    place = lax.axis_index("ctx")
    dec_ids = dec_segments[0]
    mem_ids = mem_segments[0]
    query_ids = lax.dynamic_slice_in_dim(dec_ids, place * count_rows, count_rows)
    normed_one = rms_norm(hidden_in, gain_one).astype(jnp.bfloat16)
    query_one = forward_mm(normed_one, query_self).astype(jnp.bfloat16)
    pairs_own = jnp.concatenate(
        [forward_mm(normed_one, key_self), forward_mm(normed_one, value_self)], axis=1
    ).astype(jnp.bfloat16)
    pairs_one = lax.all_gather(pairs_own, "ctx", axis=0, tiled=True)
    context_one, probs_one = attend_fast(
        query_one, pairs_one, query_ids, dec_ids, near, far, True
    )
    first = hidden_in + lax.psum(
        backward_mm(context_one, out_self).astype(jnp.bfloat16), "tensor"
    ).astype(jnp.float32)
    normed_two = rms_norm(first, gain_two).astype(jnp.bfloat16)
    query_two = forward_mm(normed_two, query_cross).astype(jnp.bfloat16)
    pairs_mem = jnp.concatenate(
        [forward_mm(mem_rows, key_cross), forward_mm(mem_rows, value_cross)], axis=1
    ).astype(jnp.bfloat16)
    pairs_two = lax.all_gather(pairs_mem, "ctx", axis=0, tiled=True)
    context_two, probs_two = attend_fast(
        query_two, pairs_two, query_ids, mem_ids, near, far, False
    )
    second = first + lax.psum(
        backward_mm(context_two, out_cross).astype(jnp.bfloat16), "tensor"
    ).astype(jnp.float32)
    normed_three = rms_norm(second, gain_three).astype(jnp.bfloat16)
    gate = forward_mm(normed_three, gate_full)
    upper = forward_mm(normed_three, up_full)
    activated = gated(gate, upper).astype(jnp.bfloat16)
    result = second + lax.psum(
        backward_mm(activated, down_full).astype(jnp.bfloat16), "tensor"
    ).astype(jnp.float32)
    dec_out = result.astype(jnp.bfloat16)
    grad_low = cotangent[0]
    grad_down_w = weight_mm(grad_low, activated)
    grad_hidden = forward_mm(grad_low, down_full)
    _, pull_gate = jax.vjp(gated, gate, upper)
    grad_gate, grad_upper = pull_gate(grad_hidden)
    gate_low = grad_gate.astype(jnp.bfloat16)
    upper_low = grad_upper.astype(jnp.bfloat16)
    grad_gate_w = weight_mm(normed_three, gate_low)
    grad_up_w = weight_mm(normed_three, upper_low)
    grad_normed_three = backward_mm(gate_low, gate_full) + backward_mm(upper_low, up_full)
    grad_normed_three = lax.psum(grad_normed_three.astype(jnp.bfloat16), "tensor").astype(
        jnp.float32
    )
    _, pull_three = jax.vjp(rms_norm, second, gain_three)
    grad_second, grad_gain_three = pull_three(grad_normed_three)
    grad_second = grad_out + grad_second
    second_low = grad_second.astype(jnp.bfloat16)
    grad_out_cross = weight_mm(second_low, context_two)
    grad_context_two = forward_mm(second_low, out_cross).astype(jnp.bfloat16)
    query_two_low, grad_pairs_two, _, _ = attend_back_fast(
        query_two, pairs_two, probs_two, grad_context_two, False
    )
    pairs_grad_mem = lax.psum_scatter(grad_pairs_two, "ctx", scatter_dimension=0, tiled=True)
    grad_mem_keys = pairs_grad_mem[:, :width]
    grad_mem_values = pairs_grad_mem[:, width:]
    grad_query_cross = weight_mm(normed_two, query_two_low)
    grad_key_cross = weight_mm(mem_rows, grad_mem_keys)
    grad_value_cross = weight_mm(mem_rows, grad_mem_values)
    grad_normed_two = backward_mm(query_two_low, query_cross)
    grad_memory = backward_mm(grad_mem_keys, key_cross) + backward_mm(grad_mem_values, value_cross)
    grad_normed_two, grad_memory = (
        lax.psum(grad_normed_two.astype(jnp.bfloat16), "tensor").astype(jnp.float32),
        lax.psum(grad_memory.astype(jnp.bfloat16), "tensor").astype(jnp.float32),
    )
    _, pull_two = jax.vjp(rms_norm, first, gain_two)
    grad_first, grad_gain_two = pull_two(grad_normed_two)
    grad_first = grad_second + grad_first
    first_low = grad_first.astype(jnp.bfloat16)
    grad_out_self = weight_mm(first_low, context_one)
    grad_context_one = forward_mm(first_low, out_self).astype(jnp.bfloat16)
    query_one_low, grad_pairs_one, dnear, dfar = attend_back_fast(
        query_one, pairs_one, probs_one, grad_context_one, True
    )
    grad_table = jnp.dot(lanes, dnear[:heads].T, precision=highest)
    grad_table = grad_table.at[-1].add(jnp.sum(dfar[:heads], axis=1))
    pairs_grad_own = lax.psum_scatter(grad_pairs_one, "ctx", scatter_dimension=0, tiled=True)
    grad_keys_own = pairs_grad_own[:, :width]
    grad_values_own = pairs_grad_own[:, width:]
    grad_query_self = weight_mm(normed_one, query_one_low)
    grad_key_self = weight_mm(normed_one, grad_keys_own)
    grad_value_self = weight_mm(normed_one, grad_values_own)
    grad_normed_one = (
        backward_mm(query_one_low, query_self)
        + backward_mm(grad_keys_own, key_self)
        + backward_mm(grad_values_own, value_self)
    )
    grad_normed_one = lax.psum(grad_normed_one.astype(jnp.bfloat16), "tensor").astype(jnp.float32)
    _, pull_one = jax.vjp(rms_norm, hidden_in, gain_one)
    grad_input, grad_gain_one = pull_one(grad_normed_one)
    grad_input = grad_first + grad_input

    def scattered(grads):
        widths = [g.shape[1] for g in grads]
        joined = jnp.concatenate([g.astype(jnp.bfloat16) for g in grads], axis=1)
        own = lax.psum_scatter(joined, "shard", scatter_dimension=0, tiled=True)
        own = lax.psum(own, "ctx").astype(jnp.float32)
        return jnp.split(own, list(np.cumsum(widths)[:-1]), axis=1)

    ffn_grads = scattered([grad_gate_w, grad_up_w, grad_down_w])
    cross_grads = scattered([grad_query_cross, grad_key_cross, grad_value_cross, grad_out_cross])
    self_grads = scattered([grad_query_self, grad_key_self, grad_value_self, grad_out_self])
    tiny = jnp.concatenate(
        [
            grad_gain_one.reshape(shards, -1),
            grad_gain_two.reshape(shards, -1),
            grad_gain_three.reshape(shards, -1),
            grad_table.reshape(shards, -1),
        ],
        axis=1,
    )
    tiny = lax.psum(tiny, ("shard", "ctx"))
    tiny = lax.dynamic_index_in_dim(tiny, lax.axis_index("shard"), 0, keepdims=False)
    return (
        dec_out[None],
        grad_input[None],
        grad_memory[None],
        tiny[:part],
        tiny[part : 2 * part],
        tiny[2 * part : 3 * part],
        *self_grads,
        *cross_grads,
        *ffn_grads,
        tiny[3 * part :].reshape(buckets_part, heads),
    )


def shard_part(parts):
    return (
        lax.psum_scatter(
            parts[0].astype(jnp.bfloat16), "shard", scatter_dimension=0, tiled=True
        ).astype(jnp.float32),
        lax.psum_scatter(
            parts[1].astype(jnp.bfloat16), "shard", scatter_dimension=0, tiled=True
        ).astype(jnp.float32),
        lax.psum_scatter(
            parts[2].astype(jnp.bfloat16), "shard", scatter_dimension=0, tiled=True
        ).astype(jnp.float32),
        lax.psum_scatter(
            parts[3].astype(jnp.bfloat16), "shard", scatter_dimension=0, tiled=True
        ).astype(jnp.float32),
        lax.psum_scatter(
            parts[4].astype(jnp.bfloat16), "shard", scatter_dimension=0, tiled=True
        ).astype(jnp.float32),
        lax.psum_scatter(
            parts[5].astype(jnp.bfloat16), "shard", scatter_dimension=0, tiled=True
        ).astype(jnp.float32),
        lax.psum_scatter(
            parts[6].astype(jnp.bfloat16), "shard", scatter_dimension=0, tiled=True
        ).astype(jnp.float32),
        lax.psum_scatter(
            parts[7].astype(jnp.bfloat16), "shard", scatter_dimension=0, tiled=True
        ).astype(jnp.float32),
        lax.psum_scatter(
            parts[8].astype(jnp.bfloat16), "shard", scatter_dimension=0, tiled=True
        ).astype(jnp.float32),
        lax.psum_scatter(
            parts[9].astype(jnp.bfloat16), "shard", scatter_dimension=0, tiled=True
        ).astype(jnp.float32),
        lax.psum_scatter(
            parts[10].astype(jnp.bfloat16), "shard", scatter_dimension=0, tiled=True
        ).astype(jnp.float32),
        lax.psum_scatter(
            parts[11].astype(jnp.bfloat16), "shard", scatter_dimension=0, tiled=True
        ).astype(jnp.float32),
        lax.psum_scatter(
            parts[12].astype(jnp.bfloat16), "shard", scatter_dimension=0, tiled=True
        ).astype(jnp.float32),
        lax.psum_scatter(
            parts[13].astype(jnp.bfloat16), "shard", scatter_dimension=0, tiled=True
        ).astype(jnp.float32),
        lax.psum_scatter(
            parts[14].astype(jnp.bfloat16), "shard", scatter_dimension=0, tiled=True
        ).astype(jnp.float32),
    )


def context_total(parts):
    return (
        lax.psum(parts[0].astype(jnp.bfloat16), "ctx").astype(jnp.float32),
        lax.psum(parts[1].astype(jnp.bfloat16), "ctx").astype(jnp.float32),
        lax.psum(parts[2].astype(jnp.bfloat16), "ctx").astype(jnp.float32),
        lax.psum(parts[3].astype(jnp.bfloat16), "ctx").astype(jnp.float32),
        lax.psum(parts[4].astype(jnp.bfloat16), "ctx").astype(jnp.float32),
        lax.psum(parts[5].astype(jnp.bfloat16), "ctx").astype(jnp.float32),
        lax.psum(parts[6].astype(jnp.bfloat16), "ctx").astype(jnp.float32),
        lax.psum(parts[7].astype(jnp.bfloat16), "ctx").astype(jnp.float32),
        lax.psum(parts[8].astype(jnp.bfloat16), "ctx").astype(jnp.float32),
        lax.psum(parts[9].astype(jnp.bfloat16), "ctx").astype(jnp.float32),
        lax.psum(parts[10].astype(jnp.bfloat16), "ctx").astype(jnp.float32),
        lax.psum(parts[11].astype(jnp.bfloat16), "ctx").astype(jnp.float32),
        lax.psum(parts[12].astype(jnp.bfloat16), "ctx").astype(jnp.float32),
        lax.psum(parts[13].astype(jnp.bfloat16), "ctx").astype(jnp.float32),
        lax.psum(parts[14].astype(jnp.bfloat16), "ctx").astype(jnp.float32),
    )


def local(
    dec_in,
    memory,
    dec_segments,
    mem_segments,
    gain_self,
    gain_cross,
    gain_ffn,
    self_q,
    self_k,
    self_v,
    self_o,
    cross_q,
    cross_k,
    cross_v,
    cross_o,
    ffn_gate,
    ffn_up,
    ffn_down,
    bias_table,
    cotangent,
):
    gathered = (
        lax.all_gather(gain_self, "shard", axis=0, tiled=True),
        lax.all_gather(gain_cross, "shard", axis=0, tiled=True),
        lax.all_gather(gain_ffn, "shard", axis=0, tiled=True),
        lax.all_gather(self_q, "shard", axis=0, tiled=True),
        lax.all_gather(self_k, "shard", axis=0, tiled=True),
        lax.all_gather(self_v, "shard", axis=0, tiled=True),
        lax.all_gather(self_o, "shard", axis=0, tiled=True),
        lax.all_gather(cross_q, "shard", axis=0, tiled=True),
        lax.all_gather(cross_k, "shard", axis=0, tiled=True),
        lax.all_gather(cross_v, "shard", axis=0, tiled=True),
        lax.all_gather(cross_o, "shard", axis=0, tiled=True),
        lax.all_gather(ffn_gate, "shard", axis=0, tiled=True),
        lax.all_gather(ffn_up, "shard", axis=0, tiled=True),
        lax.all_gather(ffn_down, "shard", axis=0, tiled=True),
        lax.all_gather(bias_table, "shard", axis=0, tiled=True),
    )
    (
        norm_one,
        norm_two,
        norm_three,
        query_self,
        key_self,
        value_self,
        out_self,
        query_cross,
        key_cross,
        value_cross,
        out_cross,
        gate_full,
        up_full,
        down_full,
        table_full,
    ) = gathered
    gain_one = norm_one.astype(jnp.float32)
    gain_two = norm_two.astype(jnp.float32)
    gain_three = norm_three.astype(jnp.float32)
    table = table_full.astype(jnp.float32)
    width = query_self.shape[1]
    hidden_in = dec_in[0].astype(jnp.float32)
    mem_rows = memory[0]
    grad_out = cotangent[0].astype(jnp.float32)
    count_rows = hidden_in.shape[0]
    place = lax.axis_index("ctx")
    dec_ids = dec_segments[0]
    mem_ids = mem_segments[0]
    query_ids = lax.dynamic_slice_in_dim(dec_ids, place * count_rows, count_rows)
    query_pos = place * count_rows + jnp.arange(count_rows, dtype=jnp.int32)
    key_pos = jnp.arange(dec_ids.shape[0], dtype=jnp.int32)
    mem_pos = jnp.arange(mem_ids.shape[0], dtype=jnp.int32)
    normed_one = rms_norm(hidden_in, gain_one).astype(jnp.bfloat16)
    query_one = forward_mm(normed_one, query_self).astype(jnp.bfloat16)
    pairs_own = jnp.concatenate(
        [forward_mm(normed_one, key_self), forward_mm(normed_one, value_self)], axis=1
    ).astype(jnp.bfloat16)
    pairs_one = lax.all_gather(pairs_own, "ctx", axis=0, tiled=True)
    mixed_one, lse_one = attend(
        query_one, pairs_one, key_pos, dec_ids, query_pos, query_ids, table, True
    )
    context_one = mixed_one.astype(jnp.bfloat16)
    first = hidden_in + lax.psum(
        backward_mm(context_one, out_self).astype(jnp.bfloat16), "tensor"
    ).astype(jnp.float32)
    normed_two = rms_norm(first, gain_two).astype(jnp.bfloat16)
    query_two = forward_mm(normed_two, query_cross).astype(jnp.bfloat16)
    pairs_mem = jnp.concatenate(
        [forward_mm(mem_rows, key_cross), forward_mm(mem_rows, value_cross)], axis=1
    ).astype(jnp.bfloat16)
    pairs_two = lax.all_gather(pairs_mem, "ctx", axis=0, tiled=True)
    mixed_two, lse_two = attend(
        query_two, pairs_two, mem_pos, mem_ids, query_pos, query_ids, table, False
    )
    context_two = mixed_two.astype(jnp.bfloat16)
    second = first + lax.psum(
        backward_mm(context_two, out_cross).astype(jnp.bfloat16), "tensor"
    ).astype(jnp.float32)
    normed_three = rms_norm(second, gain_three).astype(jnp.bfloat16)
    gate = forward_mm(normed_three, gate_full)
    upper = forward_mm(normed_three, up_full)
    activated = gated(gate, upper).astype(jnp.bfloat16)
    result = second + lax.psum(
        backward_mm(activated, down_full).astype(jnp.bfloat16), "tensor"
    ).astype(jnp.float32)
    dec_out = result.astype(jnp.bfloat16)
    grad_low = cotangent[0]
    grad_down_w = weight_mm(grad_low, activated)
    grad_hidden = forward_mm(grad_low, down_full)
    _, pull_gate = jax.vjp(gated, gate, upper)
    grad_gate, grad_upper = pull_gate(grad_hidden)
    gate_low = grad_gate.astype(jnp.bfloat16)
    upper_low = grad_upper.astype(jnp.bfloat16)
    grad_gate_w = weight_mm(normed_three, gate_low)
    grad_up_w = weight_mm(normed_three, upper_low)
    grad_normed_three = backward_mm(gate_low, gate_full) + backward_mm(upper_low, up_full)
    grad_normed_three = lax.psum(grad_normed_three.astype(jnp.bfloat16), "tensor").astype(
        jnp.float32
    )
    _, pull_three = jax.vjp(rms_norm, second, gain_three)
    grad_second, grad_gain_three = pull_three(grad_normed_three)
    grad_second = grad_out + grad_second
    second_low = grad_second.astype(jnp.bfloat16)
    grad_out_cross = weight_mm(second_low, context_two)
    grad_context_two = forward_mm(second_low, out_cross).astype(jnp.bfloat16)
    grad_query_two, grad_pairs_two, _ = attend_back(
        query_two,
        pairs_two,
        mem_pos,
        mem_ids,
        query_pos,
        query_ids,
        table,
        False,
        mixed_two,
        lse_two,
        grad_context_two,
    )
    pairs_grad_mem = lax.psum_scatter(
        grad_pairs_two.astype(jnp.bfloat16), "ctx", scatter_dimension=0, tiled=True
    )
    query_two_low = grad_query_two.astype(jnp.bfloat16)
    grad_mem_keys = pairs_grad_mem[:, :width]
    grad_mem_values = pairs_grad_mem[:, width:]
    grad_query_cross = weight_mm(normed_two, query_two_low)
    grad_key_cross = weight_mm(mem_rows, grad_mem_keys)
    grad_value_cross = weight_mm(mem_rows, grad_mem_values)
    grad_normed_two = backward_mm(query_two_low, query_cross)
    grad_memory = backward_mm(grad_mem_keys, key_cross) + backward_mm(grad_mem_values, value_cross)
    grad_normed_two, grad_memory = (
        lax.psum(grad_normed_two.astype(jnp.bfloat16), "tensor").astype(jnp.float32),
        lax.psum(grad_memory.astype(jnp.bfloat16), "tensor").astype(jnp.float32),
    )
    _, pull_two = jax.vjp(rms_norm, first, gain_two)
    grad_first, grad_gain_two = pull_two(grad_normed_two)
    grad_first = grad_second + grad_first
    first_low = grad_first.astype(jnp.bfloat16)
    grad_out_self = weight_mm(first_low, context_one)
    grad_context_one = forward_mm(first_low, out_self).astype(jnp.bfloat16)
    grad_query_one, grad_pairs_one, grad_table = attend_back(
        query_one,
        pairs_one,
        key_pos,
        dec_ids,
        query_pos,
        query_ids,
        table,
        True,
        mixed_one,
        lse_one,
        grad_context_one,
    )
    pairs_grad_own = lax.psum_scatter(
        grad_pairs_one.astype(jnp.bfloat16), "ctx", scatter_dimension=0, tiled=True
    )
    query_one_low = grad_query_one.astype(jnp.bfloat16)
    grad_keys_own = pairs_grad_own[:, :width]
    grad_values_own = pairs_grad_own[:, width:]
    grad_query_self = weight_mm(normed_one, query_one_low)
    grad_key_self = weight_mm(normed_one, grad_keys_own)
    grad_value_self = weight_mm(normed_one, grad_values_own)
    grad_normed_one = (
        backward_mm(query_one_low, query_self)
        + backward_mm(grad_keys_own, key_self)
        + backward_mm(grad_values_own, value_self)
    )
    grad_normed_one = lax.psum(grad_normed_one.astype(jnp.bfloat16), "tensor").astype(jnp.float32)
    _, pull_one = jax.vjp(rms_norm, hidden_in, gain_one)
    grad_input, grad_gain_one = pull_one(grad_normed_one)
    grad_input = grad_first + grad_input
    local_grads = (
        grad_gain_one,
        grad_gain_two,
        grad_gain_three,
        grad_query_self,
        grad_key_self,
        grad_value_self,
        grad_out_self,
        grad_query_cross,
        grad_key_cross,
        grad_value_cross,
        grad_out_cross,
        grad_gate_w,
        grad_up_w,
        grad_down_w,
        grad_table,
    )
    summed = shard_part(context_total(local_grads))
    return (
        dec_out[None],
        grad_input[None],
        grad_memory[None],
        summed[0],
        summed[1],
        summed[2],
        summed[3],
        summed[4],
        summed[5],
        summed[6],
        summed[7],
        summed[8],
        summed[9],
        summed[10],
        summed[11],
        summed[12],
        summed[13],
        summed[14],
    )


def solution(mesh):
    in_specs = (
        P("shard", "ctx", None),
        P("shard", "ctx", None),
        P("shard", None),
        P("shard", None),
        P("shard"),
        P("shard"),
        P("shard"),
        P("shard", "tensor"),
        P("shard", "tensor"),
        P("shard", "tensor"),
        P("shard", "tensor"),
        P("shard", "tensor"),
        P("shard", "tensor"),
        P("shard", "tensor"),
        P("shard", "tensor"),
        P("shard", "tensor"),
        P("shard", "tensor"),
        P("shard", "tensor"),
        P("shard", "tensor"),
        P("shard", "ctx", None),
    )
    out_specs = (
        P("shard", "ctx", None),
        P("shard", "ctx", None),
        P("shard", "ctx", None),
        P("shard"),
        P("shard"),
        P("shard"),
        P("shard", "tensor"),
        P("shard", "tensor"),
        P("shard", "tensor"),
        P("shard", "tensor"),
        P("shard", "tensor"),
        P("shard", "tensor"),
        P("shard", "tensor"),
        P("shard", "tensor"),
        P("shard", "tensor"),
        P("shard", "tensor"),
        P("shard", "tensor"),
        P("shard", "tensor"),
    )
    fast = mesh.shape["ctx"] == 2
    body = local_fast if fast else local
    return jax.shard_map(body, mesh=mesh, in_specs=in_specs, out_specs=out_specs, check_vma=False)
```

```python
import functools
import types

import jax
import jax.numpy as jnp
import numpy as np
from jax import lax
from jax.experimental import pallas as pl
from jax.experimental.pallas import tpu as pltpu
from jax.sharding import PartitionSpec as P

SHARD, CTX, TENSOR = "shard", "ctx", "tensor"
HEAD_DIM = 64
BUCKETS = 32
MAX_DIST = 128


highest = lax.Precision.HIGHEST
epsilon = 1e-06
negative = -1e30


def thresholds():
    exact_part = BUCKETS // 2
    small_part = np.arange(1, exact_part + 1)
    steps_up = np.arange(exact_part + 1, BUCKETS)
    large_part = np.ceil(
        exact_part * (MAX_DIST / exact_part) ** ((steps_up - exact_part) / (BUCKETS - exact_part))
    )
    return np.concatenate([small_part, large_part]).astype(np.int32)


def bucket_of(distance):
    limits = jnp.asarray(thresholds())
    return jnp.sum((distance[..., None] >= limits).astype(jnp.int32), axis=-1)


def rms_norm(values, gain):
    return values * lax.rsqrt(jnp.mean(values * values, axis=-1, keepdims=True) + epsilon) * gain


def gated(gate, upper):
    return jax.nn.gelu(gate, approximate=True) * upper


def forward_mm(left, right):
    return jnp.dot(left, right, preferred_element_type=jnp.float32)


def backward_mm(left, right):
    return lax.dot_general(
        left, right, (((1,), (1,)), ((), ())), preferred_element_type=jnp.float32
    )


def weight_mm(left, right):
    return lax.dot_general(
        left, right, (((0,), (0,)), ((), ())), preferred_element_type=jnp.float32
    )


def toeplitz(vector, count_rows, count_cols):
    heads = vector.shape[0]
    span = count_rows + count_cols - 1
    tiled = jnp.pad(jnp.tile(vector, (1, count_rows)), ((0, 0), (0, count_rows)))
    grid = tiled.reshape(heads, count_rows, span + 1)[:, :, :count_cols]
    return grid[:, :, ::-1]


def diagonal_sums(block):
    heads, count_rows, count_cols = block.shape
    span = count_rows + count_cols - 1
    flipped = jnp.pad(block[:, :, ::-1], ((0, 0), (0, 0), (0, count_rows)))
    flat = flipped.reshape(heads, count_rows * (span + 1))[:, : count_rows * span]
    return jnp.sum(flat.reshape(heads, count_rows, span), axis=1)


def bias_block(table, offset, count_rows, count_cols):
    span = count_rows + count_cols - 1
    distance = jnp.arange(span, dtype=jnp.int32) - (count_cols - 1) + offset
    onehot = (
        bucket_of(distance)[:, None] == jnp.arange(table.shape[0], dtype=jnp.int32)[None, :]
    ).astype(jnp.float32)
    column = jnp.dot(onehot, table, precision=highest)
    return (toeplitz(column.T, count_rows, count_cols), onehot)


def key_blocks(pairs, key_pos, key_seg):
    length = pairs.shape[0]
    width = min(512, length)
    count = length // width
    heads = pairs.shape[1] // (2 * HEAD_DIM)
    blocks = pairs.reshape(count, width, 2, heads, HEAD_DIM)
    starts = jnp.arange(count, dtype=jnp.int32) * width
    return (blocks, key_pos.reshape(count, width), key_seg.reshape(count, width), starts)


def scores_of(query, block, block_pos, block_seg, start, query_pos, query_seg, table, causal):
    scores = jnp.einsum("qhd,khd->hqk", query, block[:, 0], preferred_element_type=jnp.float32)
    mask = query_seg[:, None] == block_seg[None, :]
    onehot = None
    if causal:
        mask = mask & (query_pos[:, None] >= block_pos[None, :])
        bias, onehot = bias_block(table, query_pos[0] - start, query.shape[0], block.shape[0])
        scores = scores + bias
    return (jnp.where(mask[None], scores, negative), mask, onehot)


def attend(query, pairs, key_pos, key_seg, query_pos, query_seg, table, causal):
    count_rows = query.shape[0]
    heads = query.shape[1] // HEAD_DIM
    query = query.reshape(count_rows, heads, HEAD_DIM)
    blocks = key_blocks(pairs, key_pos, key_seg)

    def stats(carry, item):
        peak, total = carry
        block, block_pos, block_seg, start = item
        scores, mask, _ = scores_of(
            query, block, block_pos, block_seg, start, query_pos, query_seg, table, causal
        )
        fresh = jnp.maximum(peak, jnp.max(scores, axis=-1))
        weights = jnp.where(mask[None], jnp.exp(scores - fresh[..., None]), 0.0)
        total = total * jnp.exp(peak - fresh) + jnp.sum(weights, axis=-1)
        return ((fresh, total), None)

    start_peak = jnp.full((heads, count_rows), negative, jnp.float32)
    start_total = jnp.zeros((heads, count_rows), jnp.float32)
    (peak, total), _ = lax.scan(stats, (start_peak, start_total), blocks)
    log_total = peak + jnp.log(total)

    def collect(accum, item):
        block, block_pos, block_seg, start = item
        scores, mask, _ = scores_of(
            query, block, block_pos, block_seg, start, query_pos, query_seg, table, causal
        )
        probs = jnp.where(mask[None], jnp.exp(scores - log_total[..., None]), 0.0).astype(
            jnp.bfloat16
        )
        accum = accum + jnp.einsum(
            "hqk,khd->qhd", probs, block[:, 1], preferred_element_type=jnp.float32
        )
        return (accum, None)

    mixed, _ = lax.scan(collect, jnp.zeros((count_rows, heads, HEAD_DIM), jnp.float32), blocks)
    return (mixed.reshape(count_rows, heads * HEAD_DIM), log_total)


def correction_of(grad_mixed, mixed):
    count_rows = mixed.shape[0]
    heads = mixed.shape[1] // HEAD_DIM
    return jnp.einsum(
        "qhd,qhd->hq",
        grad_mixed.reshape(count_rows, heads, HEAD_DIM).astype(jnp.float32),
        mixed.reshape(count_rows, heads, HEAD_DIM),
    )


def attend_back(
    query,
    pairs,
    key_pos,
    key_seg,
    query_pos,
    query_seg,
    table,
    causal,
    mixed,
    log_total,
    grad_mixed,
):
    count_rows = query.shape[0]
    heads = query.shape[1] // HEAD_DIM
    query = query.reshape(count_rows, heads, HEAD_DIM)
    grad_heads = grad_mixed.reshape(count_rows, heads, HEAD_DIM)
    correction = correction_of(grad_mixed, mixed)
    blocks = key_blocks(pairs, key_pos, key_seg)

    def step(carry, item):
        grad_query, grad_table = carry
        block, block_pos, block_seg, start = item
        scores, mask, onehot = scores_of(
            query, block, block_pos, block_seg, start, query_pos, query_seg, table, causal
        )
        probs = jnp.where(mask[None], jnp.exp(scores - log_total[..., None]), 0.0)
        grad_probs = jnp.einsum(
            "qhd,khd->hqk", grad_heads, block[:, 1], preferred_element_type=jnp.float32
        )
        grad_scores = probs * (grad_probs - correction[..., None])
        if causal:
            grad_table = grad_table + jnp.dot(
                onehot.T, diagonal_sums(grad_scores).T, precision=highest
            )
        low_scores = grad_scores.astype(jnp.bfloat16)
        grad_query = grad_query + jnp.einsum(
            "hqk,khd->qhd", low_scores, block[:, 0], preferred_element_type=jnp.float32
        )
        stacked = None
        grad_values = jnp.einsum(
            "hqk,qhd->khd",
            probs.astype(jnp.bfloat16),
            grad_heads,
            preferred_element_type=jnp.float32,
        )
        grad_keys = jnp.einsum(
            "hqk,qhd->khd", low_scores, query, preferred_element_type=jnp.float32
        )
        width = block.shape[0]
        stacked = jnp.concatenate(
            [
                grad_keys.reshape(width, heads * HEAD_DIM),
                grad_values.reshape(width, heads * HEAD_DIM),
            ],
            axis=1,
        )
        return ((grad_query, grad_table), stacked)

    start = (
        jnp.zeros((count_rows, heads, HEAD_DIM), jnp.float32),
        jnp.zeros(table.shape, jnp.float32),
    )
    (grad_query, grad_table), grad_pairs = lax.scan(step, start, blocks)
    grad_pairs = grad_pairs.reshape(pairs.shape[0], pairs.shape[1])
    return (grad_query.reshape(count_rows, heads * HEAD_DIM), grad_pairs, grad_table)


BLOCK = 128


def nt(left, right):
    return lax.dot_general(
        left, right, (((1,), (1,)), ((), ())), preferred_element_type=jnp.float32
    )


def tn(left, right):
    return lax.dot_general(
        left, right, (((0,), (0,)), ((), ())), preferred_element_type=jnp.float32
    )


def lane_buckets():
    lane = np.arange(BLOCK)
    distance = (BLOCK - lane) % BLOCK
    bucket = (distance[:, None] >= thresholds()[None, :]).sum(axis=1)
    return (bucket[None, :] == np.arange(BUCKETS)[:, None]).astype(np.float32)


def build_strip(near_ref, far_ref, strip_ref, tiles, heads):
    row = lax.broadcasted_iota(jnp.int32, (BLOCK, BLOCK), 0)
    col = lax.broadcasted_iota(jnp.int32, (BLOCK, BLOCK), 1)
    for h in range(heads):
        near = jnp.broadcast_to(near_ref[h : h + 1, :], (BLOCK, BLOCK))
        near = pltpu.roll(near, 0, 1, stride=1, stride_axis=0)
        far = jnp.broadcast_to(far_ref[h : h + 1, :], (BLOCK, BLOCK))
        for m in range(tiles - 2):
            strip_ref[h, :, m * BLOCK : (m + 1) * BLOCK] = far
        strip_ref[h, :, (tiles - 2) * BLOCK : (tiles - 1) * BLOCK] = jnp.where(
            row < col, near, far
        )
        strip_ref[h, :, (tiles - 1) * BLOCK : tiles * BLOCK] = near
        strip_ref[h, :, tiles * BLOCK :] = jnp.zeros((BLOCK, (tiles - 1) * BLOCK), jnp.float32)


def fold_diagonals(tile):
    rows = BLOCK
    while rows > 8:
        rows //= 2
        tile = tile[:rows] + pltpu.roll(tile[rows:], BLOCK - rows, 1)
    total = tile[0:1]
    for r in range(1, 8):
        total = total + pltpu.roll(tile[r : r + 1], BLOCK - r, 1)
    return total


SELF_Q, SELF_K, SELF_V, SELF_O, CROSS_Q, CROSS_K, CROSS_V, CROSS_O, GATE, UP, DOWN = range(11)
GROUPS = (
    (DOWN,), (GATE,), (UP,), (CROSS_O, CROSS_Q), (CROSS_K, CROSS_V),
    (SELF_O, SELF_Q), (SELF_K, SELF_V),
)
CHUNK = 128
BIG = 256
SHARDS = 4
MESH = pl.DeviceIdType.MESH
bf16 = jnp.bfloat16
f32 = jnp.float32


def loop_rows(count, block, step):
    def body(i, carry):
        step(pl.multiple_of(i * block, block))
        return carry

    lax.fori_loop(0, count // block, body, 0)


def layer_kernel(shape, trees, *refs):
    found, at = {}, 0
    for tree in trees:
        found.update(tree.unflatten(refs[at : at + tree.num_leaves]))
        at += tree.num_leaves
    r = types.SimpleNamespace(**found)
    rows, mem_count, dim, width, heads = shape
    keys = 2 * rows
    mem_keys = 2 * mem_count
    half = dim // SHARDS // 2
    z = lax.axis_index(SHARD)
    x = lax.axis_index(CTX)
    t = lax.axis_index(TENSOR)
    core = lax.rem(t, 2)
    to_x = {CTX: 1 - x}
    to_core = {TENSOR: t + 1 - 2 * core}
    to_y = {TENSOR: lax.rem(t + 2, 4)}

    def to_z(k):
        return {SHARD: lax.rem(z + k, SHARDS)}

    send_sem, recv_sem = r.send_sem, r.recv_sem
    used = [0]
    unsent = []

    def copy(src, dst, where):
        i = used[0]
        used[0] += 1
        return pltpu.make_async_remote_copy(
            src_ref=src, dst_ref=dst, send_sem=send_sem.at[i], recv_sem=recv_sem.at[i],
            device_id=where, device_id_type=MESH,
        )

    def start(src, dst, where):
        c = copy(src, dst, where)
        c.start()
        unsent.append(c)
        return c

    barrier = pltpu.get_barrier_semaphore()
    partners = [to_z(1), to_z(2), to_z(3), to_x, to_core, to_y]
    for p in partners:
        pl.semaphore_signal(barrier, inc=1, device_id=p, device_id_type=MESH)
    pl.semaphore_wait(barrier, len(partners))

    def own_copies(name, index):
        full, part = r.full[name], r.part[name]
        local = []
        for side in range(2):
            c = pltpu.make_async_copy(
                part.at[pl.ds(side * half, half), :], full.at[z, side],
                r.own_sem.at[2 * index + side],
            )
            c.start()
            local.append(c)
        return local

    gathers = {}

    def gather_start(name, index):
        full, part = r.full[name], r.part[name]
        own = own_copies(name, index)
        sent = [
            start(part.at[pl.ds(x * half, half), :], full.at[z, x], to_z(k)) for k in (1, 2, 3)
        ]
        gathers[name] = (own, sent, [])

    def gather_pump(name):
        own, sent, passed = gathers[name]
        full = r.full[name]
        for k in (1, 2, 3):
            sent[k - 1].wait_recv()
            source = lax.rem(z + SHARDS - k, SHARDS)
            passed.append(start(full.at[source, x], full.at[source, x], to_x))

    def gather_wait(name):
        own, sent, passed = gathers[name]
        for c in own:
            c.wait()
        for c in passed:
            c.wait_recv()

    def weight(name):
        ref = r.full[name]
        return ref[...].reshape(dim, ref.shape[-1])

    small_own = pltpu.make_async_copy(r.in_small, r.small.at[z], r.own_sem.at[22])
    small_own.start()
    small_sent = [start(r.in_small, r.small.at[z], to_z(k)) for k in (1, 2, 3)]
    for i, name in enumerate(range(3)):
        gather_start(name, i)

    seg = r.in_seg[...].astype(f32)
    r.seg[...] = seg
    r.mseg[...] = r.in_mseg[...].astype(f32)
    own_seg = r.seg[:, pl.ds(pl.multiple_of(x * rows, BLOCK), rows)]
    r.seg_col[...] = jnp.broadcast_to(own_seg, (8, rows)).T

    for name in range(3):
        gather_pump(name)
    for i, name in enumerate(range(3, 8)):
        gather_start(name, 3 + i)

    small_own.wait()
    for c in small_sent:
        c.wait_recv()
    gathered = [r.small[s].astype(f32) for s in range(SHARDS)]
    for k in range(3):
        r.gains[k : k + 1, :] = jnp.concatenate(
            [g[k : k + 1, : dim // SHARDS] for g in gathered], axis=1
        )
    table = jnp.concatenate([g[8:16, :BLOCK] for g in gathered], axis=0)
    near = tn(table.astype(bf16), r.in_lanes[...].astype(bf16))
    r.near[...] = near[:8]
    lane_of = lax.broadcasted_iota(jnp.int32, (8, BLOCK), 1)
    row_of = lax.broadcasted_iota(jnp.int32, (8, BLOCK), 0)
    last = jnp.broadcast_to(table[BUCKETS - 1 : BUCKETS, :], (8, BLOCK))
    last = jnp.sum(jnp.where(lane_of == row_of, last, 0.0), axis=1, keepdims=True)
    r.far[...] = jnp.broadcast_to(last, (8, BLOCK))
    build_strip(r.near, r.far, r.strip, keys // BLOCK, heads)

    def inverse(v):
        return lax.rsqrt(jnp.mean(v * v, axis=1, keepdims=True) + epsilon)

    def norm(v, k):
        return (v * inverse(v) * r.gains[k : k + 1, :]).astype(bf16)

    for name in range(3):
        gather_wait(name)

    def project(base):
        here = pl.ds(base, BIG)
        h = norm(r.in_dec[here, :].astype(f32), 0)
        r.h1[here, :] = h
        r.q1[here, :] = forward_mm(h, weight(SELF_Q)).astype(bf16)
        r.kv1[x, here, :] = jnp.concatenate(
            [forward_mm(h, weight(SELF_K)), forward_mm(h, weight(SELF_V))], axis=1
        ).astype(bf16)

    loop_rows(rows, BIG, project)
    kv1_sent = start(r.kv1.at[x], r.kv1.at[x], to_x)
    for name in range(3, 8):
        gather_pump(name)
    for i, name in ((10, DOWN), (8, GATE), (9, UP)):
        gather_start(name, i)
    kv1_sent.wait_recv()

    def attend_rows(causal, q, kv, cols, p_ref, a_ref, total):
        tiles = total // BLOCK

        def step(base):
            here = pl.ds(base, BLOCK)
            mask = r.seg_col[here, 0:1] == cols[...]
            if causal:
                first = x * rows + base
                row = lax.broadcasted_iota(jnp.int32, (BLOCK, total), 0) + first
                col = lax.broadcasted_iota(jnp.int32, (BLOCK, total), 1)
                mask = mask & (row >= col)
                begin = pl.multiple_of((tiles - 1) * BLOCK - first, BLOCK)
            outs = []
            for h in range(heads):
                lanes = slice(h * HEAD_DIM, (h + 1) * HEAD_DIM)
                tail = slice(width + h * HEAD_DIM, width + (h + 1) * HEAD_DIM)
                scores = nt(q[here, lanes], kv[:, :, lanes].reshape(total, HEAD_DIM))
                if causal:
                    scores = scores + r.strip[h, :, pl.ds(begin, total)]
                scores = jnp.where(mask, scores, negative)
                peak = jnp.max(scores, axis=1, keepdims=True)
                weights = jnp.exp(scores - peak)
                probs = (weights / jnp.sum(weights, axis=1, keepdims=True)).astype(bf16)
                p_ref[h, here, :] = probs
                outs.append(forward_mm(probs, kv[:, :, tail].reshape(total, HEAD_DIM)))
            a_ref[here, :] = jnp.concatenate(outs, axis=1).astype(bf16)

        loop_rows(rows, BLOCK, step)

    sums = {}

    def flush(key):
        for c in sums[key]["sends"]:
            c.wait_send()
            unsent[:] = [u for u in unsent if u is not c]
        sums[key]["sends"] = []

    def sum_begin(key, piece, chunks):
        if key in sums:
            flush(key)
        out, into = r.ps_out[key], r.ps_in[key]
        y_out, y_in, acc = r.py_out[key], r.py_in[key], r.p_acc[key]
        state = {"sends": [], "y": [], "chunks": chunks}
        sums[key] = state
        arriving = []

        def go(src, dst, where):
            c = start(src, dst, where)
            state["sends"].append(c)
            return c

        for j in range(chunks):
            base = pl.multiple_of(((1 - core) * chunks + j) * CHUNK, CHUNK)
            out[j] = piece(base).astype(bf16)
            arriving.append(go(out.at[j], into.at[j], to_core))
        for j in range(chunks):
            acc[j] = piece(pl.multiple_of((core * chunks + j) * CHUNK, CHUNK))
        for j in range(chunks):
            arriving[j].wait_recv()
            y_out[j] = (acc[j] + into[j].astype(f32)).astype(bf16)
            state["y"].append(go(y_out.at[j], y_in.at[j], to_y))

    def sum_finish(key):
        state = sums[key]
        y_out, y_in, res = r.py_out[key], r.py_in[key], r.p_res[key]
        last = []
        for j in range(state["chunks"]):
            state["y"][j].wait_recv()
            res[core, j] = (y_out[j].astype(f32) + y_in[j].astype(f32)).astype(bf16)
            c = start(res.at[core, j], res.at[core, j], to_core)
            state["sends"].append(c)
            last.append(c)
        for c in last:
            c.wait_recv()

    def summed(key, base, count):
        res = r.p_res[key]
        return res[base // (res.shape[1] * CHUNK)].reshape(count, dim).astype(f32)

    wide = rows // 2 // CHUNK
    slim = mem_count // 2 // CHUNK
    attend_rows(True, r.q1, r.kv1, r.seg, r.p1, r.a1, keys)
    gather_wait(SELF_O)
    sum_begin(0, lambda base: nt(r.a1[pl.ds(base, CHUNK), :], weight(SELF_O)), wide)

    for name in (DOWN, GATE, UP):
        gather_pump(name)
    for name in range(4, 8):
        gather_wait(name)
    memory = r.in_mem[...]
    r.kv2[x] = jnp.concatenate(
        [forward_mm(memory, weight(CROSS_K)), forward_mm(memory, weight(CROSS_V))], axis=1
    ).astype(bf16)
    kv2_sent = start(r.kv2.at[x], r.kv2.at[x], to_x)
    sum_finish(0)

    def second_block(base):
        here = pl.ds(base, BIG)
        v = r.in_dec[here, :].astype(f32) + summed(0, base, BIG)
        r.x1[here, :] = v
        h = norm(v, 1)
        r.h2[here, :] = h
        r.q2[here, :] = forward_mm(h, weight(CROSS_Q)).astype(bf16)

    loop_rows(rows, BIG, second_block)
    kv2_sent.wait_recv()
    attend_rows(False, r.q2, r.kv2, r.mseg, r.p2, r.a2, mem_keys)
    sum_begin(1, lambda base: nt(r.a2[pl.ds(base, CHUNK), :], weight(CROSS_O)), wide)
    for name in (DOWN, GATE, UP):
        gather_wait(name)

    def grad_hidden_block(base):
        here = pl.ds(base, BIG)
        r.gm[here, :] = forward_mm(r.in_cot[here, :], weight(DOWN))

    loop_rows(rows, BIG, grad_hidden_block)

    def flip(src, dst, count):
        for j in range(dim // BLOCK):
            dst[j * BLOCK : (j + 1) * BLOCK, :count] = src[:, j * BLOCK : (j + 1) * BLOCK].T

    flip(r.in_cot, r.flip, rows)
    sum_finish(1)

    def ffn_block(base):
        here = pl.ds(base, BIG)
        v = r.x1[here, :] + summed(1, base, BIG)
        r.x2[here, :] = v
        h = norm(v, 2)
        r.h3[here, :] = h
        gate = forward_mm(h, weight(GATE))
        upper = forward_mm(h, weight(UP))
        scale = np.float32(np.sqrt(2.0 / np.pi))
        square = gate * gate
        curve = jnp.tanh(scale * (gate + 0.044715 * (square * gate)))
        lower = 0.5 * (1.0 + curve)
        gelu = gate * lower
        slope = lower + 0.5 * gate * (1.0 - curve * curve) * scale * (1.0 + 3 * 0.044715 * square)
        grad = r.gm[here, :]
        r.m[here, :] = (gelu * upper).astype(bf16)
        r.ggate[here, :] = (grad * upper * slope).astype(bf16)
        r.gup[here, :] = (grad * gelu).astype(bf16)

    loop_rows(rows, BIG, ffn_block)
    sum_begin(
        0,
        lambda base: nt(r.ggate[pl.ds(base, CHUNK), :], weight(GATE))
        + nt(r.gup[pl.ds(base, CHUNK), :], weight(UP)),
        wide,
    )

    shard_rows = dim // SHARDS

    def grad_into(g, at, flipped, right, count):
        stage = r.stage[g]
        cols = right.shape[1]

        def step(d, carry):
            here = pl.ds(pl.multiple_of(d * shard_rows, shard_rows), shard_rows)
            value = forward_mm(flipped[here, :count], right[...]).astype(bf16)
            stage[d, :, :, at : at + cols] = value.reshape(2, half, cols)
            return carry

        lax.fori_loop(0, SHARDS, step, 0)

    reduces = {}

    def reduce_x(g):
        stage = r.stage[g]
        reduces[g] = [start(stage.at[:, 1 - x], r.xr[g], to_x)]

    def reduce_z(g):
        stage, xr, zr = r.stage[g], r.xr[g], r.zr[g]
        reduces[g][0].wait_recv()

        def step(d, carry):
            stage[d, x] = (stage[d, x].astype(f32) + xr[d].astype(f32)).astype(bf16)
            return carry

        lax.fori_loop(0, SHARDS, step, 0)
        for k in (1, 2, 3):
            d = lax.rem(z + k, SHARDS)
            reduces[g].append(start(stage.at[d, x], zr.at[k - 1], to_z(k)))

    def reduce_f(g):
        stage, zr, both = r.stage[g], r.zr[g], r.fb[g]
        total = stage[z, x].astype(f32)
        for k in (1, 2, 3):
            reduces[g][k].wait_recv()
            total = total + zr[k - 1].astype(f32)
        both[x] = total.astype(bf16)
        reduces[g].append(start(both.at[x], both.at[x], to_x))

    def reduce_o(g):
        reduces[g][4].wait_recv()
        both = r.fb[g]
        at = 0
        for name in GROUPS[g]:
            out = r.out_grad[name]
            cols = out.shape[1]
            out[...] = both[:, :, at : at + cols].reshape(shard_rows, cols).astype(f32)
            at += cols

    grad_into(0, 0, r.flip, r.m, rows)
    reduce_x(0)
    flip(r.h3, r.flip, rows)
    grad_into(1, 0, r.flip, r.ggate, rows)
    reduce_x(1)
    grad_into(2, 0, r.flip, r.gup, rows)
    reduce_x(2)

    def norm_back(v, grad, k):
        inv = inverse(v)
        unit = v * inv
        scaled = grad * r.gains[k : k + 1, :]
        mean = jnp.mean(scaled * unit, axis=1, keepdims=True)
        return inv * (scaled - unit * mean), jnp.sum(grad * unit, axis=0, keepdims=True)

    r.tiny[...] = jnp.zeros_like(r.tiny)
    sum_finish(0)

    def second_grad(base):
        here = pl.ds(base, BIG)
        back, gain = norm_back(r.x2[here, :], summed(0, base, BIG), 2)
        grad = r.in_cot[here, :].astype(f32) + back
        r.tiny[2:3, :] = r.tiny[2:3, :] + gain
        r.gx[here, :] = grad
        low = grad.astype(bf16)
        r.gxb[here, :] = low
        r.ga[here, :] = forward_mm(low, weight(CROSS_O)).astype(bf16)

    loop_rows(rows, BIG, second_grad)
    sum_begin(1, lambda base: nt(r.m[pl.ds(base, CHUNK), :], weight(DOWN)), wide)
    reduce_z(0)

    def attend_back_rows(causal, q, kv, p_ref, gq, gkv, total):
        tiles = total // BLOCK
        strip = r.strip
        if causal:
            strip[...] = jnp.zeros_like(strip)
        for h in range(heads):
            lanes = slice(h * HEAD_DIM, (h + 1) * HEAD_DIM)
            tail = slice(width + h * HEAD_DIM, width + (h + 1) * HEAD_DIM)

            def step(base):
                here = pl.ds(base, BLOCK)
                probs = p_ref[h, here, :].astype(f32)
                grad_probs = nt(r.ga[here, lanes], kv[:, :, tail].reshape(total, HEAD_DIM))
                mean = jnp.sum(probs * grad_probs, axis=1, keepdims=True)
                scores = probs * (grad_probs - mean)
                if causal:
                    begin = pl.multiple_of((tiles - 1) * BLOCK - x * rows - base, BLOCK)
                    window = pl.ds(begin, total)
                    strip[h, :, window] = strip[h, :, window] + scores
                low = scores.astype(bf16)
                r.ds[here, :total] = low
                gq[here, lanes] = forward_mm(low, kv[:, :, lanes].reshape(total, HEAD_DIM)).astype(
                    bf16
                )

            loop_rows(rows, BLOCK, step)
            r.gkv_t[lanes, :total] = tn(q[:, lanes], r.ds[:, :total])
            r.gkv_t[tail, :total] = tn(r.ga[:, lanes], p_ref[h])
        part = total // 2
        for side in range(2):
            gkv[side] = r.gkv_t[:, side * part : (side + 1) * part].T.astype(bf16)

    attend_back_rows(False, r.q2, r.kv2, r.p2, r.gq2, r.gkv2, mem_keys)
    gkv2_sent = start(r.gkv2.at[1 - x], r.gkv2_in, to_x)
    sum_finish(1)

    def output_block(base):
        here = pl.ds(base, BIG)
        r.out_dec[here, :] = (r.x2[here, :] + summed(1, base, BIG)).astype(bf16)

    loop_rows(rows, BIG, output_block)
    sum_begin(0, lambda base: nt(r.gq2[pl.ds(base, CHUNK), :], weight(CROSS_Q)), wide)
    reduce_z(1)
    reduce_z(2)
    flip(r.gxb, r.flip, rows)
    grad_into(3, 0, r.flip, r.a2, rows)
    flip(r.h2, r.flip, rows)
    grad_into(3, width, r.flip, r.gq2, rows)
    reduce_x(3)
    gkv2_sent.wait_recv()
    r.gkv2_sum[...] = (r.gkv2[x].astype(f32) + r.gkv2_in[...].astype(f32)).astype(bf16)
    sum_begin(
        2,
        lambda base: nt(r.gkv2_sum[pl.ds(base, CHUNK), :width], weight(CROSS_K))
        + nt(r.gkv2_sum[pl.ds(base, CHUNK), width:], weight(CROSS_V)),
        slim,
    )
    flip(r.in_mem, r.flip, mem_count)
    grad_into(4, 0, r.flip, r.gkv2_sum, mem_count)
    reduce_x(4)
    sum_finish(0)

    def first_grad(base):
        here = pl.ds(base, BIG)
        back, gain = norm_back(r.x1[here, :], summed(0, base, BIG), 1)
        grad = r.gx[here, :] + back
        r.tiny[1:2, :] = r.tiny[1:2, :] + gain
        r.gx[here, :] = grad
        low = grad.astype(bf16)
        r.gxb[here, :] = low
        r.ga[here, :] = forward_mm(low, weight(SELF_O)).astype(bf16)

    loop_rows(rows, BIG, first_grad)
    for g in (0, 1, 2):
        reduce_f(g)
    sum_finish(2)
    for side in range(2):
        r.out_mem[side * (mem_count // 2) : (side + 1) * (mem_count // 2), :] = (
            r.p_res[2][side].reshape(mem_count // 2, dim).astype(f32)
        )
    attend_back_rows(True, r.q1, r.kv1, r.p1, r.gq1, r.gkv1, keys)
    gkv1_sent = start(r.gkv1.at[1 - x], r.gkv1_in, to_x)
    reduce_z(3)
    reduce_z(4)
    flip(r.gxb, r.flip, rows)
    grad_into(5, 0, r.flip, r.a1, rows)
    flip(r.h1, r.flip, rows)
    grad_into(5, width, r.flip, r.gq1, rows)
    reduce_x(5)
    tiles = keys // BLOCK
    row = lax.broadcasted_iota(jnp.int32, (BLOCK, BLOCK), 0)
    col = lax.broadcasted_iota(jnp.int32, (BLOCK, BLOCK), 1)
    for h in range(heads):
        own = r.strip[h, :, (tiles - 1) * BLOCK : tiles * BLOCK]
        prior = r.strip[h, :, (tiles - 2) * BLOCK : (tiles - 1) * BLOCK]
        far = jnp.where(row < col, 0.0, prior)
        for j in range(tiles - 2):
            far = far + r.strip[h, :, j * BLOCK : (j + 1) * BLOCK]
        r.tiny[3 + h : 4 + h, :BLOCK] = fold_diagonals(own + jnp.where(row < col, prior, 0.0))
        r.tiny[3 + h : 4 + h, BLOCK : 2 * BLOCK] = jnp.sum(far, axis=0, keepdims=True)
    gkv1_sent.wait_recv()
    r.gkv1_sum[...] = (r.gkv1[x].astype(f32) + r.gkv1_in[...].astype(f32)).astype(bf16)

    def input_piece(base):
        here = pl.ds(base, CHUNK)
        return (
            nt(r.gq1[here, :], weight(SELF_Q))
            + nt(r.gkv1_sum[here, :width], weight(SELF_K))
            + nt(r.gkv1_sum[here, width:], weight(SELF_V))
        )

    sum_begin(1, input_piece, wide)
    grad_into(6, 0, r.flip, r.gkv1_sum, rows)
    reduce_x(6)
    for g in (0, 1, 2):
        reduce_o(g)
    for g in (3, 4):
        reduce_f(g)
    reduce_z(5)
    sum_finish(1)

    def input_grad(base):
        here = pl.ds(base, BIG)
        back, gain = norm_back(r.in_dec[here, :].astype(f32), summed(1, base, BIG), 0)
        r.tiny[0:1, :] = r.tiny[0:1, :] + gain
        r.out_input[here, :] = r.gx[here, :] + back

    loop_rows(rows, BIG, input_grad)
    tiny_x = start(r.tiny, r.tiny_in, to_x)
    reduce_z(6)
    tiny_x.wait_recv()
    r.tiny_z[z] = r.tiny[...] + r.tiny_in[...]
    tiny_sent = [start(r.tiny_z.at[z], r.tiny_z.at[z], to_z(k)) for k in (1, 2, 3)]
    reduce_f(5)
    for g in (3, 4):
        reduce_o(g)
    reduce_f(6)
    for c in tiny_sent:
        c.wait_recv()
    total = ((r.tiny_z[0] + r.tiny_z[1]) + r.tiny_z[2]) + r.tiny_z[3]
    for k in range(3):
        piece = jnp.zeros((1, shard_rows), f32)
        for s in range(SHARDS):
            piece = jnp.where(
                z == s, total[k : k + 1, s * shard_rows : (s + 1) * shard_rows], piece
            )
        r.out_gain[k][...] = piece
    lanes = r.in_lanes[...]
    bucket = lax.broadcasted_iota(jnp.int32, (BUCKETS, 1), 0)
    columns = []
    for h in range(heads):
        near = jnp.sum(lanes * total[3 + h : 4 + h, :BLOCK], axis=1, keepdims=True)
        far = jnp.sum(total[3 + h : 4 + h, BLOCK : 2 * BLOCK], axis=1, keepdims=True)
        columns.append(near + jnp.where(bucket == BUCKETS - 1, far, 0.0))
    r.table[...] = jnp.concatenate(columns, axis=1)
    share = BUCKETS // SHARDS
    r.out_table[...] = r.table[pl.ds(pl.multiple_of(z * share, share), share), :]
    for g in (5, 6):
        reduce_o(g)
    for c in unsent:
        c.wait_send()


def local_fast(
    dec_in, memory, dec_segments, mem_segments, gain_self, gain_cross, gain_ffn,
    self_q, self_k, self_v, self_o, cross_q, cross_k, cross_v, cross_o,
    ffn_gate, ffn_up, ffn_down, bias_table, cotangent,
):
    rows, dim = dec_in.shape[1:]
    mem = memory.shape[1]
    width, hidden = self_q.shape[1], ffn_gate.shape[1]
    heads = width // HEAD_DIM
    part = gain_self.shape[0]
    share = bias_table.shape[0]
    keys, mem_keys = 2 * rows, 2 * mem
    half = dim // SHARDS // 2
    gains = jnp.stack([gain_self, gain_cross, gain_ffn])
    small = jnp.pad(gains, ((0, 5), (0, 2 * BLOCK - part)))
    small = jnp.concatenate([small, jnp.pad(bias_table, ((0, 0), (0, 2 * BLOCK - heads)))])
    weights = [
        self_q, self_k, self_v, self_o, cross_q, cross_k, cross_v, cross_o,
        ffn_gate, ffn_up, ffn_down,
    ]
    widths = [w.shape[1] for w in weights]
    joined = [sum(widths[k] for k in group) for group in GROUPS]
    chunks = (rows // 2 // CHUNK, rows // 2 // CHUNK, mem // 2 // CHUNK)
    near = dict(
        in_dec=dec_in[0], in_mem=memory[0], in_seg=dec_segments, in_mseg=mem_segments,
        in_lanes=jnp.asarray(lane_buckets()), in_cot=cotangent[0],
    )
    far = dict(in_small=small, part=weights)

    def out(shape, kind):
        return jax.ShapeDtypeStruct(shape, kind)

    outs = dict(
        out_dec=out((rows, dim), bf16), out_input=out((rows, dim), f32),
        out_mem=out((mem, dim), f32), out_gain=[out((1, part), f32)] * 3,
        out_grad=[out((part, c), f32) for c in widths], out_table=out((share, heads), f32),
    )
    vmem = pltpu.VMEM
    held = dict(
        full=[vmem((SHARDS, 2, half, c), bf16) for c in widths],
        small=vmem((SHARDS, 16, 2 * BLOCK), bf16), seg=vmem((1, keys), f32),
        mseg=vmem((1, mem_keys), f32), seg_col=vmem((rows, 8), f32), gains=vmem((8, dim), f32),
        near=vmem((8, BLOCK), f32), far=vmem((8, BLOCK), f32),
        strip=vmem((heads, BLOCK, (2 * (keys // BLOCK) - 1) * BLOCK), f32),
        h1=vmem((rows, dim), bf16), h2=vmem((rows, dim), bf16), h3=vmem((rows, dim), bf16),
        x1=vmem((rows, dim), f32), x2=vmem((rows, dim), f32),
        q1=vmem((rows, width), bf16), q2=vmem((rows, width), bf16),
        kv1=vmem((2, rows, 2 * width), bf16), kv2=vmem((2, mem, 2 * width), bf16),
        p1=vmem((heads, rows, keys), bf16), p2=vmem((heads, rows, mem_keys), bf16),
        a1=vmem((rows, width), bf16), a2=vmem((rows, width), bf16),
        gm=vmem((rows, hidden), f32), m=vmem((rows, hidden), bf16),
        ggate=vmem((rows, hidden), bf16), gup=vmem((rows, hidden), bf16),
        flip=vmem((dim, rows), bf16), gx=vmem((rows, dim), f32), gxb=vmem((rows, dim), bf16),
        ga=vmem((rows, width), bf16), ds=vmem((rows, keys), bf16),
        gkv_t=vmem((2 * width, keys), f32), gq1=vmem((rows, width), bf16),
        gq2=vmem((rows, width), bf16), gkv1=vmem((2, rows, 2 * width), bf16),
        gkv2=vmem((2, mem, 2 * width), bf16), gkv1_in=vmem((rows, 2 * width), bf16),
        gkv2_in=vmem((mem, 2 * width), bf16), gkv1_sum=vmem((rows, 2 * width), bf16),
        gkv2_sum=vmem((mem, 2 * width), bf16), tiny=vmem((8, dim), f32),
        tiny_in=vmem((8, dim), f32), tiny_z=vmem((SHARDS, 8, dim), f32),
        table=vmem((BUCKETS, heads), f32),
        ps_out=[vmem((n, CHUNK, dim), bf16) for n in chunks],
        ps_in=[vmem((n, CHUNK, dim), bf16) for n in chunks],
        py_out=[vmem((n, CHUNK, dim), bf16) for n in chunks],
        py_in=[vmem((n, CHUNK, dim), bf16) for n in chunks],
        p_acc=[vmem((n, CHUNK, dim), f32) for n in chunks],
        p_res=[vmem((2, n, CHUNK, dim), bf16) for n in chunks],
        stage=[vmem((SHARDS, 2, half, c), bf16) for c in joined],
        xr=[vmem((SHARDS, half, c), bf16) for c in joined],
        zr=[vmem((3, half, c), bf16) for c in joined],
        fb=[vmem((2, half, c), bf16) for c in joined],
        send_sem=pltpu.SemaphoreType.DMA((160,)), recv_sem=pltpu.SemaphoreType.DMA((160,)),
        own_sem=pltpu.SemaphoreType.DMA((24,)),
    )
    in_vmem = pl.BlockSpec(memory_space=pltpu.VMEM)
    flat = [jax.tree.flatten(v) for v in (near, far, outs, held)]
    results = pl.pallas_call(
        functools.partial(
            layer_kernel, (rows, mem, dim, width, heads), [tree for _, tree in flat]
        ),
        out_shape=tuple(flat[2][0]),
        in_specs=[in_vmem] * len(flat[0][0])
        + [pl.BlockSpec(memory_space=pl.ANY)] * len(flat[1][0]),
        out_specs=tuple([in_vmem] * len(flat[2][0])),
        scratch_shapes=flat[3][0],
        compiler_params=pltpu.CompilerParams(
            collective_id=0, has_side_effects=True, vmem_limit_bytes=67043328
        ),
        name="layer",
    )(*flat[0][0], *flat[1][0])
    got = types.SimpleNamespace(**flat[2][1].unflatten(results))
    return (
        got.out_dec[None], got.out_input[None], got.out_mem[None],
        *[g[0] for g in got.out_gain], *got.out_grad, got.out_table,
    )


def shard_part(parts):
    return tuple(
        lax.psum_scatter(p.astype(jnp.bfloat16), SHARD, scatter_dimension=0, tiled=True).astype(
            jnp.float32
        )
        for p in parts
    )


def context_total(parts):
    return tuple(lax.psum(p.astype(jnp.bfloat16), CTX).astype(jnp.float32) for p in parts)


def local(
    dec_in,
    memory,
    dec_segments,
    mem_segments,
    gain_self,
    gain_cross,
    gain_ffn,
    self_q,
    self_k,
    self_v,
    self_o,
    cross_q,
    cross_k,
    cross_v,
    cross_o,
    ffn_gate,
    ffn_up,
    ffn_down,
    bias_table,
    cotangent,
):
    gathered = (
        lax.all_gather(gain_self, SHARD, axis=0, tiled=True),
        lax.all_gather(gain_cross, SHARD, axis=0, tiled=True),
        lax.all_gather(gain_ffn, SHARD, axis=0, tiled=True),
        lax.all_gather(self_q, SHARD, axis=0, tiled=True),
        lax.all_gather(self_k, SHARD, axis=0, tiled=True),
        lax.all_gather(self_v, SHARD, axis=0, tiled=True),
        lax.all_gather(self_o, SHARD, axis=0, tiled=True),
        lax.all_gather(cross_q, SHARD, axis=0, tiled=True),
        lax.all_gather(cross_k, SHARD, axis=0, tiled=True),
        lax.all_gather(cross_v, SHARD, axis=0, tiled=True),
        lax.all_gather(cross_o, SHARD, axis=0, tiled=True),
        lax.all_gather(ffn_gate, SHARD, axis=0, tiled=True),
        lax.all_gather(ffn_up, SHARD, axis=0, tiled=True),
        lax.all_gather(ffn_down, SHARD, axis=0, tiled=True),
        lax.all_gather(bias_table, SHARD, axis=0, tiled=True),
    )
    (
        norm_one,
        norm_two,
        norm_three,
        query_self,
        key_self,
        value_self,
        out_self,
        query_cross,
        key_cross,
        value_cross,
        out_cross,
        gate_full,
        up_full,
        down_full,
        table_full,
    ) = gathered
    gain_one = norm_one.astype(jnp.float32)
    gain_two = norm_two.astype(jnp.float32)
    gain_three = norm_three.astype(jnp.float32)
    table = table_full.astype(jnp.float32)
    width = query_self.shape[1]
    hidden_in = dec_in[0].astype(jnp.float32)
    mem_rows = memory[0]
    grad_out = cotangent[0].astype(jnp.float32)
    count_rows = hidden_in.shape[0]
    place = lax.axis_index(CTX)
    dec_ids = dec_segments[0]
    mem_ids = mem_segments[0]
    query_ids = lax.dynamic_slice_in_dim(dec_ids, place * count_rows, count_rows)
    query_pos = place * count_rows + jnp.arange(count_rows, dtype=jnp.int32)
    key_pos = jnp.arange(dec_ids.shape[0], dtype=jnp.int32)
    mem_pos = jnp.arange(mem_ids.shape[0], dtype=jnp.int32)
    normed_one = rms_norm(hidden_in, gain_one).astype(jnp.bfloat16)
    query_one = forward_mm(normed_one, query_self).astype(jnp.bfloat16)
    pairs_own = jnp.concatenate(
        [forward_mm(normed_one, key_self), forward_mm(normed_one, value_self)], axis=1
    ).astype(jnp.bfloat16)
    pairs_one = lax.all_gather(pairs_own, CTX, axis=0, tiled=True)
    mixed_one, lse_one = attend(
        query_one, pairs_one, key_pos, dec_ids, query_pos, query_ids, table, True
    )
    context_one = mixed_one.astype(jnp.bfloat16)
    first = hidden_in + lax.psum(
        backward_mm(context_one, out_self).astype(jnp.bfloat16), TENSOR
    ).astype(jnp.float32)
    normed_two = rms_norm(first, gain_two).astype(jnp.bfloat16)
    query_two = forward_mm(normed_two, query_cross).astype(jnp.bfloat16)
    pairs_mem = jnp.concatenate(
        [forward_mm(mem_rows, key_cross), forward_mm(mem_rows, value_cross)], axis=1
    ).astype(jnp.bfloat16)
    pairs_two = lax.all_gather(pairs_mem, CTX, axis=0, tiled=True)
    mixed_two, lse_two = attend(
        query_two, pairs_two, mem_pos, mem_ids, query_pos, query_ids, table, False
    )
    context_two = mixed_two.astype(jnp.bfloat16)
    second = first + lax.psum(
        backward_mm(context_two, out_cross).astype(jnp.bfloat16), TENSOR
    ).astype(jnp.float32)
    normed_three = rms_norm(second, gain_three).astype(jnp.bfloat16)
    gate = forward_mm(normed_three, gate_full)
    upper = forward_mm(normed_three, up_full)
    activated = gated(gate, upper).astype(jnp.bfloat16)
    result = second + lax.psum(
        backward_mm(activated, down_full).astype(jnp.bfloat16), TENSOR
    ).astype(jnp.float32)
    dec_out = result.astype(jnp.bfloat16)
    grad_low = cotangent[0]
    grad_down_w = weight_mm(grad_low, activated)
    grad_hidden = forward_mm(grad_low, down_full)
    _, pull_gate = jax.vjp(gated, gate, upper)
    grad_gate, grad_upper = pull_gate(grad_hidden)
    gate_low = grad_gate.astype(jnp.bfloat16)
    upper_low = grad_upper.astype(jnp.bfloat16)
    grad_gate_w = weight_mm(normed_three, gate_low)
    grad_up_w = weight_mm(normed_three, upper_low)
    grad_normed_three = backward_mm(gate_low, gate_full) + backward_mm(upper_low, up_full)
    grad_normed_three = lax.psum(grad_normed_three.astype(jnp.bfloat16), TENSOR).astype(
        jnp.float32
    )
    _, pull_three = jax.vjp(rms_norm, second, gain_three)
    grad_second, grad_gain_three = pull_three(grad_normed_three)
    grad_second = grad_out + grad_second
    second_low = grad_second.astype(jnp.bfloat16)
    grad_out_cross = weight_mm(second_low, context_two)
    grad_context_two = forward_mm(second_low, out_cross).astype(jnp.bfloat16)
    grad_query_two, grad_pairs_two, _ = attend_back(
        query_two,
        pairs_two,
        mem_pos,
        mem_ids,
        query_pos,
        query_ids,
        table,
        False,
        mixed_two,
        lse_two,
        grad_context_two,
    )
    pairs_grad_mem = lax.psum_scatter(
        grad_pairs_two.astype(jnp.bfloat16), CTX, scatter_dimension=0, tiled=True
    )
    query_two_low = grad_query_two.astype(jnp.bfloat16)
    grad_mem_keys = pairs_grad_mem[:, :width]
    grad_mem_values = pairs_grad_mem[:, width:]
    grad_query_cross = weight_mm(normed_two, query_two_low)
    grad_key_cross = weight_mm(mem_rows, grad_mem_keys)
    grad_value_cross = weight_mm(mem_rows, grad_mem_values)
    grad_normed_two = backward_mm(query_two_low, query_cross)
    grad_memory = backward_mm(grad_mem_keys, key_cross) + backward_mm(grad_mem_values, value_cross)
    grad_normed_two, grad_memory = (
        lax.psum(grad_normed_two.astype(jnp.bfloat16), TENSOR).astype(jnp.float32),
        lax.psum(grad_memory.astype(jnp.bfloat16), TENSOR).astype(jnp.float32),
    )
    _, pull_two = jax.vjp(rms_norm, first, gain_two)
    grad_first, grad_gain_two = pull_two(grad_normed_two)
    grad_first = grad_second + grad_first
    first_low = grad_first.astype(jnp.bfloat16)
    grad_out_self = weight_mm(first_low, context_one)
    grad_context_one = forward_mm(first_low, out_self).astype(jnp.bfloat16)
    grad_query_one, grad_pairs_one, grad_table = attend_back(
        query_one,
        pairs_one,
        key_pos,
        dec_ids,
        query_pos,
        query_ids,
        table,
        True,
        mixed_one,
        lse_one,
        grad_context_one,
    )
    pairs_grad_own = lax.psum_scatter(
        grad_pairs_one.astype(jnp.bfloat16), CTX, scatter_dimension=0, tiled=True
    )
    query_one_low = grad_query_one.astype(jnp.bfloat16)
    grad_keys_own = pairs_grad_own[:, :width]
    grad_values_own = pairs_grad_own[:, width:]
    grad_query_self = weight_mm(normed_one, query_one_low)
    grad_key_self = weight_mm(normed_one, grad_keys_own)
    grad_value_self = weight_mm(normed_one, grad_values_own)
    grad_normed_one = (
        backward_mm(query_one_low, query_self)
        + backward_mm(grad_keys_own, key_self)
        + backward_mm(grad_values_own, value_self)
    )
    grad_normed_one = lax.psum(grad_normed_one.astype(jnp.bfloat16), TENSOR).astype(jnp.float32)
    _, pull_one = jax.vjp(rms_norm, hidden_in, gain_one)
    grad_input, grad_gain_one = pull_one(grad_normed_one)
    grad_input = grad_first + grad_input
    local_grads = (
        grad_gain_one,
        grad_gain_two,
        grad_gain_three,
        grad_query_self,
        grad_key_self,
        grad_value_self,
        grad_out_self,
        grad_query_cross,
        grad_key_cross,
        grad_value_cross,
        grad_out_cross,
        grad_gate_w,
        grad_up_w,
        grad_down_w,
        grad_table,
    )
    summed = shard_part(context_total(local_grads))
    return (
        dec_out[None],
        grad_input[None],
        grad_memory[None],
        summed[0],
        summed[1],
        summed[2],
        summed[3],
        summed[4],
        summed[5],
        summed[6],
        summed[7],
        summed[8],
        summed[9],
        summed[10],
        summed[11],
        summed[12],
        summed[13],
        summed[14],
    )


def solution(mesh):
    in_specs = (
        P(SHARD, CTX, None),
        P(SHARD, CTX, None),
        P(SHARD, None),
        P(SHARD, None),
        P(SHARD),
        P(SHARD),
        P(SHARD),
        P(SHARD, TENSOR),
        P(SHARD, TENSOR),
        P(SHARD, TENSOR),
        P(SHARD, TENSOR),
        P(SHARD, TENSOR),
        P(SHARD, TENSOR),
        P(SHARD, TENSOR),
        P(SHARD, TENSOR),
        P(SHARD, TENSOR),
        P(SHARD, TENSOR),
        P(SHARD, TENSOR),
        P(SHARD, TENSOR),
        P(SHARD, CTX, None),
    )
    out_specs = (
        P(SHARD, CTX, None),
        P(SHARD, CTX, None),
        P(SHARD, CTX, None),
        P(SHARD),
        P(SHARD),
        P(SHARD),
        P(SHARD, TENSOR),
        P(SHARD, TENSOR),
        P(SHARD, TENSOR),
        P(SHARD, TENSOR),
        P(SHARD, TENSOR),
        P(SHARD, TENSOR),
        P(SHARD, TENSOR),
        P(SHARD, TENSOR),
        P(SHARD, TENSOR),
        P(SHARD, TENSOR),
        P(SHARD, TENSOR),
        P(SHARD, TENSOR),
    )
    fast = (mesh.shape[SHARD], mesh.shape[CTX], mesh.shape[TENSOR]) == (SHARDS, 2, 4)
    body = local_fast if fast else local
    return jax.shard_map(body, mesh=mesh, in_specs=in_specs, out_specs=out_specs, check_vma=False)
```

```python
import functools
import types

import jax
import jax.numpy as jnp
import numpy as np
from jax import lax
from jax.experimental import pallas as pl
from jax.experimental.pallas import tpu as pltpu
from jax.sharding import PartitionSpec as P

SHARD, CTX, TENSOR = "shard", "ctx", "tensor"
HEAD_DIM = 64
BUCKETS = 32
MAX_DIST = 128


highest = lax.Precision.HIGHEST
epsilon = 1e-06
negative = -1e30


def thresholds():
    exact_part = BUCKETS // 2
    small_part = np.arange(1, exact_part + 1)
    steps_up = np.arange(exact_part + 1, BUCKETS)
    large_part = np.ceil(
        exact_part * (MAX_DIST / exact_part) ** ((steps_up - exact_part) / (BUCKETS - exact_part))
    )
    return np.concatenate([small_part, large_part]).astype(np.int32)


def bucket_of(distance):
    limits = jnp.asarray(thresholds())
    return jnp.sum((distance[..., None] >= limits).astype(jnp.int32), axis=-1)


def rms_norm(values, gain):
    return values * lax.rsqrt(jnp.mean(values * values, axis=-1, keepdims=True) + epsilon) * gain


def gated(gate, upper):
    return jax.nn.gelu(gate, approximate=True) * upper


def forward_mm(left, right):
    return jnp.dot(left, right, preferred_element_type=jnp.float32)


def backward_mm(left, right):
    return lax.dot_general(
        left, right, (((1,), (1,)), ((), ())), preferred_element_type=jnp.float32
    )


def weight_mm(left, right):
    return lax.dot_general(
        left, right, (((0,), (0,)), ((), ())), preferred_element_type=jnp.float32
    )


def toeplitz(vector, count_rows, count_cols):
    heads = vector.shape[0]
    span = count_rows + count_cols - 1
    tiled = jnp.pad(jnp.tile(vector, (1, count_rows)), ((0, 0), (0, count_rows)))
    grid = tiled.reshape(heads, count_rows, span + 1)[:, :, :count_cols]
    return grid[:, :, ::-1]


def diagonal_sums(block):
    heads, count_rows, count_cols = block.shape
    span = count_rows + count_cols - 1
    flipped = jnp.pad(block[:, :, ::-1], ((0, 0), (0, 0), (0, count_rows)))
    flat = flipped.reshape(heads, count_rows * (span + 1))[:, : count_rows * span]
    return jnp.sum(flat.reshape(heads, count_rows, span), axis=1)


def bias_block(table, offset, count_rows, count_cols):
    span = count_rows + count_cols - 1
    distance = jnp.arange(span, dtype=jnp.int32) - (count_cols - 1) + offset
    onehot = (
        bucket_of(distance)[:, None] == jnp.arange(table.shape[0], dtype=jnp.int32)[None, :]
    ).astype(jnp.float32)
    column = jnp.dot(onehot, table, precision=highest)
    return (toeplitz(column.T, count_rows, count_cols), onehot)


def key_blocks(pairs, key_pos, key_seg):
    length = pairs.shape[0]
    width = min(512, length)
    count = length // width
    heads = pairs.shape[1] // (2 * HEAD_DIM)
    blocks = pairs.reshape(count, width, 2, heads, HEAD_DIM)
    starts = jnp.arange(count, dtype=jnp.int32) * width
    return (blocks, key_pos.reshape(count, width), key_seg.reshape(count, width), starts)


def scores_of(query, block, block_pos, block_seg, start, query_pos, query_seg, table, causal):
    scores = jnp.einsum("qhd,khd->hqk", query, block[:, 0], preferred_element_type=jnp.float32)
    mask = query_seg[:, None] == block_seg[None, :]
    onehot = None
    if causal:
        mask = mask & (query_pos[:, None] >= block_pos[None, :])
        bias, onehot = bias_block(table, query_pos[0] - start, query.shape[0], block.shape[0])
        scores = scores + bias
    return (jnp.where(mask[None], scores, negative), mask, onehot)


def attend(query, pairs, key_pos, key_seg, query_pos, query_seg, table, causal):
    count_rows = query.shape[0]
    heads = query.shape[1] // HEAD_DIM
    query = query.reshape(count_rows, heads, HEAD_DIM)
    blocks = key_blocks(pairs, key_pos, key_seg)

    def stats(carry, item):
        peak, total = carry
        block, block_pos, block_seg, start = item
        scores, mask, _ = scores_of(
            query, block, block_pos, block_seg, start, query_pos, query_seg, table, causal
        )
        fresh = jnp.maximum(peak, jnp.max(scores, axis=-1))
        weights = jnp.where(mask[None], jnp.exp(scores - fresh[..., None]), 0.0)
        total = total * jnp.exp(peak - fresh) + jnp.sum(weights, axis=-1)
        return ((fresh, total), None)

    start_peak = jnp.full((heads, count_rows), negative, jnp.float32)
    start_total = jnp.zeros((heads, count_rows), jnp.float32)
    (peak, total), _ = lax.scan(stats, (start_peak, start_total), blocks)
    log_total = peak + jnp.log(total)

    def collect(accum, item):
        block, block_pos, block_seg, start = item
        scores, mask, _ = scores_of(
            query, block, block_pos, block_seg, start, query_pos, query_seg, table, causal
        )
        probs = jnp.where(mask[None], jnp.exp(scores - log_total[..., None]), 0.0).astype(
            jnp.bfloat16
        )
        accum = accum + jnp.einsum(
            "hqk,khd->qhd", probs, block[:, 1], preferred_element_type=jnp.float32
        )
        return (accum, None)

    mixed, _ = lax.scan(collect, jnp.zeros((count_rows, heads, HEAD_DIM), jnp.float32), blocks)
    return (mixed.reshape(count_rows, heads * HEAD_DIM), log_total)


def correction_of(grad_mixed, mixed):
    count_rows = mixed.shape[0]
    heads = mixed.shape[1] // HEAD_DIM
    return jnp.einsum(
        "qhd,qhd->hq",
        grad_mixed.reshape(count_rows, heads, HEAD_DIM).astype(jnp.float32),
        mixed.reshape(count_rows, heads, HEAD_DIM),
    )


def attend_back(
    query,
    pairs,
    key_pos,
    key_seg,
    query_pos,
    query_seg,
    table,
    causal,
    mixed,
    log_total,
    grad_mixed,
):
    count_rows = query.shape[0]
    heads = query.shape[1] // HEAD_DIM
    query = query.reshape(count_rows, heads, HEAD_DIM)
    grad_heads = grad_mixed.reshape(count_rows, heads, HEAD_DIM)
    correction = correction_of(grad_mixed, mixed)
    blocks = key_blocks(pairs, key_pos, key_seg)

    def step(carry, item):
        grad_query, grad_table = carry
        block, block_pos, block_seg, start = item
        scores, mask, onehot = scores_of(
            query, block, block_pos, block_seg, start, query_pos, query_seg, table, causal
        )
        probs = jnp.where(mask[None], jnp.exp(scores - log_total[..., None]), 0.0)
        grad_probs = jnp.einsum(
            "qhd,khd->hqk", grad_heads, block[:, 1], preferred_element_type=jnp.float32
        )
        grad_scores = probs * (grad_probs - correction[..., None])
        if causal:
            grad_table = grad_table + jnp.dot(
                onehot.T, diagonal_sums(grad_scores).T, precision=highest
            )
        low_scores = grad_scores.astype(jnp.bfloat16)
        grad_query = grad_query + jnp.einsum(
            "hqk,khd->qhd", low_scores, block[:, 0], preferred_element_type=jnp.float32
        )
        stacked = None
        grad_values = jnp.einsum(
            "hqk,qhd->khd",
            probs.astype(jnp.bfloat16),
            grad_heads,
            preferred_element_type=jnp.float32,
        )
        grad_keys = jnp.einsum(
            "hqk,qhd->khd", low_scores, query, preferred_element_type=jnp.float32
        )
        width = block.shape[0]
        stacked = jnp.concatenate(
            [
                grad_keys.reshape(width, heads * HEAD_DIM),
                grad_values.reshape(width, heads * HEAD_DIM),
            ],
            axis=1,
        )
        return ((grad_query, grad_table), stacked)

    start = (
        jnp.zeros((count_rows, heads, HEAD_DIM), jnp.float32),
        jnp.zeros(table.shape, jnp.float32),
    )
    (grad_query, grad_table), grad_pairs = lax.scan(step, start, blocks)
    grad_pairs = grad_pairs.reshape(pairs.shape[0], pairs.shape[1])
    return (grad_query.reshape(count_rows, heads * HEAD_DIM), grad_pairs, grad_table)


BLOCK = 128


def nt(left, right):
    return lax.dot_general(
        left, right, (((1,), (1,)), ((), ())), preferred_element_type=jnp.float32
    )


def tn(left, right):
    return lax.dot_general(
        left, right, (((0,), (0,)), ((), ())), preferred_element_type=jnp.float32
    )


def lane_buckets():
    lane = np.arange(BLOCK)
    distance = (BLOCK - lane) % BLOCK
    bucket = (distance[:, None] >= thresholds()[None, :]).sum(axis=1)
    return (bucket[None, :] == np.arange(BUCKETS)[:, None]).astype(np.float32)


def build_strip(near_ref, far_ref, strip_ref, tiles, heads):
    row = lax.broadcasted_iota(jnp.int32, (BLOCK, BLOCK), 0)
    col = lax.broadcasted_iota(jnp.int32, (BLOCK, BLOCK), 1)
    for h in range(heads):
        near = jnp.broadcast_to(near_ref[h : h + 1, :], (BLOCK, BLOCK))
        near = pltpu.roll(near, 0, 1, stride=1, stride_axis=0)
        far = jnp.broadcast_to(far_ref[h : h + 1, :], (BLOCK, BLOCK))
        for m in range(tiles - 2):
            strip_ref[h, :, m * BLOCK : (m + 1) * BLOCK] = far
        strip_ref[h, :, (tiles - 2) * BLOCK : (tiles - 1) * BLOCK] = jnp.where(
            row < col, near, far
        )
        strip_ref[h, :, (tiles - 1) * BLOCK : tiles * BLOCK] = near
        strip_ref[h, :, tiles * BLOCK :] = jnp.zeros((BLOCK, (tiles - 1) * BLOCK), jnp.float32)


def fold_diagonals(tile):
    rows = BLOCK
    while rows > 8:
        rows //= 2
        tile = tile[:rows] + pltpu.roll(tile[rows:], BLOCK - rows, 1)
    total = tile[0:1]
    for r in range(1, 8):
        total = total + pltpu.roll(tile[r : r + 1], BLOCK - r, 1)
    return total


SELF_Q, SELF_K, SELF_V, SELF_O, CROSS_Q, CROSS_K, CROSS_V, CROSS_O, GATE, UP, DOWN = range(11)
GROUPS = (
    (DOWN,), (GATE,), (UP,), (CROSS_O, CROSS_Q), (CROSS_K, CROSS_V),
    (SELF_O, SELF_Q), (SELF_K, SELF_V),
)
ORDER = (
    SELF_K, SELF_V, SELF_Q, SELF_O, CROSS_K, CROSS_V, CROSS_Q, CROSS_O, GATE, UP, DOWN,
)
CHUNK = 128
BIG = 256
SHARDS = 4
MESH = pl.DeviceIdType.MESH
bf16 = jnp.bfloat16
f32 = jnp.float32


def loop_rows(count, block, step):
    def body(i, carry):
        step(pl.multiple_of(i * block, block))
        return carry

    lax.fori_loop(0, count // block, body, 0)


def layer_kernel(shape, trees, *refs):
    found, at = {}, 0
    for tree in trees:
        found.update(tree.unflatten(refs[at : at + tree.num_leaves]))
        at += tree.num_leaves
    r = types.SimpleNamespace(**found)
    rows, mem_count, dim, width, heads = shape
    keys = 2 * rows
    mem_keys = 2 * mem_count
    half = dim // SHARDS // 2
    z = lax.axis_index(SHARD)
    x = lax.axis_index(CTX)
    t = lax.axis_index(TENSOR)
    core = lax.rem(t, 2)
    to_x = {CTX: 1 - x}
    to_core = {TENSOR: t + 1 - 2 * core}
    to_y = {TENSOR: lax.rem(t + 2, 4)}

    def to_z(k):
        return {SHARD: lax.rem(z + k, SHARDS)}

    send_sem, recv_sem = r.send_sem, r.recv_sem
    used = [0]
    unsent = []

    def copy(src, dst, where):
        i = used[0]
        used[0] += 1
        return pltpu.make_async_remote_copy(
            src_ref=src, dst_ref=dst, send_sem=send_sem.at[i], recv_sem=recv_sem.at[i],
            device_id=where, device_id_type=MESH,
        )

    def start(src, dst, where):
        c = copy(src, dst, where)
        c.start()
        unsent.append(c)
        return c

    barrier = pltpu.get_barrier_semaphore()
    others = [dict(to_z(k), ctx=1 - x) for k in (1, 2, 3)]
    partners = [to_z(1), to_z(2), to_z(3), to_x, to_core, to_y] + others
    for p in partners:
        pl.semaphore_signal(barrier, inc=1, device_id=p, device_id_type=MESH)

    own_copies = {}
    for name in ORDER:
        full, part = r.full[name], r.part[name]
        own_copies[name] = []
        for side in range(2):
            c = pltpu.make_async_copy(
                part.at[pl.ds(side * half, half), :], full.at[z, side],
                r.own_sem.at[2 * name + side],
            )
            c.start()
            own_copies[name].append(c)
    small_own = pltpu.make_async_copy(r.in_small, r.small.at[z], r.own_sem.at[22])
    small_own.start()
    leaving = []

    def leave(src, dst):
        c = pltpu.make_async_copy(src, dst, r.own_sem.at[23 + len(leaving)])
        c.start()
        leaving.append(c)

    seg = r.in_seg[...].astype(f32)
    r.seg[...] = seg
    r.mseg[...] = r.in_mseg[...].astype(f32)
    own_seg = r.seg[:, pl.ds(pl.multiple_of(x * rows, BLOCK), rows)]
    r.seg_col[...] = jnp.broadcast_to(own_seg, (8, rows)).T
    pl.semaphore_wait(barrier, len(partners))

    gathers = {}

    def gather_start(name):
        full, part = r.full[name], r.part[name]
        sent = [
            start(part.at[pl.ds(x * half, half), :], full.at[z, x], to_z(k)) for k in (1, 2, 3)
        ]
        gathers[name] = (sent, [])

    def gather_pump(*chosen):
        for name in chosen:
            sent, passed = gathers[name]
            full = r.full[name]
            for k in (1, 2, 3):
                sent[k - 1].wait_recv()
                source = lax.rem(z + SHARDS - k, SHARDS)
                passed.append(start(full.at[source, x], full.at[source, x], to_x))

    def gather_wait(*chosen):
        for name in chosen:
            for c in own_copies[name]:
                c.wait()
            for c in gathers[name][1]:
                c.wait_recv()

    def weight(name):
        ref = r.full[name]
        return ref[...].reshape(dim, ref.shape[-1])

    small_sent = [start(r.in_small, r.small.at[z], to_z(k)) for k in (1, 2, 3)]
    for name in ORDER:
        gather_start(name)

    small_own.wait()
    for c in small_sent:
        c.wait_recv()
    gathered = [r.small[n].astype(f32) for n in range(SHARDS)]
    for k in range(3):
        r.gains[k : k + 1, :] = jnp.concatenate(
            [g[k : k + 1, : dim // SHARDS] for g in gathered], axis=1
        )
    table = jnp.concatenate([g[8:16, :BLOCK] for g in gathered], axis=0)
    near = tn(table.astype(bf16), r.in_lanes[...].astype(bf16))
    r.near[...] = near[:8]
    lane_of = lax.broadcasted_iota(jnp.int32, (8, BLOCK), 1)
    row_of = lax.broadcasted_iota(jnp.int32, (8, BLOCK), 0)
    last = jnp.broadcast_to(table[BUCKETS - 1 : BUCKETS, :], (8, BLOCK))
    last = jnp.sum(jnp.where(lane_of == row_of, last, 0.0), axis=1, keepdims=True)
    r.far[...] = jnp.broadcast_to(last, (8, BLOCK))
    build_strip(r.near, r.far, r.strip, keys // BLOCK, heads)

    def inverse(v):
        return lax.rsqrt(jnp.mean(v * v, axis=1, keepdims=True) + epsilon)

    def norm(v, k):
        return (v * inverse(v) * r.gains[k : k + 1, :]).astype(bf16)

    def input_norm(base):
        here = pl.ds(base, BIG)
        r.h1[here, :] = norm(r.in_dec[here, :].astype(f32), 0)

    loop_rows(rows, BIG, input_norm)

    def head_pairs(dst, here, left, right):
        for h in range(heads):
            lanes = slice(h * HEAD_DIM, (h + 1) * HEAD_DIM)
            dst[h, x, here, :] = jnp.concatenate([left[:, lanes], right[:, lanes]], axis=1).astype(
                bf16
            )

    gather_pump(SELF_K, SELF_V)
    gather_wait(SELF_K, SELF_V)
    gather_pump(SELF_Q)

    def project(base):
        here = pl.ds(base, BIG)
        h = r.h1[here, :]
        head_pairs(
            r.kv1, here, forward_mm(h, weight(SELF_K)), forward_mm(h, weight(SELF_V))
        )

    loop_rows(rows, BIG, project)
    kv1_sent = [start(r.kv1.at[h, x], r.kv1.at[h, x], to_x) for h in range(heads)]
    gather_wait(SELF_Q)

    def project_query(base):
        here = pl.ds(base, BIG)
        r.q1[here, :] = forward_mm(r.h1[here, :], weight(SELF_Q)).astype(bf16)

    loop_rows(rows, BIG, project_query)
    gather_pump(SELF_O)

    def attend_block(causal, h, base, q, kv, cols, p_ref, a_ref, total):
        tiles = total // BLOCK
        here = pl.ds(base, BLOCK)
        lanes = slice(h * HEAD_DIM, (h + 1) * HEAD_DIM)
        pair = kv[h].reshape(total, 2 * HEAD_DIM)
        mask = r.seg_col[here, 0:1] == cols[...]
        scores = nt(q[here, lanes], pair[:, :HEAD_DIM])
        if causal:
            first = x * rows + base
            row = lax.broadcasted_iota(jnp.int32, (BLOCK, total), 0) + first
            col = lax.broadcasted_iota(jnp.int32, (BLOCK, total), 1)
            mask = mask & (row >= col)
            begin = pl.multiple_of((tiles - 1) * BLOCK - first, BLOCK)
            scores = scores + r.strip[h, :, pl.ds(begin, total)]
        scores = jnp.where(mask, scores, negative)
        peak = jnp.max(scores, axis=1, keepdims=True)
        weights = jnp.exp(scores - peak)
        probs = (weights / jnp.sum(weights, axis=1, keepdims=True)).astype(bf16)
        p_ref[h, here, :] = probs
        a_ref[here, lanes] = forward_mm(probs, pair[:, HEAD_DIM:]).astype(bf16)

    sums = {}

    def sides(key, j):
        n = r.p_res[key].shape[1]
        return [
            pl.multiple_of(((1 - core) * n + j) * CHUNK, CHUNK),
            pl.multiple_of((core * n + j) * CHUNK, CHUNK),
        ]

    def sum_send(key, j, piece):
        state = sums.setdefault((key, j), {})
        for c in state.values():
            c.wait_send()
            unsent[:] = [u for u in unsent if u is not c]
        other, own = sides(key, j)
        r.ps_out[key][j] = piece(other).astype(bf16)
        state[0] = start(r.ps_out[key].at[j], r.ps_in[key].at[j], to_core)
        mine = piece(own)
        state[0].wait_recv()
        r.py_out[key][j] = (mine + r.ps_in[key][j].astype(f32)).astype(bf16)
        state[1] = start(r.py_out[key].at[j], r.py_in[key].at[j], to_y)

    def sum_recv(key, j, between=None):
        state = sums[(key, j)]
        res = r.p_res[key]
        state[1].wait_recv()
        res[core, j] = (r.py_out[key][j].astype(f32) + r.py_in[key][j].astype(f32)).astype(bf16)
        state[2] = start(res.at[core, j], res.at[core, j], to_core)
        if between is not None:
            between()
        state[2].wait_recv()

    def both_sides(key, j, step):
        other, own = sides(key, j)
        step(other, r.p_res[key][1 - core, j].astype(f32))
        step(own, r.p_res[key][core, j].astype(f32))

    wide = r.p_res[0].shape[1]
    slim = r.p_res[2].shape[1]
    for h in range(heads):
        kv1_sent[h].wait_recv()
        if h == 0:
            gather_pump(CROSS_K, CROSS_V, CROSS_Q, CROSS_O)

        def self_rows(base):
            attend_block(True, h, base, r.q1, r.kv1, r.seg, r.p1, r.a1, keys)

        loop_rows(rows, BLOCK, self_rows)
    gather_wait(SELF_O)
    for j in range(wide):
        sum_send(0, j, lambda base: nt(r.a1[pl.ds(base, CHUNK), :], weight(SELF_O)))
    gather_wait(CROSS_K, CROSS_V)
    memory = r.in_mem[...]
    head_pairs(
        r.kv2, slice(None), forward_mm(memory, weight(CROSS_K)),
        forward_mm(memory, weight(CROSS_V)),
    )
    kv2_sent = [start(r.kv2.at[h, x], r.kv2.at[h, x], to_x) for h in range(heads)]
    gather_wait(CROSS_Q, CROSS_O)
    gather_pump(GATE)

    for j in range(wide):
        sum_recv(0, j)

        def second(base, value):
            here = pl.ds(base, CHUNK)
            v = r.in_dec[here, :].astype(f32) + value
            r.x1[here, :] = v
            h = norm(v, 1)
            r.h2[here, :] = h
            r.q2[here, :] = forward_mm(h, weight(CROSS_Q)).astype(bf16)

        both_sides(0, j, second)
        if j == 0:
            for c in kv2_sent:
                c.wait_recv()
            gather_pump(UP)

        def mixed(base):
            for h in range(heads):
                attend_block(False, h, base, r.q2, r.kv2, r.mseg, r.p2, r.a2, mem_keys)
            return nt(r.a2[pl.ds(base, CHUNK), :], weight(CROSS_O))

        sum_send(1, j, mixed)
    gather_pump(DOWN)

    def flip(src, dst, count):
        for j in range(dim // BLOCK):
            dst[j * BLOCK : (j + 1) * BLOCK, :count] = src[:, j * BLOCK : (j + 1) * BLOCK].T

    flip(r.in_cot, r.flip, rows)
    gather_wait(DOWN)

    def grad_hidden_block(base):
        here = pl.ds(base, BIG)
        r.gm[here, :] = forward_mm(r.in_cot[here, :], weight(DOWN))

    loop_rows(rows, BIG, grad_hidden_block)
    gather_wait(GATE, UP)

    for j in range(wide):
        sum_recv(1, j)

        def third(base, value):
            here = pl.ds(base, CHUNK)
            v = r.x1[here, :] + value
            r.x2[here, :] = v
            r.h3[here, :] = norm(v, 2)

        both_sides(1, j, third)

        def hidden_piece(base):
            here = pl.ds(base, CHUNK)
            h = r.h3[here, :]
            gate = forward_mm(h, weight(GATE))
            upper = forward_mm(h, weight(UP))
            scale = np.float32(np.sqrt(2.0 / np.pi))
            square = gate * gate
            curve = jnp.tanh(scale * (gate + 0.044715 * (square * gate)))
            lower = 0.5 * (1.0 + curve)
            gelu = gate * lower
            slope = lower + 0.5 * gate * (1.0 - curve * curve) * scale * (
                1.0 + 3 * 0.044715 * square
            )
            grad = r.gm[here, :]
            r.m[here, :] = (gelu * upper).astype(bf16)
            grad_gate = (grad * upper * slope).astype(bf16)
            grad_up = (grad * gelu).astype(bf16)
            r.ggate[here, :] = grad_gate
            r.gup[here, :] = grad_up
            return nt(grad_gate, weight(GATE)) + nt(grad_up, weight(UP))

        sum_send(0, j, hidden_piece)

    shard_rows = dim // SHARDS

    def grad_into(g, at, flipped, right, count):
        stage = r.stage[g]
        cols = right.shape[1]

        def step(d, carry):
            here = pl.ds(pl.multiple_of(d * shard_rows, shard_rows), shard_rows)
            value = forward_mm(flipped[here, :count], right[...]).astype(bf16)
            stage[d, :, :, at : at + cols] = value.reshape(2, half, cols)
            return carry

        lax.fori_loop(0, SHARDS, step, 0)

    reduces = {}

    def reduce_x(g):
        stage = r.stage[g]
        reduces[g] = [start(stage.at[:, 1 - x], r.xr[g], to_x)]

    def reduce_z(g):
        stage, xr, zr = r.stage[g], r.xr[g], r.zr[g]
        reduces[g][0].wait_recv()

        def step(d, carry):
            stage[d, x] = (stage[d, x].astype(f32) + xr[d].astype(f32)).astype(bf16)
            return carry

        lax.fori_loop(0, SHARDS, step, 0)
        for k in (1, 2, 3):
            d = lax.rem(z + k, SHARDS)
            reduces[g].append(start(stage.at[d, x], zr.at[k - 1], to_z(k)))

    def reduce_f(g):
        stage, zr, both = r.stage[g], r.zr[g], r.fb[g]
        total = stage[z, x].astype(f32)
        for k in (1, 2, 3):
            reduces[g][k].wait_recv()
            total = total + zr[k - 1].astype(f32)
        both[x] = total.astype(bf16)
        reduces[g].append(start(both.at[x], both.at[x], to_x))

    def reduce_o(g):
        reduces[g][4].wait_recv()
        leave(r.fb[g], r.o_fb[g])

    grad_into(0, 0, r.flip, r.m, rows)
    reduce_x(0)
    flip(r.h3, r.flip, rows)
    grad_into(1, 0, r.flip, r.ggate, rows)
    reduce_x(1)
    grad_into(2, 0, r.flip, r.gup, rows)
    reduce_x(2)

    def norm_back(v, grad, k):
        inv = inverse(v)
        unit = v * inv
        scaled = grad * r.gains[k : k + 1, :]
        mean = jnp.mean(scaled * unit, axis=1, keepdims=True)
        return inv * (scaled - unit * mean), jnp.sum(grad * unit, axis=0, keepdims=True)

    def attend_back_block(causal, h, base, q, kv, p_ref, gq, ds, total):
        tiles = total // BLOCK
        here = pl.ds(base, BLOCK)
        lanes = slice(h * HEAD_DIM, (h + 1) * HEAD_DIM)
        pair = kv[h].reshape(total, 2 * HEAD_DIM)
        probs = p_ref[h, here, :].astype(f32)
        grad_probs = nt(r.ga[here, lanes], pair[:, HEAD_DIM:])
        mean = jnp.sum(probs * grad_probs, axis=1, keepdims=True)
        scores = probs * (grad_probs - mean)
        if causal:
            begin = pl.multiple_of((tiles - 1) * BLOCK - x * rows - base, BLOCK)
            window = pl.ds(begin, total)
            r.strip[h, :, window] = r.strip[h, :, window] + scores
        low = scores.astype(bf16)
        ds[here, :] = low
        gq[here, lanes] = forward_mm(low, pair[:, :HEAD_DIM]).astype(bf16)

    def pair_grads(h, q, p_ref, ds, gkv, total):
        lanes = slice(h * HEAD_DIM, (h + 1) * HEAD_DIM)
        r.gkv_t[:HEAD_DIM, :total] = tn(q[:, lanes], ds[...])
        r.gkv_t[HEAD_DIM:, :total] = tn(r.ga[:, lanes], p_ref[h])
        part = total // 2
        for side in range(2):
            gkv[h, side] = r.gkv_t[:, side * part : (side + 1) * part].T.astype(bf16)

    def pairs_sum(gkv, arrived, out):
        left, right = [], []
        for h in range(heads):
            value = gkv[h, x].astype(f32) + arrived[h].astype(f32)
            left.append(value[:, :HEAD_DIM])
            right.append(value[:, HEAD_DIM:])
        out[...] = jnp.concatenate(left + right, axis=1).astype(bf16)

    r.tiny[...] = jnp.zeros_like(r.tiny)
    for j in range(wide):
        sum_recv(0, j)

        def second_grad(base, value):
            here = pl.ds(base, CHUNK)
            back, gain = norm_back(r.x2[here, :], value, 2)
            grad = r.in_cot[here, :].astype(f32) + back
            r.tiny[2:3, :] = r.tiny[2:3, :] + gain
            r.gx[here, :] = grad
            low = grad.astype(bf16)
            r.gxb[here, :] = low
            r.ga[here, :] = forward_mm(low, weight(CROSS_O)).astype(bf16)

        both_sides(0, j, second_grad)

        def query_piece(base):
            for h in range(heads):
                attend_back_block(
                    False, h, base, r.q2, r.kv2, r.p2, r.gq2, r.ds2.at[h], mem_keys
                )
            return nt(r.gq2[pl.ds(base, CHUNK), :], weight(CROSS_Q))

        sum_send(1, j, query_piece)
    gkv2_sent = []
    for h in range(heads):
        pair_grads(h, r.q2, r.p2, r.ds2.at[h], r.gkv2, mem_keys)
        gkv2_sent.append(start(r.gkv2.at[h, 1 - x], r.gkv2_in.at[h], to_x))
    flip(r.gxb, r.flip, rows)
    grad_into(3, 0, r.flip, r.a2, rows)
    reduce_z(0)

    for j in range(wide):
        sum_recv(1, j)

        def first_grad(base, value):
            here = pl.ds(base, CHUNK)
            back, gain = norm_back(r.x1[here, :], value, 1)
            grad = r.gx[here, :] + back
            r.tiny[1:2, :] = r.tiny[1:2, :] + gain
            r.gx[here, :] = grad
            low = grad.astype(bf16)
            r.gxb[here, :] = low
            r.ga1[here, :] = forward_mm(low, weight(SELF_O)).astype(bf16)

        both_sides(1, j, first_grad)
    for j in range(wide):
        sum_send(3, j, lambda base: nt(r.m[pl.ds(base, CHUNK), :], weight(DOWN)))
    r.ga[...] = r.ga1[...]
    r.strip[...] = jnp.zeros_like(r.strip)
    gkv1_sent = []
    for h in range(heads):

        def self_back_rows(base):
            attend_back_block(True, h, base, r.q1, r.kv1, r.p1, r.gq1, r.ds, keys)

        loop_rows(rows, BLOCK, self_back_rows)
        pair_grads(h, r.q1, r.p1, r.ds, r.gkv1, keys)
        gkv1_sent.append(start(r.gkv1.at[h, 1 - x], r.gkv1_in.at[h], to_x))
    reduce_z(1)
    reduce_z(2)
    tiles = keys // BLOCK
    row = lax.broadcasted_iota(jnp.int32, (BLOCK, BLOCK), 0)
    col = lax.broadcasted_iota(jnp.int32, (BLOCK, BLOCK), 1)
    for h in range(heads):
        own = r.strip[h, :, (tiles - 1) * BLOCK : tiles * BLOCK]
        prior = r.strip[h, :, (tiles - 2) * BLOCK : (tiles - 1) * BLOCK]
        far = jnp.where(row < col, 0.0, prior)
        for j in range(tiles - 2):
            far = far + r.strip[h, :, j * BLOCK : (j + 1) * BLOCK]
        r.tiny[3 + h : 4 + h, :BLOCK] = fold_diagonals(own + jnp.where(row < col, prior, 0.0))
        r.tiny[3 + h : 4 + h, BLOCK : 2 * BLOCK] = jnp.sum(far, axis=0, keepdims=True)
    flip(r.h2, r.flip, rows)
    grad_into(3, width, r.flip, r.gq2, rows)
    flip(r.gxb, r.flip, rows)
    grad_into(5, 0, r.flip, r.a1, rows)
    for c in gkv1_sent:
        c.wait_recv()
    pairs_sum(r.gkv1, r.gkv1_in, r.gkv1_sum)

    def input_piece(base):
        here = pl.ds(base, CHUNK)
        return (
            nt(r.gq1[here, :], weight(SELF_Q))
            + nt(r.gkv1_sum[here, :width], weight(SELF_K))
            + nt(r.gkv1_sum[here, width:], weight(SELF_V))
        )

    for j in range(wide):
        sum_send(0, j, input_piece)
    flip(r.h1, r.flip, rows)
    grad_into(6, 0, r.flip, r.gkv1_sum, rows)
    reduce_x(6)
    grad_into(5, width, r.flip, r.gq1, rows)
    reduce_x(5)
    reduce_x(3)
    for c in gkv2_sent:
        c.wait_recv()
    pairs_sum(r.gkv2, r.gkv2_in, r.gkv2_sum)

    def memory_piece(base):
        here = pl.ds(base, CHUNK)
        return nt(r.gkv2_sum[here, :width], weight(CROSS_K)) + nt(
            r.gkv2_sum[here, width:], weight(CROSS_V)
        )

    for j in range(slim):
        sum_send(2, j, memory_piece)
    flip(r.in_mem, r.flip, mem_count)
    grad_into(4, 0, r.flip, r.gkv2_sum, mem_count)
    reduce_x(4)
    for j in range(wide):
        sum_recv(3, j)

        def output_rows(base, value):
            here = pl.ds(base, CHUNK)
            r.dec[here, :] = (r.x2[here, :] + value).astype(bf16)

        both_sides(3, j, output_rows)
    leave(r.dec, r.o_dec)
    for g in (0, 1, 2):
        reduce_f(g)

    def tail():
        reduce_z(6)
        reduce_z(5)

    for j in range(wide):
        sum_recv(0, j, tail if j == wide - 1 else None)

        def input_grad(base, value):
            here = pl.ds(base, CHUNK)
            back, gain = norm_back(r.in_dec[here, :].astype(f32), value, 0)
            r.tiny[0:1, :] = r.tiny[0:1, :] + gain
            r.gx[here, :] = r.gx[here, :] + back

        both_sides(0, j, input_grad)
    slot = x * SHARDS + z
    r.tiny_all[slot] = r.tiny[...]
    tiny_sent = [
        start(r.tiny, r.tiny_all.at[slot], p) for p in [to_x] + partners[:3] + others
    ]
    leave(r.gx, r.o_input)
    reduce_z(3)
    reduce_z(4)
    for j in range(slim):
        sum_recv(2, j)
    leave(r.p_res[2], r.o_mem)
    for g in (6, 5, 3, 4):
        reduce_f(g)
    for c in tiny_sent:
        c.wait_recv()
    total = r.tiny_all[0]
    for n in range(1, 2 * SHARDS):
        total = total + r.tiny_all[n]
    r.tiny_sum[...] = total
    leave(r.tiny_sum, r.o_tiny)
    for g in range(7):
        reduce_o(g)
    for c in unsent:
        c.wait_send()
    for c in leaving:
        c.wait()


def output_kernel(trees, *refs):
    found, at = {}, 0
    for tree in trees:
        found.update(tree.unflatten(refs[at : at + tree.num_leaves]))
        at += tree.num_leaves
    r = types.SimpleNamespace(**found)
    z = lax.axis_index(SHARD)
    r.out_dec[...] = r.o_dec[...]
    r.out_input[...] = r.o_input[...]
    r.out_mem[...] = r.o_mem[...].reshape(r.out_mem.shape).astype(f32)
    for g, group in enumerate(GROUPS):
        at = 0
        for name in group:
            out = r.out_grad[name]
            cols = out.shape[1]
            out[...] = r.o_fb[g][:, :, at : at + cols].reshape(out.shape).astype(f32)
            at += cols
    total = r.o_tiny[...]
    part = r.out_gain[0].shape[1]
    for k in range(3):
        piece = jnp.zeros((1, part), f32)
        for n in range(SHARDS):
            piece = jnp.where(z == n, total[k : k + 1, n * part : (n + 1) * part], piece)
        r.out_gain[k][...] = piece
    lanes = r.in_lanes[...]
    bucket = lax.broadcasted_iota(jnp.int32, (BUCKETS, 1), 0)
    share, heads = r.out_table.shape
    columns = []
    for h in range(heads):
        near = jnp.sum(lanes * total[3 + h : 4 + h, :BLOCK], axis=1, keepdims=True)
        far = jnp.sum(total[3 + h : 4 + h, BLOCK : 2 * BLOCK], axis=1, keepdims=True)
        columns.append(near + jnp.where(bucket == BUCKETS - 1, far, 0.0))
    r.table[...] = jnp.concatenate(columns, axis=1)
    r.out_table[...] = r.table[pl.ds(pl.multiple_of(z * share, share), share), :]


def local_fast(
    dec_in, memory, dec_segments, mem_segments, gain_self, gain_cross, gain_ffn,
    self_q, self_k, self_v, self_o, cross_q, cross_k, cross_v, cross_o,
    ffn_gate, ffn_up, ffn_down, bias_table, cotangent,
):
    rows, dim = dec_in.shape[1:]
    mem = memory.shape[1]
    width, hidden = self_q.shape[1], ffn_gate.shape[1]
    heads = width // HEAD_DIM
    part = gain_self.shape[0]
    share = bias_table.shape[0]
    keys, mem_keys = 2 * rows, 2 * mem
    half = dim // SHARDS // 2
    line = lax.broadcasted_iota(jnp.int32, (16, part), 0)
    small = jnp.pad(bias_table, ((8, 0), (0, part - heads)))
    for k, gain in enumerate((gain_self, gain_cross, gain_ffn)):
        small = jnp.where(line == k, gain[None, :], small)
    weights = [
        self_q, self_k, self_v, self_o, cross_q, cross_k, cross_v, cross_o,
        ffn_gate, ffn_up, ffn_down,
    ]
    widths = [w.shape[1] for w in weights]
    joined = [sum(widths[k] for k in group) for group in GROUPS]
    chunks = [n // 2 // CHUNK for n in (rows, rows, mem, rows)]
    near = dict(
        in_dec=dec_in[0], in_mem=memory[0], in_seg=dec_segments, in_mseg=mem_segments,
        in_lanes=jnp.asarray(lane_buckets()), in_cot=cotangent[0],
    )
    far = dict(in_small=small, part=weights)

    def out(shape, kind):
        return jax.ShapeDtypeStruct(shape, kind)

    outs = dict(
        out_dec=out((rows, dim), bf16), out_input=out((rows, dim), f32),
        out_mem=out((mem, dim), f32), out_gain=[out((1, part), f32)] * 3,
        out_grad=[out((part, c), f32) for c in widths], out_table=out((share, heads), f32),
    )
    passed = dict(
        o_dec=out((rows, dim), bf16), o_input=out((rows, dim), f32),
        o_mem=out((2, chunks[2], CHUNK, dim), bf16), o_tiny=out((8, dim), f32),
        o_fb=[out((2, half, c), bf16) for c in joined],
    )
    vmem = pltpu.VMEM
    held = dict(
        full=[vmem((SHARDS, 2, half, c), bf16) for c in widths],
        small=vmem((SHARDS, 16, part), bf16), seg=vmem((1, keys), f32),
        mseg=vmem((1, mem_keys), f32), seg_col=vmem((rows, 8), f32), gains=vmem((8, dim), f32),
        near=vmem((8, BLOCK), f32), far=vmem((8, BLOCK), f32),
        strip=vmem((heads, BLOCK, (2 * (keys // BLOCK) - 1) * BLOCK), f32),
        h1=vmem((rows, dim), bf16), h2=vmem((rows, dim), bf16), h3=vmem((rows, dim), bf16),
        x1=vmem((rows, dim), f32), x2=vmem((rows, dim), f32),
        q1=vmem((rows, width), bf16), q2=vmem((rows, width), bf16),
        kv1=vmem((heads, 2, rows, 2 * HEAD_DIM), bf16), kv2=vmem((heads, 2, mem, 2 * HEAD_DIM), bf16),
        p1=vmem((heads, rows, keys), bf16), p2=vmem((heads, rows, mem_keys), bf16),
        a1=vmem((rows, width), bf16), a2=vmem((rows, width), bf16),
        gm=vmem((rows, hidden), f32), m=vmem((rows, hidden), bf16),
        ggate=vmem((rows, hidden), bf16), gup=vmem((rows, hidden), bf16),
        flip=vmem((dim, rows), bf16), gx=vmem((rows, dim), f32), gxb=vmem((rows, dim), bf16),
        ga=vmem((rows, width), bf16), ds=vmem((rows, keys), bf16),
        gkv_t=vmem((2 * HEAD_DIM, keys), f32), ds2=vmem((heads, rows, mem_keys), bf16),
        ga1=vmem((rows, width), bf16), dec=vmem((rows, dim), bf16), gq1=vmem((rows, width), bf16),
        gq2=vmem((rows, width), bf16), gkv1=vmem((heads, 2, rows, 2 * HEAD_DIM), bf16),
        gkv2=vmem((heads, 2, mem, 2 * HEAD_DIM), bf16), gkv1_in=vmem((heads, rows, 2 * HEAD_DIM), bf16),
        gkv2_in=vmem((heads, mem, 2 * HEAD_DIM), bf16), gkv1_sum=vmem((rows, 2 * width), bf16),
        gkv2_sum=vmem((mem, 2 * width), bf16), tiny=vmem((8, dim), f32),
        tiny_all=vmem((2 * SHARDS, 8, dim), f32), tiny_sum=vmem((8, dim), f32),
        ps_out=[vmem((n, CHUNK, dim), bf16) for n in chunks],
        ps_in=[vmem((n, CHUNK, dim), bf16) for n in chunks],
        py_out=[vmem((n, CHUNK, dim), bf16) for n in chunks],
        py_in=[vmem((n, CHUNK, dim), bf16) for n in chunks],
        p_res=[vmem((2, n, CHUNK, dim), bf16) for n in chunks],
        stage=[vmem((SHARDS, 2, half, c), bf16) for c in joined],
        xr=[vmem((SHARDS, half, c), bf16) for c in joined],
        zr=[vmem((3, half, c), bf16) for c in joined],
        fb=[vmem((2, half, c), bf16) for c in joined],
        send_sem=pltpu.SemaphoreType.DMA((192,)), recv_sem=pltpu.SemaphoreType.DMA((192,)),
        own_sem=pltpu.SemaphoreType.DMA((40,)),
    )
    in_vmem = pl.BlockSpec(memory_space=pltpu.VMEM)
    anywhere = pl.BlockSpec(memory_space=pl.ANY)
    flat = [jax.tree.flatten(v) for v in (near, far, passed, held)]
    results = pl.pallas_call(
        functools.partial(
            layer_kernel, (rows, mem, dim, width, heads), [tree for _, tree in flat]
        ),
        out_shape=tuple(flat[2][0]),
        in_specs=[in_vmem] * len(flat[0][0]) + [anywhere] * len(flat[1][0]),
        out_specs=tuple([anywhere] * len(flat[2][0])),
        scratch_shapes=flat[3][0],
        compiler_params=pltpu.CompilerParams(
            collective_id=0, has_side_effects=True, vmem_limit_bytes=67043328
        ),
        name="layer",
    )(*flat[0][0], *flat[1][0])
    ready = dict(flat[2][1].unflatten(results), in_lanes=near["in_lanes"])
    table = dict(table=vmem((BUCKETS, heads), f32))
    flat = [jax.tree.flatten(v) for v in (ready, outs, table)]
    results = pl.pallas_call(
        functools.partial(output_kernel, [tree for _, tree in flat]),
        out_shape=tuple(flat[1][0]),
        in_specs=[in_vmem] * len(flat[0][0]),
        out_specs=tuple([in_vmem] * len(flat[1][0])),
        scratch_shapes=flat[2][0],
        compiler_params=pltpu.CompilerParams(vmem_limit_bytes=48 * 1024 * 1024),
        name="outputs",
    )(*flat[0][0])
    flat = flat[:1] + [None] + flat[1:2]
    got = types.SimpleNamespace(**flat[2][1].unflatten(results))
    return (
        got.out_dec[None], got.out_input[None], got.out_mem[None],
        *[g[0] for g in got.out_gain], *got.out_grad, got.out_table,
    )


def shard_part(parts):
    return tuple(
        lax.psum_scatter(p.astype(jnp.bfloat16), SHARD, scatter_dimension=0, tiled=True).astype(
            jnp.float32
        )
        for p in parts
    )


def context_total(parts):
    return tuple(lax.psum(p.astype(jnp.bfloat16), CTX).astype(jnp.float32) for p in parts)


def local(
    dec_in,
    memory,
    dec_segments,
    mem_segments,
    gain_self,
    gain_cross,
    gain_ffn,
    self_q,
    self_k,
    self_v,
    self_o,
    cross_q,
    cross_k,
    cross_v,
    cross_o,
    ffn_gate,
    ffn_up,
    ffn_down,
    bias_table,
    cotangent,
):
    gathered = (
        lax.all_gather(gain_self, SHARD, axis=0, tiled=True),
        lax.all_gather(gain_cross, SHARD, axis=0, tiled=True),
        lax.all_gather(gain_ffn, SHARD, axis=0, tiled=True),
        lax.all_gather(self_q, SHARD, axis=0, tiled=True),
        lax.all_gather(self_k, SHARD, axis=0, tiled=True),
        lax.all_gather(self_v, SHARD, axis=0, tiled=True),
        lax.all_gather(self_o, SHARD, axis=0, tiled=True),
        lax.all_gather(cross_q, SHARD, axis=0, tiled=True),
        lax.all_gather(cross_k, SHARD, axis=0, tiled=True),
        lax.all_gather(cross_v, SHARD, axis=0, tiled=True),
        lax.all_gather(cross_o, SHARD, axis=0, tiled=True),
        lax.all_gather(ffn_gate, SHARD, axis=0, tiled=True),
        lax.all_gather(ffn_up, SHARD, axis=0, tiled=True),
        lax.all_gather(ffn_down, SHARD, axis=0, tiled=True),
        lax.all_gather(bias_table, SHARD, axis=0, tiled=True),
    )
    (
        norm_one,
        norm_two,
        norm_three,
        query_self,
        key_self,
        value_self,
        out_self,
        query_cross,
        key_cross,
        value_cross,
        out_cross,
        gate_full,
        up_full,
        down_full,
        table_full,
    ) = gathered
    gain_one = norm_one.astype(jnp.float32)
    gain_two = norm_two.astype(jnp.float32)
    gain_three = norm_three.astype(jnp.float32)
    table = table_full.astype(jnp.float32)
    width = query_self.shape[1]
    hidden_in = dec_in[0].astype(jnp.float32)
    mem_rows = memory[0]
    grad_out = cotangent[0].astype(jnp.float32)
    count_rows = hidden_in.shape[0]
    place = lax.axis_index(CTX)
    dec_ids = dec_segments[0]
    mem_ids = mem_segments[0]
    query_ids = lax.dynamic_slice_in_dim(dec_ids, place * count_rows, count_rows)
    query_pos = place * count_rows + jnp.arange(count_rows, dtype=jnp.int32)
    key_pos = jnp.arange(dec_ids.shape[0], dtype=jnp.int32)
    mem_pos = jnp.arange(mem_ids.shape[0], dtype=jnp.int32)
    normed_one = rms_norm(hidden_in, gain_one).astype(jnp.bfloat16)
    query_one = forward_mm(normed_one, query_self).astype(jnp.bfloat16)
    pairs_own = jnp.concatenate(
        [forward_mm(normed_one, key_self), forward_mm(normed_one, value_self)], axis=1
    ).astype(jnp.bfloat16)
    pairs_one = lax.all_gather(pairs_own, CTX, axis=0, tiled=True)
    mixed_one, lse_one = attend(
        query_one, pairs_one, key_pos, dec_ids, query_pos, query_ids, table, True
    )
    context_one = mixed_one.astype(jnp.bfloat16)
    first = hidden_in + lax.psum(
        backward_mm(context_one, out_self).astype(jnp.bfloat16), TENSOR
    ).astype(jnp.float32)
    normed_two = rms_norm(first, gain_two).astype(jnp.bfloat16)
    query_two = forward_mm(normed_two, query_cross).astype(jnp.bfloat16)
    pairs_mem = jnp.concatenate(
        [forward_mm(mem_rows, key_cross), forward_mm(mem_rows, value_cross)], axis=1
    ).astype(jnp.bfloat16)
    pairs_two = lax.all_gather(pairs_mem, CTX, axis=0, tiled=True)
    mixed_two, lse_two = attend(
        query_two, pairs_two, mem_pos, mem_ids, query_pos, query_ids, table, False
    )
    context_two = mixed_two.astype(jnp.bfloat16)
    second = first + lax.psum(
        backward_mm(context_two, out_cross).astype(jnp.bfloat16), TENSOR
    ).astype(jnp.float32)
    normed_three = rms_norm(second, gain_three).astype(jnp.bfloat16)
    gate = forward_mm(normed_three, gate_full)
    upper = forward_mm(normed_three, up_full)
    activated = gated(gate, upper).astype(jnp.bfloat16)
    result = second + lax.psum(
        backward_mm(activated, down_full).astype(jnp.bfloat16), TENSOR
    ).astype(jnp.float32)
    dec_out = result.astype(jnp.bfloat16)
    grad_low = cotangent[0]
    grad_down_w = weight_mm(grad_low, activated)
    grad_hidden = forward_mm(grad_low, down_full)
    _, pull_gate = jax.vjp(gated, gate, upper)
    grad_gate, grad_upper = pull_gate(grad_hidden)
    gate_low = grad_gate.astype(jnp.bfloat16)
    upper_low = grad_upper.astype(jnp.bfloat16)
    grad_gate_w = weight_mm(normed_three, gate_low)
    grad_up_w = weight_mm(normed_three, upper_low)
    grad_normed_three = backward_mm(gate_low, gate_full) + backward_mm(upper_low, up_full)
    grad_normed_three = lax.psum(grad_normed_three.astype(jnp.bfloat16), TENSOR).astype(
        jnp.float32
    )
    _, pull_three = jax.vjp(rms_norm, second, gain_three)
    grad_second, grad_gain_three = pull_three(grad_normed_three)
    grad_second = grad_out + grad_second
    second_low = grad_second.astype(jnp.bfloat16)
    grad_out_cross = weight_mm(second_low, context_two)
    grad_context_two = forward_mm(second_low, out_cross).astype(jnp.bfloat16)
    grad_query_two, grad_pairs_two, _ = attend_back(
        query_two,
        pairs_two,
        mem_pos,
        mem_ids,
        query_pos,
        query_ids,
        table,
        False,
        mixed_two,
        lse_two,
        grad_context_two,
    )
    pairs_grad_mem = lax.psum_scatter(
        grad_pairs_two.astype(jnp.bfloat16), CTX, scatter_dimension=0, tiled=True
    )
    query_two_low = grad_query_two.astype(jnp.bfloat16)
    grad_mem_keys = pairs_grad_mem[:, :width]
    grad_mem_values = pairs_grad_mem[:, width:]
    grad_query_cross = weight_mm(normed_two, query_two_low)
    grad_key_cross = weight_mm(mem_rows, grad_mem_keys)
    grad_value_cross = weight_mm(mem_rows, grad_mem_values)
    grad_normed_two = backward_mm(query_two_low, query_cross)
    grad_memory = backward_mm(grad_mem_keys, key_cross) + backward_mm(grad_mem_values, value_cross)
    grad_normed_two, grad_memory = (
        lax.psum(grad_normed_two.astype(jnp.bfloat16), TENSOR).astype(jnp.float32),
        lax.psum(grad_memory.astype(jnp.bfloat16), TENSOR).astype(jnp.float32),
    )
    _, pull_two = jax.vjp(rms_norm, first, gain_two)
    grad_first, grad_gain_two = pull_two(grad_normed_two)
    grad_first = grad_second + grad_first
    first_low = grad_first.astype(jnp.bfloat16)
    grad_out_self = weight_mm(first_low, context_one)
    grad_context_one = forward_mm(first_low, out_self).astype(jnp.bfloat16)
    grad_query_one, grad_pairs_one, grad_table = attend_back(
        query_one,
        pairs_one,
        key_pos,
        dec_ids,
        query_pos,
        query_ids,
        table,
        True,
        mixed_one,
        lse_one,
        grad_context_one,
    )
    pairs_grad_own = lax.psum_scatter(
        grad_pairs_one.astype(jnp.bfloat16), CTX, scatter_dimension=0, tiled=True
    )
    query_one_low = grad_query_one.astype(jnp.bfloat16)
    grad_keys_own = pairs_grad_own[:, :width]
    grad_values_own = pairs_grad_own[:, width:]
    grad_query_self = weight_mm(normed_one, query_one_low)
    grad_key_self = weight_mm(normed_one, grad_keys_own)
    grad_value_self = weight_mm(normed_one, grad_values_own)
    grad_normed_one = (
        backward_mm(query_one_low, query_self)
        + backward_mm(grad_keys_own, key_self)
        + backward_mm(grad_values_own, value_self)
    )
    grad_normed_one = lax.psum(grad_normed_one.astype(jnp.bfloat16), TENSOR).astype(jnp.float32)
    _, pull_one = jax.vjp(rms_norm, hidden_in, gain_one)
    grad_input, grad_gain_one = pull_one(grad_normed_one)
    grad_input = grad_first + grad_input
    local_grads = (
        grad_gain_one,
        grad_gain_two,
        grad_gain_three,
        grad_query_self,
        grad_key_self,
        grad_value_self,
        grad_out_self,
        grad_query_cross,
        grad_key_cross,
        grad_value_cross,
        grad_out_cross,
        grad_gate_w,
        grad_up_w,
        grad_down_w,
        grad_table,
    )
    summed = shard_part(context_total(local_grads))
    return (
        dec_out[None],
        grad_input[None],
        grad_memory[None],
        summed[0],
        summed[1],
        summed[2],
        summed[3],
        summed[4],
        summed[5],
        summed[6],
        summed[7],
        summed[8],
        summed[9],
        summed[10],
        summed[11],
        summed[12],
        summed[13],
        summed[14],
    )


def solution(mesh):
    in_specs = (
        P(SHARD, CTX, None),
        P(SHARD, CTX, None),
        P(SHARD, None),
        P(SHARD, None),
        P(SHARD),
        P(SHARD),
        P(SHARD),
        P(SHARD, TENSOR),
        P(SHARD, TENSOR),
        P(SHARD, TENSOR),
        P(SHARD, TENSOR),
        P(SHARD, TENSOR),
        P(SHARD, TENSOR),
        P(SHARD, TENSOR),
        P(SHARD, TENSOR),
        P(SHARD, TENSOR),
        P(SHARD, TENSOR),
        P(SHARD, TENSOR),
        P(SHARD, TENSOR),
        P(SHARD, CTX, None),
    )
    out_specs = (
        P(SHARD, CTX, None),
        P(SHARD, CTX, None),
        P(SHARD, CTX, None),
        P(SHARD),
        P(SHARD),
        P(SHARD),
        P(SHARD, TENSOR),
        P(SHARD, TENSOR),
        P(SHARD, TENSOR),
        P(SHARD, TENSOR),
        P(SHARD, TENSOR),
        P(SHARD, TENSOR),
        P(SHARD, TENSOR),
        P(SHARD, TENSOR),
        P(SHARD, TENSOR),
        P(SHARD, TENSOR),
        P(SHARD, TENSOR),
        P(SHARD, TENSOR),
    )
    fast = (mesh.shape[SHARD], mesh.shape[CTX], mesh.shape[TENSOR]) == (SHARDS, 2, 4)
    body = local_fast if fast else local
    return jax.shard_map(body, mesh=mesh, in_specs=in_specs, out_specs=out_specs, check_vma=False)
```

```python
import functools
import types

import jax
import jax.numpy as jnp
import numpy as np
from jax import lax
from jax.experimental import pallas as pl
from jax.experimental.pallas import tpu as pltpu
from jax.sharding import PartitionSpec as P

SHARD, CTX, TENSOR = "shard", "ctx", "tensor"
HEAD_DIM = 64
BUCKETS = 32
MAX_DIST = 128


highest = lax.Precision.HIGHEST
epsilon = 1e-06
negative = -1e30


def thresholds():
    exact_part = BUCKETS // 2
    small_part = np.arange(1, exact_part + 1)
    steps_up = np.arange(exact_part + 1, BUCKETS)
    large_part = np.ceil(
        exact_part * (MAX_DIST / exact_part) ** ((steps_up - exact_part) / (BUCKETS - exact_part))
    )
    return np.concatenate([small_part, large_part]).astype(np.int32)


def bucket_of(distance):
    limits = jnp.asarray(thresholds())
    return jnp.sum((distance[..., None] >= limits).astype(jnp.int32), axis=-1)


def rms_norm(values, gain):
    return values * lax.rsqrt(jnp.mean(values * values, axis=-1, keepdims=True) + epsilon) * gain


def gated(gate, upper):
    return jax.nn.gelu(gate, approximate=True) * upper


def forward_mm(left, right):
    return jnp.dot(left, right, preferred_element_type=jnp.float32)


def backward_mm(left, right):
    return lax.dot_general(
        left, right, (((1,), (1,)), ((), ())), preferred_element_type=jnp.float32
    )


def weight_mm(left, right):
    return lax.dot_general(
        left, right, (((0,), (0,)), ((), ())), preferred_element_type=jnp.float32
    )


def toeplitz(vector, count_rows, count_cols):
    heads = vector.shape[0]
    span = count_rows + count_cols - 1
    tiled = jnp.pad(jnp.tile(vector, (1, count_rows)), ((0, 0), (0, count_rows)))
    grid = tiled.reshape(heads, count_rows, span + 1)[:, :, :count_cols]
    return grid[:, :, ::-1]


def diagonal_sums(block):
    heads, count_rows, count_cols = block.shape
    span = count_rows + count_cols - 1
    flipped = jnp.pad(block[:, :, ::-1], ((0, 0), (0, 0), (0, count_rows)))
    flat = flipped.reshape(heads, count_rows * (span + 1))[:, : count_rows * span]
    return jnp.sum(flat.reshape(heads, count_rows, span), axis=1)


def bias_block(table, offset, count_rows, count_cols):
    span = count_rows + count_cols - 1
    distance = jnp.arange(span, dtype=jnp.int32) - (count_cols - 1) + offset
    onehot = (
        bucket_of(distance)[:, None] == jnp.arange(table.shape[0], dtype=jnp.int32)[None, :]
    ).astype(jnp.float32)
    column = jnp.dot(onehot, table, precision=highest)
    return (toeplitz(column.T, count_rows, count_cols), onehot)


def key_blocks(pairs, key_pos, key_seg):
    length = pairs.shape[0]
    width = min(512, length)
    count = length // width
    heads = pairs.shape[1] // (2 * HEAD_DIM)
    blocks = pairs.reshape(count, width, 2, heads, HEAD_DIM)
    starts = jnp.arange(count, dtype=jnp.int32) * width
    return (blocks, key_pos.reshape(count, width), key_seg.reshape(count, width), starts)


def scores_of(query, block, block_pos, block_seg, start, query_pos, query_seg, table, causal):
    scores = jnp.einsum("qhd,khd->hqk", query, block[:, 0], preferred_element_type=jnp.float32)
    mask = query_seg[:, None] == block_seg[None, :]
    onehot = None
    if causal:
        mask = mask & (query_pos[:, None] >= block_pos[None, :])
        bias, onehot = bias_block(table, query_pos[0] - start, query.shape[0], block.shape[0])
        scores = scores + bias
    return (jnp.where(mask[None], scores, negative), mask, onehot)


def attend(query, pairs, key_pos, key_seg, query_pos, query_seg, table, causal):
    count_rows = query.shape[0]
    heads = query.shape[1] // HEAD_DIM
    query = query.reshape(count_rows, heads, HEAD_DIM)
    blocks = key_blocks(pairs, key_pos, key_seg)

    def stats(carry, item):
        peak, total = carry
        block, block_pos, block_seg, start = item
        scores, mask, _ = scores_of(
            query, block, block_pos, block_seg, start, query_pos, query_seg, table, causal
        )
        fresh = jnp.maximum(peak, jnp.max(scores, axis=-1))
        weights = jnp.where(mask[None], jnp.exp(scores - fresh[..., None]), 0.0)
        total = total * jnp.exp(peak - fresh) + jnp.sum(weights, axis=-1)
        return ((fresh, total), None)

    start_peak = jnp.full((heads, count_rows), negative, jnp.float32)
    start_total = jnp.zeros((heads, count_rows), jnp.float32)
    (peak, total), _ = lax.scan(stats, (start_peak, start_total), blocks)
    log_total = peak + jnp.log(total)

    def collect(accum, item):
        block, block_pos, block_seg, start = item
        scores, mask, _ = scores_of(
            query, block, block_pos, block_seg, start, query_pos, query_seg, table, causal
        )
        probs = jnp.where(mask[None], jnp.exp(scores - log_total[..., None]), 0.0).astype(
            jnp.bfloat16
        )
        accum = accum + jnp.einsum(
            "hqk,khd->qhd", probs, block[:, 1], preferred_element_type=jnp.float32
        )
        return (accum, None)

    mixed, _ = lax.scan(collect, jnp.zeros((count_rows, heads, HEAD_DIM), jnp.float32), blocks)
    return (mixed.reshape(count_rows, heads * HEAD_DIM), log_total)


def correction_of(grad_mixed, mixed):
    count_rows = mixed.shape[0]
    heads = mixed.shape[1] // HEAD_DIM
    return jnp.einsum(
        "qhd,qhd->hq",
        grad_mixed.reshape(count_rows, heads, HEAD_DIM).astype(jnp.float32),
        mixed.reshape(count_rows, heads, HEAD_DIM),
    )


def attend_back(
    query,
    pairs,
    key_pos,
    key_seg,
    query_pos,
    query_seg,
    table,
    causal,
    mixed,
    log_total,
    grad_mixed,
):
    count_rows = query.shape[0]
    heads = query.shape[1] // HEAD_DIM
    query = query.reshape(count_rows, heads, HEAD_DIM)
    grad_heads = grad_mixed.reshape(count_rows, heads, HEAD_DIM)
    correction = correction_of(grad_mixed, mixed)
    blocks = key_blocks(pairs, key_pos, key_seg)

    def step(carry, item):
        grad_query, grad_table = carry
        block, block_pos, block_seg, start = item
        scores, mask, onehot = scores_of(
            query, block, block_pos, block_seg, start, query_pos, query_seg, table, causal
        )
        probs = jnp.where(mask[None], jnp.exp(scores - log_total[..., None]), 0.0)
        grad_probs = jnp.einsum(
            "qhd,khd->hqk", grad_heads, block[:, 1], preferred_element_type=jnp.float32
        )
        grad_scores = probs * (grad_probs - correction[..., None])
        if causal:
            grad_table = grad_table + jnp.dot(
                onehot.T, diagonal_sums(grad_scores).T, precision=highest
            )
        low_scores = grad_scores.astype(jnp.bfloat16)
        grad_query = grad_query + jnp.einsum(
            "hqk,khd->qhd", low_scores, block[:, 0], preferred_element_type=jnp.float32
        )
        stacked = None
        grad_values = jnp.einsum(
            "hqk,qhd->khd",
            probs.astype(jnp.bfloat16),
            grad_heads,
            preferred_element_type=jnp.float32,
        )
        grad_keys = jnp.einsum(
            "hqk,qhd->khd", low_scores, query, preferred_element_type=jnp.float32
        )
        width = block.shape[0]
        stacked = jnp.concatenate(
            [
                grad_keys.reshape(width, heads * HEAD_DIM),
                grad_values.reshape(width, heads * HEAD_DIM),
            ],
            axis=1,
        )
        return ((grad_query, grad_table), stacked)

    start = (
        jnp.zeros((count_rows, heads, HEAD_DIM), jnp.float32),
        jnp.zeros(table.shape, jnp.float32),
    )
    (grad_query, grad_table), grad_pairs = lax.scan(step, start, blocks)
    grad_pairs = grad_pairs.reshape(pairs.shape[0], pairs.shape[1])
    return (grad_query.reshape(count_rows, heads * HEAD_DIM), grad_pairs, grad_table)


BLOCK = 128


def nt(left, right):
    return lax.dot_general(
        left, right, (((1,), (1,)), ((), ())), preferred_element_type=jnp.float32
    )


def tn(left, right):
    return lax.dot_general(
        left, right, (((0,), (0,)), ((), ())), preferred_element_type=jnp.float32
    )


def lane_buckets():
    lane = np.arange(BLOCK)
    distance = (BLOCK - lane) % BLOCK
    bucket = (distance[:, None] >= thresholds()[None, :]).sum(axis=1)
    return (bucket[None, :] == np.arange(BUCKETS)[:, None]).astype(np.float32)


def build_strip(near_ref, far_ref, strip_ref, tiles, heads):
    row = lax.broadcasted_iota(jnp.int32, (BLOCK, BLOCK), 0)
    col = lax.broadcasted_iota(jnp.int32, (BLOCK, BLOCK), 1)
    for h in range(heads):
        near = jnp.broadcast_to(near_ref[h : h + 1, :], (BLOCK, BLOCK))
        near = pltpu.roll(near, 0, 1, stride=1, stride_axis=0)
        far = jnp.broadcast_to(far_ref[h : h + 1, :], (BLOCK, BLOCK))
        for m in range(tiles - 2):
            strip_ref[h, :, m * BLOCK : (m + 1) * BLOCK] = far
        strip_ref[h, :, (tiles - 2) * BLOCK : (tiles - 1) * BLOCK] = jnp.where(
            row < col, near, far
        )
        strip_ref[h, :, (tiles - 1) * BLOCK : tiles * BLOCK] = near
        strip_ref[h, :, tiles * BLOCK :] = jnp.zeros((BLOCK, (tiles - 1) * BLOCK), jnp.float32)


def fold_diagonals(tile):
    rows = BLOCK
    while rows > 8:
        rows //= 2
        tile = tile[:rows] + pltpu.roll(tile[rows:], BLOCK - rows, 1)
    total = tile[0:1]
    for r in range(1, 8):
        total = total + pltpu.roll(tile[r : r + 1], BLOCK - r, 1)
    return total


SELF_Q, SELF_K, SELF_V, SELF_O, CROSS_Q, CROSS_K, CROSS_V, CROSS_O, GATE, UP, DOWN = range(11)
GROUPS = (
    (DOWN,), (GATE,), (UP,), (CROSS_O, CROSS_Q), (CROSS_K, CROSS_V),
    (SELF_O, SELF_Q), (SELF_K, SELF_V),
)
ORDER = (
    SELF_K, SELF_V, SELF_Q, SELF_O, CROSS_K, CROSS_V, CROSS_Q, CROSS_O, GATE, UP, DOWN,
)
WHOLE = (0, 1)
CHUNK = 128
BIG = 256
SHARDS = 4
MESH = pl.DeviceIdType.MESH
bf16 = jnp.bfloat16
f32 = jnp.float32


def loop_rows(count, block, step):
    def body(i, carry):
        step(pl.multiple_of(i * block, block))
        return carry

    lax.fori_loop(0, count // block, body, 0)


def layer_kernel(shape, trees, *refs):
    found, at = {}, 0
    for tree in trees:
        found.update(tree.unflatten(refs[at : at + tree.num_leaves]))
        at += tree.num_leaves
    r = types.SimpleNamespace(**found)
    rows, mem_count, dim, width, heads = shape
    keys = 2 * rows
    mem_keys = 2 * mem_count
    half = dim // SHARDS // 2
    z = lax.axis_index(SHARD)
    x = lax.axis_index(CTX)
    t = lax.axis_index(TENSOR)
    core = lax.rem(t, 2)
    to_x = {CTX: 1 - x}
    to_core = {TENSOR: t + 1 - 2 * core}
    to_y = {TENSOR: lax.rem(t + 2, 4)}

    def to_z(k):
        return {SHARD: lax.rem(z + k, SHARDS)}

    send_sem, recv_sem = r.send_sem, r.recv_sem
    used = [0]
    unsent = []

    def copy(src, dst, where):
        i = used[0]
        used[0] += 1
        return pltpu.make_async_remote_copy(
            src_ref=src, dst_ref=dst, send_sem=send_sem.at[i], recv_sem=recv_sem.at[i],
            device_id=where, device_id_type=MESH,
        )

    def start(src, dst, where):
        c = copy(src, dst, where)
        c.start()
        unsent.append(c)
        return c

    barrier = pltpu.get_barrier_semaphore()
    others = [dict(to_z(k), ctx=1 - x) for k in (1, 2, 3)]
    partners = [to_z(1), to_z(2), to_z(3), to_x, to_core, to_y] + others
    for p in partners:
        pl.semaphore_signal(barrier, inc=1, device_id=p, device_id_type=MESH)

    own_copies = {}
    for name in ORDER:
        full, part = r.full[name], r.part[name]
        own_copies[name] = []
        for side in range(2):
            c = pltpu.make_async_copy(
                part.at[pl.ds(side * half, half), :], full.at[z, side],
                r.own_sem.at[2 * name + side],
            )
            c.start()
            own_copies[name].append(c)
    small_own = pltpu.make_async_copy(r.in_small, r.small.at[z], r.own_sem.at[22])
    small_own.start()
    leaving = []

    def leave(src, dst):
        c = pltpu.make_async_copy(src, dst, r.own_sem.at[23 + len(leaving)])
        c.start()
        leaving.append(c)

    seg = r.in_seg[...].astype(f32)
    r.seg[...] = seg
    r.mseg[...] = r.in_mseg[...].astype(f32)
    own_seg = r.seg[:, pl.ds(pl.multiple_of(x * rows, BLOCK), rows)]
    r.seg_col[...] = jnp.broadcast_to(own_seg, (8, rows)).T
    pl.semaphore_wait(barrier, len(partners))

    gathers = {}

    def gather_start(name):
        full, part = r.full[name], r.part[name]
        sent = [
            start(part.at[pl.ds(x * half, half), :], full.at[z, x], to_z(k)) for k in (1, 2, 3)
        ]
        gathers[name] = (sent, [])

    def gather_pump(*chosen):
        for name in chosen:
            sent, passed = gathers[name]
            full = r.full[name]
            for k in (1, 2, 3):
                sent[k - 1].wait_recv()
                source = lax.rem(z + SHARDS - k, SHARDS)
                passed.append(start(full.at[source, x], full.at[source, x], to_x))

    def gather_wait(*chosen):
        for name in chosen:
            for c in own_copies[name]:
                c.wait()
            for c in gathers[name][1]:
                c.wait_recv()

    def weight(name):
        ref = r.full[name]
        return ref[...].reshape(dim, ref.shape[-1])

    small_sent = [start(r.in_small, r.small.at[z], to_z(k)) for k in (1, 2, 3)]
    for name in (SELF_K, SELF_V, SELF_Q, SELF_O):
        gather_start(name)

    small_own.wait()
    for c in small_sent:
        c.wait_recv()
    gathered = [r.small[n].astype(f32) for n in range(SHARDS)]
    for k in range(3):
        r.gains[k : k + 1, :] = jnp.concatenate(
            [g[k : k + 1, : dim // SHARDS] for g in gathered], axis=1
        )
    table = jnp.concatenate([g[8:16, :BLOCK] for g in gathered], axis=0)
    near = tn(table.astype(bf16), r.in_lanes[...].astype(bf16))
    r.near[...] = near[:8]
    lane_of = lax.broadcasted_iota(jnp.int32, (8, BLOCK), 1)
    row_of = lax.broadcasted_iota(jnp.int32, (8, BLOCK), 0)
    last = jnp.broadcast_to(table[BUCKETS - 1 : BUCKETS, :], (8, BLOCK))
    last = jnp.sum(jnp.where(lane_of == row_of, last, 0.0), axis=1, keepdims=True)
    r.far[...] = jnp.broadcast_to(last, (8, BLOCK))
    build_strip(r.near, r.far, r.strip, keys // BLOCK, heads)

    def inverse(v):
        return lax.rsqrt(jnp.mean(v * v, axis=1, keepdims=True) + epsilon)

    def norm(v, k):
        return (v * inverse(v) * r.gains[k : k + 1, :]).astype(bf16)

    def input_norm(base):
        here = pl.ds(base, BIG)
        r.h1[here, :] = norm(r.in_dec[here, :].astype(f32), 0)

    loop_rows(rows, BIG, input_norm)

    def head_pairs(dst, here, left, right):
        for h in range(heads):
            lanes = slice(h * HEAD_DIM, (h + 1) * HEAD_DIM)
            dst[h, x, here, :] = jnp.concatenate([left[:, lanes], right[:, lanes]], axis=1).astype(
                bf16
            )

    gather_pump(SELF_K, SELF_V)
    gather_wait(SELF_K, SELF_V)
    gather_pump(SELF_Q)
    for name in (CROSS_K, CROSS_V, CROSS_Q, CROSS_O):
        gather_start(name)

    def project(base):
        here = pl.ds(base, BIG)
        h = r.h1[here, :]
        head_pairs(
            r.kv1, here, forward_mm(h, weight(SELF_K)), forward_mm(h, weight(SELF_V))
        )

    loop_rows(rows, BIG, project)
    kv1_sent = [start(r.kv1.at[h, x], r.kv1.at[h, x], to_x) for h in range(heads)]
    gather_wait(SELF_Q)

    def project_query(base):
        here = pl.ds(base, BIG)
        r.q1[here, :] = forward_mm(r.h1[here, :], weight(SELF_Q)).astype(bf16)

    loop_rows(rows, BIG, project_query)
    gather_pump(SELF_O)
    gather_start(GATE)

    def attend_block(causal, h, base, q, kv, cols, p_ref, a_ref, total):
        tiles = total // BLOCK
        here = pl.ds(base, BLOCK)
        lanes = slice(h * HEAD_DIM, (h + 1) * HEAD_DIM)
        pair = kv[h].reshape(total, 2 * HEAD_DIM)
        mask = r.seg_col[here, 0:1] == cols[...]
        scores = nt(q[here, lanes], pair[:, :HEAD_DIM])
        if causal:
            first = x * rows + base
            row = lax.broadcasted_iota(jnp.int32, (BLOCK, total), 0) + first
            col = lax.broadcasted_iota(jnp.int32, (BLOCK, total), 1)
            mask = mask & (row >= col)
            begin = pl.multiple_of((tiles - 1) * BLOCK - first, BLOCK)
            scores = scores + r.strip[h, :, pl.ds(begin, total)]
        scores = jnp.where(mask, scores, negative)
        peak = jnp.max(scores, axis=1, keepdims=True)
        weights = jnp.exp(scores - peak)
        probs = (weights / jnp.sum(weights, axis=1, keepdims=True)).astype(bf16)
        p_ref[h, here, :] = probs
        a_ref[here, lanes] = forward_mm(probs, pair[:, HEAD_DIM:]).astype(bf16)

    sums = {}

    def sides(key, j):
        n = r.p_res[key].shape[1]
        return [
            pl.multiple_of(((1 - core) * n + j) * CHUNK, CHUNK),
            pl.multiple_of((core * n + j) * CHUNK, CHUNK),
        ]

    def sum_send(key, j, piece):
        state = sums.setdefault((key, j), {})
        for c in state.values():
            c.wait_send()
            unsent[:] = [u for u in unsent if u is not c]
        other, own = sides(key, j)
        r.ps_out[key][j] = piece(other).astype(bf16)
        state[0] = start(r.ps_out[key].at[j], r.ps_in[key].at[j], to_core)
        mine = piece(own)
        state[0].wait_recv()
        r.py_out[key][j] = (mine + r.ps_in[key][j].astype(f32)).astype(bf16)
        state[1] = start(r.py_out[key].at[j], r.py_in[key].at[j], to_y)

    def sum_send_all(key, piece):
        chunks = range(r.p_res[key].shape[1])
        for j in chunks:
            state = sums.setdefault((key, j), {})
            for c in state.values():
                c.wait_send()
                unsent[:] = [u for u in unsent if u is not c]
            r.ps_out[key][j] = piece(sides(key, j)[0]).astype(bf16)
            state[0] = start(r.ps_out[key].at[j], r.ps_in[key].at[j], to_core)
        mine = [piece(sides(key, j)[1]) for j in chunks]
        for j in chunks:
            state = sums[(key, j)]
            state[0].wait_recv()
            r.py_out[key][j] = (mine[j] + r.ps_in[key][j].astype(f32)).astype(bf16)
            state[1] = start(r.py_out[key].at[j], r.py_in[key].at[j], to_y)

    def sum_recv(key, j, between=None):
        state = sums[(key, j)]
        res = r.p_res[key]
        state[1].wait_recv()
        res[core, j] = (r.py_out[key][j].astype(f32) + r.py_in[key][j].astype(f32)).astype(bf16)
        state[2] = start(res.at[core, j], res.at[core, j], to_core)
        if between is not None:
            between()
        state[2].wait_recv()

    def both_sides(key, j, step):
        other, own = sides(key, j)
        step(other, r.p_res[key][1 - core, j].astype(f32))
        step(own, r.p_res[key][core, j].astype(f32))

    wide = r.p_res[0].shape[1]
    slim = r.p_res[2].shape[1]
    for h in range(heads):
        kv1_sent[h].wait_recv()

        def self_rows(base):
            attend_block(True, h, base, r.q1, r.kv1, r.seg, r.p1, r.a1, keys)

        loop_rows(rows, BLOCK, self_rows)
        if h == 0:
            gather_pump(CROSS_K, CROSS_V)
    gather_start(UP)
    gather_wait(SELF_O)
    sum_send_all(0, lambda base: nt(r.a1[pl.ds(base, CHUNK), :], weight(SELF_O)))
    gather_pump(CROSS_Q, CROSS_O)
    gather_start(DOWN)
    gather_wait(CROSS_K, CROSS_V)
    memory = r.in_mem[...]
    head_pairs(
        r.kv2, slice(None), forward_mm(memory, weight(CROSS_K)),
        forward_mm(memory, weight(CROSS_V)),
    )
    kv2_sent = [start(r.kv2.at[h, x], r.kv2.at[h, x], to_x) for h in range(heads)]
    gather_wait(CROSS_Q, CROSS_O)
    gather_pump(GATE)

    for j in range(wide):
        sum_recv(0, j)

        def second(base, value):
            here = pl.ds(base, CHUNK)
            v = r.in_dec[here, :].astype(f32) + value
            r.x1[here, :] = v
            h = norm(v, 1)
            r.h2[here, :] = h
            r.q2[here, :] = forward_mm(h, weight(CROSS_Q)).astype(bf16)

        both_sides(0, j, second)
        if j == 0:
            for c in kv2_sent:
                c.wait_recv()

        def mixed(base):
            for h in range(heads):
                attend_block(False, h, base, r.q2, r.kv2, r.mseg, r.p2, r.a2, mem_keys)
            return nt(r.a2[pl.ds(base, CHUNK), :], weight(CROSS_O))

        sum_send(1, j, mixed)
        if j == 0:
            gather_pump(UP)
    gather_pump(DOWN)

    def flip(src, dst, count):
        for j in range(dim // BLOCK):
            dst[j * BLOCK : (j + 1) * BLOCK, :count] = src[:, j * BLOCK : (j + 1) * BLOCK].T

    flip(r.in_cot, r.flip, rows)
    gather_wait(DOWN)

    def grad_hidden_block(base):
        here = pl.ds(base, BIG)
        r.gm[here, :] = forward_mm(r.in_cot[here, :], weight(DOWN))

    loop_rows(rows, BIG, grad_hidden_block)
    gather_wait(GATE, UP)

    for j in range(wide):
        sum_recv(1, j)

        def third(base, value):
            here = pl.ds(base, CHUNK)
            v = r.x1[here, :] + value
            r.x2[here, :] = v
            r.h3[here, :] = norm(v, 2)

        both_sides(1, j, third)

        def hidden_piece(base):
            here = pl.ds(base, CHUNK)
            h = r.h3[here, :]
            gate = forward_mm(h, weight(GATE))
            upper = forward_mm(h, weight(UP))
            scale = np.float32(np.sqrt(2.0 / np.pi))
            square = gate * gate
            curve = jnp.tanh(scale * (gate + 0.044715 * (square * gate)))
            lower = 0.5 * (1.0 + curve)
            gelu = gate * lower
            slope = lower + 0.5 * gate * (1.0 - curve * curve) * scale * (
                1.0 + 3 * 0.044715 * square
            )
            grad = r.gm[here, :]
            r.m[here, :] = (gelu * upper).astype(bf16)
            grad_gate = (grad * upper * slope).astype(bf16)
            grad_up = (grad * gelu).astype(bf16)
            r.ggate[here, :] = grad_gate
            r.gup[here, :] = grad_up
            return nt(grad_gate, weight(GATE)) + nt(grad_up, weight(UP))

        sum_send(0, j, hidden_piece)

    shard_rows = dim // SHARDS

    def grad_into(g, at, flipped, right, count):
        stage = r.stage[g]
        cols = right.shape[1]

        def step(d, carry):
            here = pl.ds(pl.multiple_of(d * shard_rows, shard_rows), shard_rows)
            value = forward_mm(flipped[here, :count], right[...]).astype(bf16)
            stage[d, :, :, at : at + cols] = value.reshape(2, half, cols)
            return carry

        lax.fori_loop(0, SHARDS, step, 0)

    reduces = {}

    def reduce_x(g):
        stage = r.stage[g]
        reduces[g] = [start(stage.at[:, 1 - x], r.xr[g], to_x)]

    def reduce_z(g):
        stage, xr, zr = r.stage[g], r.xr[g], r.zr[g]
        reduces[g][0].wait_recv()

        def step(d, carry):
            stage[d, x] = (stage[d, x].astype(f32) + xr[d].astype(f32)).astype(bf16)
            return carry

        lax.fori_loop(0, SHARDS, step, 0)
        for k in (1, 2, 3):
            d = lax.rem(z + k, SHARDS)
            reduces[g].append(start(stage.at[d, x], zr.at[k - 1], to_z(k)))

    def reduce_f(g):
        stage, zr, both = r.stage[g], r.zr[g], r.fb[g]
        total = stage[z, x].astype(f32)
        for k in (1, 2, 3):
            reduces[g][k].wait_recv()
            total = total + zr[k - 1].astype(f32)
        both[x] = total.astype(bf16)
        reduces[g].append(start(both.at[x], both.at[x], to_x))

    def reduce_o(g):
        reduces[g][4].wait_recv()
        leave(r.fb[g], r.o_fb[g])

    def whole_z(g):
        stage, zr = r.stage[g], r.zr[g]
        reduces[g] = [
            start(stage.at[lax.rem(z + k, SHARDS)], zr.at[k - 1], to_z(k)) for k in (1, 2, 3)
        ]

    def whole_x(g):
        stage, zr = r.stage[g], r.zr[g]
        total = stage[z].astype(f32)
        for k in (1, 2, 3):
            reduces[g][k - 1].wait_recv()
            total = total + zr[k - 1].astype(f32)
        r.fb[g][...] = total.astype(bf16)
        reduces[g].append(start(r.fb[g], r.xr[g], to_x))

    def whole_o(g):
        reduces[g][3].wait_recv()
        r.zr[g][0] = (r.fb[g][...].astype(f32) + r.xr[g][...].astype(f32)).astype(bf16)
        leave(r.zr[g].at[0], r.o_fb[g])

    grad_into(0, 0, r.flip, r.m, rows)
    whole_z(0)
    flip(r.h3, r.flip, rows)
    grad_into(2, 0, r.flip, r.gup, rows)
    reduce_x(2)
    grad_into(1, 0, r.flip, r.ggate, rows)
    whole_z(1)

    def norm_back(v, grad, k):
        inv = inverse(v)
        unit = v * inv
        scaled = grad * r.gains[k : k + 1, :]
        mean = jnp.mean(scaled * unit, axis=1, keepdims=True)
        return inv * (scaled - unit * mean), jnp.sum(grad * unit, axis=0, keepdims=True)

    def attend_back_block(causal, h, base, q, kv, p_ref, gq, ds, total):
        tiles = total // BLOCK
        here = pl.ds(base, BLOCK)
        lanes = slice(h * HEAD_DIM, (h + 1) * HEAD_DIM)
        pair = kv[h].reshape(total, 2 * HEAD_DIM)
        probs = p_ref[h, here, :].astype(f32)
        grad_probs = nt(r.ga[here, lanes], pair[:, HEAD_DIM:])
        mean = jnp.sum(probs * grad_probs, axis=1, keepdims=True)
        scores = probs * (grad_probs - mean)
        if causal:
            begin = pl.multiple_of((tiles - 1) * BLOCK - x * rows - base, BLOCK)
            window = pl.ds(begin, total)
            r.strip[h, :, window] = r.strip[h, :, window] + scores
        low = scores.astype(bf16)
        ds[here, :] = low
        gq[here, lanes] = forward_mm(low, pair[:, :HEAD_DIM]).astype(bf16)

    def pair_grads(h, q, p_ref, ds, gkv, total):
        lanes = slice(h * HEAD_DIM, (h + 1) * HEAD_DIM)
        r.gkv_t[:HEAD_DIM, :total] = tn(q[:, lanes], ds[...])
        r.gkv_t[HEAD_DIM:, :total] = tn(r.ga[:, lanes], p_ref[h])
        part = total // 2
        for side in range(2):
            gkv[h, side] = r.gkv_t[:, side * part : (side + 1) * part].T.astype(bf16)

    def pairs_sum(gkv, arrived, out):
        left, right = [], []
        for h in range(heads):
            value = gkv[h, x].astype(f32) + arrived[h].astype(f32)
            left.append(value[:, :HEAD_DIM])
            right.append(value[:, HEAD_DIM:])
        out[...] = jnp.concatenate(left + right, axis=1).astype(bf16)

    r.tiny[...] = jnp.zeros_like(r.tiny)
    for j in range(wide):
        sum_recv(0, j)

        def second_grad(base, value):
            here = pl.ds(base, CHUNK)
            back, gain = norm_back(r.x2[here, :], value, 2)
            grad = r.in_cot[here, :].astype(f32) + back
            r.tiny[2:3, :] = r.tiny[2:3, :] + gain
            r.gx[here, :] = grad
            low = grad.astype(bf16)
            r.gxb[here, :] = low
            r.ga[here, :] = forward_mm(low, weight(CROSS_O)).astype(bf16)

        both_sides(0, j, second_grad)

        def query_piece(base):
            for h in range(heads):
                attend_back_block(
                    False, h, base, r.q2, r.kv2, r.p2, r.gq2, r.ds2.at[h], mem_keys
                )
            return nt(r.gq2[pl.ds(base, CHUNK), :], weight(CROSS_Q))

        sum_send(1, j, query_piece)
    gkv2_sent = []
    for h in range(heads):
        pair_grads(h, r.q2, r.p2, r.ds2.at[h], r.gkv2, mem_keys)
        gkv2_sent.append(start(r.gkv2.at[h, 1 - x], r.gkv2_in.at[h], to_x))
    flip(r.gxb, r.flip, rows)
    grad_into(3, 0, r.flip, r.a2, rows)
    flip(r.h2, r.flip, rows)
    grad_into(3, width, r.flip, r.gq2, rows)
    reduce_x(3)

    for j in range(wide):
        sum_recv(1, j)

        def first_grad(base, value):
            here = pl.ds(base, CHUNK)
            back, gain = norm_back(r.x1[here, :], value, 1)
            grad = r.gx[here, :] + back
            r.tiny[1:2, :] = r.tiny[1:2, :] + gain
            r.gx[here, :] = grad
            low = grad.astype(bf16)
            r.gxb[here, :] = low
            r.ga1[here, :] = forward_mm(low, weight(SELF_O)).astype(bf16)

        both_sides(1, j, first_grad)
    reduce_z(2)
    sum_send_all(3, lambda base: nt(r.m[pl.ds(base, CHUNK), :], weight(DOWN)))
    r.ga[...] = r.ga1[...]
    r.strip[...] = jnp.zeros_like(r.strip)
    gkv1_sent = []
    for h in range(heads):

        def self_back_rows(base):
            attend_back_block(True, h, base, r.q1, r.kv1, r.p1, r.gq1, r.ds, keys)

        loop_rows(rows, BLOCK, self_back_rows)
        pair_grads(h, r.q1, r.p1, r.ds, r.gkv1, keys)
        gkv1_sent.append(start(r.gkv1.at[h, 1 - x], r.gkv1_in.at[h], to_x))
        if h == 0:
            for c in gkv2_sent:
                c.wait_recv()
            pairs_sum(r.gkv2, r.gkv2_in, r.gkv2_sum)
            flip(r.in_mem, r.flip, mem_count)
            grad_into(4, 0, r.flip, r.gkv2_sum, mem_count)
            reduce_x(4)
        if h == 1:
            reduce_z(3)
    tiles = keys // BLOCK
    row = lax.broadcasted_iota(jnp.int32, (BLOCK, BLOCK), 0)
    col = lax.broadcasted_iota(jnp.int32, (BLOCK, BLOCK), 1)
    for h in range(heads):
        own = r.strip[h, :, (tiles - 1) * BLOCK : tiles * BLOCK]
        prior = r.strip[h, :, (tiles - 2) * BLOCK : (tiles - 1) * BLOCK]
        far = jnp.where(row < col, 0.0, prior)
        for j in range(tiles - 2):
            far = far + r.strip[h, :, j * BLOCK : (j + 1) * BLOCK]
        r.tiny[3 + h : 4 + h, :BLOCK] = fold_diagonals(own + jnp.where(row < col, prior, 0.0))
        r.tiny[3 + h : 4 + h, BLOCK : 2 * BLOCK] = jnp.sum(far, axis=0, keepdims=True)
    flip(r.gxb, r.flip, rows)
    grad_into(5, 0, r.flip, r.a1, rows)
    flip(r.h1, r.flip, rows)
    grad_into(5, width, r.flip, r.gq1, rows)
    for c in gkv1_sent:
        c.wait_recv()
    pairs_sum(r.gkv1, r.gkv1_in, r.gkv1_sum)

    def input_piece(base):
        here = pl.ds(base, CHUNK)
        return (
            nt(r.gq1[here, :], weight(SELF_Q))
            + nt(r.gkv1_sum[here, :width], weight(SELF_K))
            + nt(r.gkv1_sum[here, width:], weight(SELF_V))
        )

    sum_send_all(0, input_piece)
    reduce_x(5)
    grad_into(6, 0, r.flip, r.gkv1_sum, rows)
    reduce_x(6)

    def memory_piece(base):
        here = pl.ds(base, CHUNK)
        return nt(r.gkv2_sum[here, :width], weight(CROSS_K)) + nt(
            r.gkv2_sum[here, width:], weight(CROSS_V)
        )

    sum_send_all(2, memory_piece)
    reduce_z(4)
    for j in range(wide):
        sum_recv(3, j)

        def output_rows(base, value):
            here = pl.ds(base, CHUNK)
            r.dec[here, :] = (r.x2[here, :] + value).astype(bf16)

        both_sides(3, j, output_rows)
    leave(r.dec, r.o_dec)
    reduce_f(2)

    def tail():
        reduce_z(5)

    for j in range(wide):
        sum_recv(0, j, tail if j == wide - 1 else None)

        def input_grad(base, value):
            here = pl.ds(base, CHUNK)
            back, gain = norm_back(r.in_dec[here, :].astype(f32), value, 0)
            r.tiny[0:1, :] = r.tiny[0:1, :] + gain
            r.gx[here, :] = r.gx[here, :] + back

        both_sides(0, j, input_grad)
    slot = x * SHARDS + z
    r.tiny_all[slot] = r.tiny[...]
    tiny_sent = [
        start(r.tiny, r.tiny_all.at[slot], p) for p in [to_x] + partners[:3] + others
    ]
    leave(r.gx, r.o_input)
    reduce_z(6)
    for g in WHOLE:
        whole_x(g)
    for g in (3, 4):
        reduce_f(g)
    for j in range(slim):
        sum_recv(2, j)
    leave(r.p_res[2], r.o_mem)
    for g in (5, 6):
        reduce_f(g)
    for c in tiny_sent:
        c.wait_recv()
    total = r.tiny_all[0]
    for n in range(1, 2 * SHARDS):
        total = total + r.tiny_all[n]
    r.tiny_sum[...] = total
    leave(r.tiny_sum, r.o_tiny)
    for g in (2, 3, 4, 5):
        reduce_o(g)
    for g in WHOLE:
        whole_o(g)
    reduce_o(6)
    for c in unsent:
        c.wait_send()
    for c in leaving:
        c.wait()


def output_kernel(trees, *refs):
    found, at = {}, 0
    for tree in trees:
        found.update(tree.unflatten(refs[at : at + tree.num_leaves]))
        at += tree.num_leaves
    r = types.SimpleNamespace(**found)
    z = lax.axis_index(SHARD)
    r.out_dec[...] = r.o_dec[...]
    r.out_input[...] = r.o_input[...]
    r.out_mem[...] = r.o_mem[...].reshape(r.out_mem.shape).astype(f32)
    for g, group in enumerate(GROUPS):
        at = 0
        for name in group:
            out = r.out_grad[name]
            cols = out.shape[1]
            out[...] = r.o_fb[g][:, :, at : at + cols].reshape(out.shape).astype(f32)
            at += cols
    total = r.o_tiny[...]
    part = r.out_gain[0].shape[1]
    for k in range(3):
        piece = jnp.zeros((1, part), f32)
        for n in range(SHARDS):
            piece = jnp.where(z == n, total[k : k + 1, n * part : (n + 1) * part], piece)
        r.out_gain[k][...] = piece
    lanes = r.in_lanes[...]
    bucket = lax.broadcasted_iota(jnp.int32, (BUCKETS, 1), 0)
    share, heads = r.out_table.shape
    columns = []
    for h in range(heads):
        near = jnp.sum(lanes * total[3 + h : 4 + h, :BLOCK], axis=1, keepdims=True)
        far = jnp.sum(total[3 + h : 4 + h, BLOCK : 2 * BLOCK], axis=1, keepdims=True)
        columns.append(near + jnp.where(bucket == BUCKETS - 1, far, 0.0))
    r.table[...] = jnp.concatenate(columns, axis=1)
    r.out_table[...] = r.table[pl.ds(pl.multiple_of(z * share, share), share), :]


def local_fast(
    dec_in, memory, dec_segments, mem_segments, gain_self, gain_cross, gain_ffn,
    self_q, self_k, self_v, self_o, cross_q, cross_k, cross_v, cross_o,
    ffn_gate, ffn_up, ffn_down, bias_table, cotangent,
):
    rows, dim = dec_in.shape[1:]
    mem = memory.shape[1]
    width, hidden = self_q.shape[1], ffn_gate.shape[1]
    heads = width // HEAD_DIM
    part = gain_self.shape[0]
    share = bias_table.shape[0]
    keys, mem_keys = 2 * rows, 2 * mem
    half = dim // SHARDS // 2
    line = lax.broadcasted_iota(jnp.int32, (16, part), 0)
    small = jnp.pad(bias_table, ((8, 0), (0, part - heads)))
    for k, gain in enumerate((gain_self, gain_cross, gain_ffn)):
        small = jnp.where(line == k, gain[None, :], small)
    weights = [
        self_q, self_k, self_v, self_o, cross_q, cross_k, cross_v, cross_o,
        ffn_gate, ffn_up, ffn_down,
    ]
    widths = [w.shape[1] for w in weights]
    joined = [sum(widths[k] for k in group) for group in GROUPS]
    chunks = [n // 2 // CHUNK for n in (rows, rows, mem, rows)]
    near = dict(
        in_dec=dec_in[0], in_mem=memory[0], in_seg=dec_segments, in_mseg=mem_segments,
        in_lanes=jnp.asarray(lane_buckets()), in_cot=cotangent[0],
    )
    far = dict(in_small=small, part=weights)

    def out(shape, kind):
        return jax.ShapeDtypeStruct(shape, kind)

    outs = dict(
        out_dec=out((rows, dim), bf16), out_input=out((rows, dim), f32),
        out_mem=out((mem, dim), f32), out_gain=[out((1, part), f32)] * 3,
        out_grad=[out((part, c), f32) for c in widths], out_table=out((share, heads), f32),
    )
    passed = dict(
        o_dec=out((rows, dim), bf16), o_input=out((rows, dim), f32),
        o_mem=out((2, chunks[2], CHUNK, dim), bf16), o_tiny=out((8, dim), f32),
        o_fb=[out((2, half, c), bf16) for c in joined],
    )
    vmem = pltpu.VMEM
    held = dict(
        full=[vmem((SHARDS, 2, half, c), bf16) for c in widths],
        small=vmem((SHARDS, 16, part), bf16), seg=vmem((1, keys), f32),
        mseg=vmem((1, mem_keys), f32), seg_col=vmem((rows, 8), f32), gains=vmem((8, dim), f32),
        near=vmem((8, BLOCK), f32), far=vmem((8, BLOCK), f32),
        strip=vmem((heads, BLOCK, (2 * (keys // BLOCK) - 1) * BLOCK), f32),
        h1=vmem((rows, dim), bf16), h2=vmem((rows, dim), bf16), h3=vmem((rows, dim), bf16),
        x1=vmem((rows, dim), f32), x2=vmem((rows, dim), f32),
        q1=vmem((rows, width), bf16), q2=vmem((rows, width), bf16),
        kv1=vmem((heads, 2, rows, 2 * HEAD_DIM), bf16), kv2=vmem((heads, 2, mem, 2 * HEAD_DIM), bf16),
        p1=vmem((heads, rows, keys), bf16), p2=vmem((heads, rows, mem_keys), bf16),
        a1=vmem((rows, width), bf16), a2=vmem((rows, width), bf16),
        gm=vmem((rows, hidden), f32), m=vmem((rows, hidden), bf16),
        ggate=vmem((rows, hidden), bf16), gup=vmem((rows, hidden), bf16),
        flip=vmem((dim, rows), bf16), gx=vmem((rows, dim), f32), gxb=vmem((rows, dim), bf16),
        ga=vmem((rows, width), bf16), ds=vmem((rows, keys), bf16),
        gkv_t=vmem((2 * HEAD_DIM, keys), f32), ds2=vmem((heads, rows, mem_keys), bf16),
        ga1=vmem((rows, width), bf16), dec=vmem((rows, dim), bf16), gq1=vmem((rows, width), bf16),
        gq2=vmem((rows, width), bf16), gkv1=vmem((heads, 2, rows, 2 * HEAD_DIM), bf16),
        gkv2=vmem((heads, 2, mem, 2 * HEAD_DIM), bf16), gkv1_in=vmem((heads, rows, 2 * HEAD_DIM), bf16),
        gkv2_in=vmem((heads, mem, 2 * HEAD_DIM), bf16), gkv1_sum=vmem((rows, 2 * width), bf16),
        gkv2_sum=vmem((mem, 2 * width), bf16), tiny=vmem((8, dim), f32),
        tiny_all=vmem((2 * SHARDS, 8, dim), f32), tiny_sum=vmem((8, dim), f32),
        ps_out=[vmem((n, CHUNK, dim), bf16) for n in chunks],
        ps_in=[vmem((n, CHUNK, dim), bf16) for n in chunks],
        py_out=[vmem((n, CHUNK, dim), bf16) for n in chunks],
        py_in=[vmem((n, CHUNK, dim), bf16) for n in chunks],
        p_res=[vmem((2, n, CHUNK, dim), bf16) for n in chunks],
        stage=[vmem((SHARDS, 2, half, c), bf16) for c in joined],
        xr=[
            vmem((2 if g in WHOLE else SHARDS, half, c), bf16) for g, c in enumerate(joined)
        ],
        zr=[
            vmem((3, 2, half, c) if g in WHOLE else (3, half, c), bf16)
            for g, c in enumerate(joined)
        ],
        fb=[vmem((2, half, c), bf16) for c in joined],
        send_sem=pltpu.SemaphoreType.DMA((192,)), recv_sem=pltpu.SemaphoreType.DMA((192,)),
        own_sem=pltpu.SemaphoreType.DMA((40,)),
    )
    in_vmem = pl.BlockSpec(memory_space=pltpu.VMEM)
    anywhere = pl.BlockSpec(memory_space=pl.ANY)
    flat = [jax.tree.flatten(v) for v in (near, far, passed, held)]
    results = pl.pallas_call(
        functools.partial(
            layer_kernel, (rows, mem, dim, width, heads), [tree for _, tree in flat]
        ),
        out_shape=tuple(flat[2][0]),
        in_specs=[in_vmem] * len(flat[0][0]) + [anywhere] * len(flat[1][0]),
        out_specs=tuple([anywhere] * len(flat[2][0])),
        scratch_shapes=flat[3][0],
        compiler_params=pltpu.CompilerParams(
            collective_id=0, has_side_effects=True, vmem_limit_bytes=67043328
        ),
        name="layer",
    )(*flat[0][0], *flat[1][0])
    ready = dict(flat[2][1].unflatten(results), in_lanes=near["in_lanes"])
    table = dict(table=vmem((BUCKETS, heads), f32))
    flat = [jax.tree.flatten(v) for v in (ready, outs, table)]
    results = pl.pallas_call(
        functools.partial(output_kernel, [tree for _, tree in flat]),
        out_shape=tuple(flat[1][0]),
        in_specs=[in_vmem] * len(flat[0][0]),
        out_specs=tuple([in_vmem] * len(flat[1][0])),
        scratch_shapes=flat[2][0],
        compiler_params=pltpu.CompilerParams(vmem_limit_bytes=67043328),
        name="outputs",
    )(*flat[0][0])
    flat = flat[:1] + [None] + flat[1:2]
    got = types.SimpleNamespace(**flat[2][1].unflatten(results))
    return (
        got.out_dec[None], got.out_input[None], got.out_mem[None],
        *[g[0] for g in got.out_gain], *got.out_grad, got.out_table,
    )


def shard_part(parts):
    return tuple(
        lax.psum_scatter(p.astype(jnp.bfloat16), SHARD, scatter_dimension=0, tiled=True).astype(
            jnp.float32
        )
        for p in parts
    )


def context_total(parts):
    return tuple(lax.psum(p.astype(jnp.bfloat16), CTX).astype(jnp.float32) for p in parts)


def local(
    dec_in,
    memory,
    dec_segments,
    mem_segments,
    gain_self,
    gain_cross,
    gain_ffn,
    self_q,
    self_k,
    self_v,
    self_o,
    cross_q,
    cross_k,
    cross_v,
    cross_o,
    ffn_gate,
    ffn_up,
    ffn_down,
    bias_table,
    cotangent,
):
    gathered = (
        lax.all_gather(gain_self, SHARD, axis=0, tiled=True),
        lax.all_gather(gain_cross, SHARD, axis=0, tiled=True),
        lax.all_gather(gain_ffn, SHARD, axis=0, tiled=True),
        lax.all_gather(self_q, SHARD, axis=0, tiled=True),
        lax.all_gather(self_k, SHARD, axis=0, tiled=True),
        lax.all_gather(self_v, SHARD, axis=0, tiled=True),
        lax.all_gather(self_o, SHARD, axis=0, tiled=True),
        lax.all_gather(cross_q, SHARD, axis=0, tiled=True),
        lax.all_gather(cross_k, SHARD, axis=0, tiled=True),
        lax.all_gather(cross_v, SHARD, axis=0, tiled=True),
        lax.all_gather(cross_o, SHARD, axis=0, tiled=True),
        lax.all_gather(ffn_gate, SHARD, axis=0, tiled=True),
        lax.all_gather(ffn_up, SHARD, axis=0, tiled=True),
        lax.all_gather(ffn_down, SHARD, axis=0, tiled=True),
        lax.all_gather(bias_table, SHARD, axis=0, tiled=True),
    )
    (
        norm_one,
        norm_two,
        norm_three,
        query_self,
        key_self,
        value_self,
        out_self,
        query_cross,
        key_cross,
        value_cross,
        out_cross,
        gate_full,
        up_full,
        down_full,
        table_full,
    ) = gathered
    gain_one = norm_one.astype(jnp.float32)
    gain_two = norm_two.astype(jnp.float32)
    gain_three = norm_three.astype(jnp.float32)
    table = table_full.astype(jnp.float32)
    width = query_self.shape[1]
    hidden_in = dec_in[0].astype(jnp.float32)
    mem_rows = memory[0]
    grad_out = cotangent[0].astype(jnp.float32)
    count_rows = hidden_in.shape[0]
    place = lax.axis_index(CTX)
    dec_ids = dec_segments[0]
    mem_ids = mem_segments[0]
    query_ids = lax.dynamic_slice_in_dim(dec_ids, place * count_rows, count_rows)
    query_pos = place * count_rows + jnp.arange(count_rows, dtype=jnp.int32)
    key_pos = jnp.arange(dec_ids.shape[0], dtype=jnp.int32)
    mem_pos = jnp.arange(mem_ids.shape[0], dtype=jnp.int32)
    normed_one = rms_norm(hidden_in, gain_one).astype(jnp.bfloat16)
    query_one = forward_mm(normed_one, query_self).astype(jnp.bfloat16)
    pairs_own = jnp.concatenate(
        [forward_mm(normed_one, key_self), forward_mm(normed_one, value_self)], axis=1
    ).astype(jnp.bfloat16)
    pairs_one = lax.all_gather(pairs_own, CTX, axis=0, tiled=True)
    mixed_one, lse_one = attend(
        query_one, pairs_one, key_pos, dec_ids, query_pos, query_ids, table, True
    )
    context_one = mixed_one.astype(jnp.bfloat16)
    first = hidden_in + lax.psum(
        backward_mm(context_one, out_self).astype(jnp.bfloat16), TENSOR
    ).astype(jnp.float32)
    normed_two = rms_norm(first, gain_two).astype(jnp.bfloat16)
    query_two = forward_mm(normed_two, query_cross).astype(jnp.bfloat16)
    pairs_mem = jnp.concatenate(
        [forward_mm(mem_rows, key_cross), forward_mm(mem_rows, value_cross)], axis=1
    ).astype(jnp.bfloat16)
    pairs_two = lax.all_gather(pairs_mem, CTX, axis=0, tiled=True)
    mixed_two, lse_two = attend(
        query_two, pairs_two, mem_pos, mem_ids, query_pos, query_ids, table, False
    )
    context_two = mixed_two.astype(jnp.bfloat16)
    second = first + lax.psum(
        backward_mm(context_two, out_cross).astype(jnp.bfloat16), TENSOR
    ).astype(jnp.float32)
    normed_three = rms_norm(second, gain_three).astype(jnp.bfloat16)
    gate = forward_mm(normed_three, gate_full)
    upper = forward_mm(normed_three, up_full)
    activated = gated(gate, upper).astype(jnp.bfloat16)
    result = second + lax.psum(
        backward_mm(activated, down_full).astype(jnp.bfloat16), TENSOR
    ).astype(jnp.float32)
    dec_out = result.astype(jnp.bfloat16)
    grad_low = cotangent[0]
    grad_down_w = weight_mm(grad_low, activated)
    grad_hidden = forward_mm(grad_low, down_full)
    _, pull_gate = jax.vjp(gated, gate, upper)
    grad_gate, grad_upper = pull_gate(grad_hidden)
    gate_low = grad_gate.astype(jnp.bfloat16)
    upper_low = grad_upper.astype(jnp.bfloat16)
    grad_gate_w = weight_mm(normed_three, gate_low)
    grad_up_w = weight_mm(normed_three, upper_low)
    grad_normed_three = backward_mm(gate_low, gate_full) + backward_mm(upper_low, up_full)
    grad_normed_three = lax.psum(grad_normed_three.astype(jnp.bfloat16), TENSOR).astype(
        jnp.float32
    )
    _, pull_three = jax.vjp(rms_norm, second, gain_three)
    grad_second, grad_gain_three = pull_three(grad_normed_three)
    grad_second = grad_out + grad_second
    second_low = grad_second.astype(jnp.bfloat16)
    grad_out_cross = weight_mm(second_low, context_two)
    grad_context_two = forward_mm(second_low, out_cross).astype(jnp.bfloat16)
    grad_query_two, grad_pairs_two, _ = attend_back(
        query_two,
        pairs_two,
        mem_pos,
        mem_ids,
        query_pos,
        query_ids,
        table,
        False,
        mixed_two,
        lse_two,
        grad_context_two,
    )
    pairs_grad_mem = lax.psum_scatter(
        grad_pairs_two.astype(jnp.bfloat16), CTX, scatter_dimension=0, tiled=True
    )
    query_two_low = grad_query_two.astype(jnp.bfloat16)
    grad_mem_keys = pairs_grad_mem[:, :width]
    grad_mem_values = pairs_grad_mem[:, width:]
    grad_query_cross = weight_mm(normed_two, query_two_low)
    grad_key_cross = weight_mm(mem_rows, grad_mem_keys)
    grad_value_cross = weight_mm(mem_rows, grad_mem_values)
    grad_normed_two = backward_mm(query_two_low, query_cross)
    grad_memory = backward_mm(grad_mem_keys, key_cross) + backward_mm(grad_mem_values, value_cross)
    grad_normed_two, grad_memory = (
        lax.psum(grad_normed_two.astype(jnp.bfloat16), TENSOR).astype(jnp.float32),
        lax.psum(grad_memory.astype(jnp.bfloat16), TENSOR).astype(jnp.float32),
    )
    _, pull_two = jax.vjp(rms_norm, first, gain_two)
    grad_first, grad_gain_two = pull_two(grad_normed_two)
    grad_first = grad_second + grad_first
    first_low = grad_first.astype(jnp.bfloat16)
    grad_out_self = weight_mm(first_low, context_one)
    grad_context_one = forward_mm(first_low, out_self).astype(jnp.bfloat16)
    grad_query_one, grad_pairs_one, grad_table = attend_back(
        query_one,
        pairs_one,
        key_pos,
        dec_ids,
        query_pos,
        query_ids,
        table,
        True,
        mixed_one,
        lse_one,
        grad_context_one,
    )
    pairs_grad_own = lax.psum_scatter(
        grad_pairs_one.astype(jnp.bfloat16), CTX, scatter_dimension=0, tiled=True
    )
    query_one_low = grad_query_one.astype(jnp.bfloat16)
    grad_keys_own = pairs_grad_own[:, :width]
    grad_values_own = pairs_grad_own[:, width:]
    grad_query_self = weight_mm(normed_one, query_one_low)
    grad_key_self = weight_mm(normed_one, grad_keys_own)
    grad_value_self = weight_mm(normed_one, grad_values_own)
    grad_normed_one = (
        backward_mm(query_one_low, query_self)
        + backward_mm(grad_keys_own, key_self)
        + backward_mm(grad_values_own, value_self)
    )
    grad_normed_one = lax.psum(grad_normed_one.astype(jnp.bfloat16), TENSOR).astype(jnp.float32)
    _, pull_one = jax.vjp(rms_norm, hidden_in, gain_one)
    grad_input, grad_gain_one = pull_one(grad_normed_one)
    grad_input = grad_first + grad_input
    local_grads = (
        grad_gain_one,
        grad_gain_two,
        grad_gain_three,
        grad_query_self,
        grad_key_self,
        grad_value_self,
        grad_out_self,
        grad_query_cross,
        grad_key_cross,
        grad_value_cross,
        grad_out_cross,
        grad_gate_w,
        grad_up_w,
        grad_down_w,
        grad_table,
    )
    summed = shard_part(context_total(local_grads))
    return (
        dec_out[None],
        grad_input[None],
        grad_memory[None],
        summed[0],
        summed[1],
        summed[2],
        summed[3],
        summed[4],
        summed[5],
        summed[6],
        summed[7],
        summed[8],
        summed[9],
        summed[10],
        summed[11],
        summed[12],
        summed[13],
        summed[14],
    )


def solution(mesh):
    in_specs = (
        P(SHARD, CTX, None),
        P(SHARD, CTX, None),
        P(SHARD, None),
        P(SHARD, None),
        P(SHARD),
        P(SHARD),
        P(SHARD),
        P(SHARD, TENSOR),
        P(SHARD, TENSOR),
        P(SHARD, TENSOR),
        P(SHARD, TENSOR),
        P(SHARD, TENSOR),
        P(SHARD, TENSOR),
        P(SHARD, TENSOR),
        P(SHARD, TENSOR),
        P(SHARD, TENSOR),
        P(SHARD, TENSOR),
        P(SHARD, TENSOR),
        P(SHARD, TENSOR),
        P(SHARD, CTX, None),
    )
    out_specs = (
        P(SHARD, CTX, None),
        P(SHARD, CTX, None),
        P(SHARD, CTX, None),
        P(SHARD),
        P(SHARD),
        P(SHARD),
        P(SHARD, TENSOR),
        P(SHARD, TENSOR),
        P(SHARD, TENSOR),
        P(SHARD, TENSOR),
        P(SHARD, TENSOR),
        P(SHARD, TENSOR),
        P(SHARD, TENSOR),
        P(SHARD, TENSOR),
        P(SHARD, TENSOR),
        P(SHARD, TENSOR),
        P(SHARD, TENSOR),
        P(SHARD, TENSOR),
    )
    fast = (mesh.shape[SHARD], mesh.shape[CTX], mesh.shape[TENSOR]) == (SHARDS, 2, 4)
    body = local_fast if fast else local
    return jax.shard_map(body, mesh=mesh, in_specs=in_specs, out_specs=out_specs, check_vma=False)
```

```python
import functools
import types

import jax
import jax.numpy as jnp
import numpy as np
from jax import lax
from jax.experimental import pallas as pl
from jax.experimental.pallas import tpu as pltpu
from jax.sharding import PartitionSpec as P

SHARD, CTX, TENSOR = "shard", "ctx", "tensor"
HEAD_DIM = 64
BUCKETS = 32
MAX_DIST = 128


highest = lax.Precision.HIGHEST
epsilon = 1e-06
negative = -1e30


def thresholds():
    exact_part = BUCKETS // 2
    small_part = np.arange(1, exact_part + 1)
    steps_up = np.arange(exact_part + 1, BUCKETS)
    large_part = np.ceil(
        exact_part * (MAX_DIST / exact_part) ** ((steps_up - exact_part) / (BUCKETS - exact_part))
    )
    return np.concatenate([small_part, large_part]).astype(np.int32)


def bucket_of(distance):
    limits = jnp.asarray(thresholds())
    return jnp.sum((distance[..., None] >= limits).astype(jnp.int32), axis=-1)


def rms_norm(values, gain):
    return values * lax.rsqrt(jnp.mean(values * values, axis=-1, keepdims=True) + epsilon) * gain


def gated(gate, upper):
    return jax.nn.gelu(gate, approximate=True) * upper


def forward_mm(left, right):
    return jnp.dot(left, right, preferred_element_type=jnp.float32)


def backward_mm(left, right):
    return lax.dot_general(
        left, right, (((1,), (1,)), ((), ())), preferred_element_type=jnp.float32
    )


def weight_mm(left, right):
    return lax.dot_general(
        left, right, (((0,), (0,)), ((), ())), preferred_element_type=jnp.float32
    )


def toeplitz(vector, count_rows, count_cols):
    heads = vector.shape[0]
    span = count_rows + count_cols - 1
    tiled = jnp.pad(jnp.tile(vector, (1, count_rows)), ((0, 0), (0, count_rows)))
    grid = tiled.reshape(heads, count_rows, span + 1)[:, :, :count_cols]
    return grid[:, :, ::-1]


def diagonal_sums(block):
    heads, count_rows, count_cols = block.shape
    span = count_rows + count_cols - 1
    flipped = jnp.pad(block[:, :, ::-1], ((0, 0), (0, 0), (0, count_rows)))
    flat = flipped.reshape(heads, count_rows * (span + 1))[:, : count_rows * span]
    return jnp.sum(flat.reshape(heads, count_rows, span), axis=1)


def bias_block(table, offset, count_rows, count_cols):
    span = count_rows + count_cols - 1
    distance = jnp.arange(span, dtype=jnp.int32) - (count_cols - 1) + offset
    onehot = (
        bucket_of(distance)[:, None] == jnp.arange(table.shape[0], dtype=jnp.int32)[None, :]
    ).astype(jnp.float32)
    column = jnp.dot(onehot, table, precision=highest)
    return (toeplitz(column.T, count_rows, count_cols), onehot)


def key_blocks(pairs, key_pos, key_seg):
    length = pairs.shape[0]
    width = min(512, length)
    count = length // width
    heads = pairs.shape[1] // (2 * HEAD_DIM)
    blocks = pairs.reshape(count, width, 2, heads, HEAD_DIM)
    starts = jnp.arange(count, dtype=jnp.int32) * width
    return (blocks, key_pos.reshape(count, width), key_seg.reshape(count, width), starts)


def scores_of(query, block, block_pos, block_seg, start, query_pos, query_seg, table, causal):
    scores = jnp.einsum("qhd,khd->hqk", query, block[:, 0], preferred_element_type=jnp.float32)
    mask = query_seg[:, None] == block_seg[None, :]
    onehot = None
    if causal:
        mask = mask & (query_pos[:, None] >= block_pos[None, :])
        bias, onehot = bias_block(table, query_pos[0] - start, query.shape[0], block.shape[0])
        scores = scores + bias
    return (jnp.where(mask[None], scores, negative), mask, onehot)


def attend(query, pairs, key_pos, key_seg, query_pos, query_seg, table, causal):
    count_rows = query.shape[0]
    heads = query.shape[1] // HEAD_DIM
    query = query.reshape(count_rows, heads, HEAD_DIM)
    blocks = key_blocks(pairs, key_pos, key_seg)

    def stats(carry, item):
        peak, total = carry
        block, block_pos, block_seg, start = item
        scores, mask, _ = scores_of(
            query, block, block_pos, block_seg, start, query_pos, query_seg, table, causal
        )
        fresh = jnp.maximum(peak, jnp.max(scores, axis=-1))
        weights = jnp.where(mask[None], jnp.exp(scores - fresh[..., None]), 0.0)
        total = total * jnp.exp(peak - fresh) + jnp.sum(weights, axis=-1)
        return ((fresh, total), None)

    start_peak = jnp.full((heads, count_rows), negative, jnp.float32)
    start_total = jnp.zeros((heads, count_rows), jnp.float32)
    (peak, total), _ = lax.scan(stats, (start_peak, start_total), blocks)
    log_total = peak + jnp.log(total)

    def collect(accum, item):
        block, block_pos, block_seg, start = item
        scores, mask, _ = scores_of(
            query, block, block_pos, block_seg, start, query_pos, query_seg, table, causal
        )
        probs = jnp.where(mask[None], jnp.exp(scores - log_total[..., None]), 0.0).astype(
            jnp.bfloat16
        )
        accum = accum + jnp.einsum(
            "hqk,khd->qhd", probs, block[:, 1], preferred_element_type=jnp.float32
        )
        return (accum, None)

    mixed, _ = lax.scan(collect, jnp.zeros((count_rows, heads, HEAD_DIM), jnp.float32), blocks)
    return (mixed.reshape(count_rows, heads * HEAD_DIM), log_total)


def correction_of(grad_mixed, mixed):
    count_rows = mixed.shape[0]
    heads = mixed.shape[1] // HEAD_DIM
    return jnp.einsum(
        "qhd,qhd->hq",
        grad_mixed.reshape(count_rows, heads, HEAD_DIM).astype(jnp.float32),
        mixed.reshape(count_rows, heads, HEAD_DIM),
    )


def attend_back(
    query,
    pairs,
    key_pos,
    key_seg,
    query_pos,
    query_seg,
    table,
    causal,
    mixed,
    log_total,
    grad_mixed,
):
    count_rows = query.shape[0]
    heads = query.shape[1] // HEAD_DIM
    query = query.reshape(count_rows, heads, HEAD_DIM)
    grad_heads = grad_mixed.reshape(count_rows, heads, HEAD_DIM)
    correction = correction_of(grad_mixed, mixed)
    blocks = key_blocks(pairs, key_pos, key_seg)

    def step(carry, item):
        grad_query, grad_table = carry
        block, block_pos, block_seg, start = item
        scores, mask, onehot = scores_of(
            query, block, block_pos, block_seg, start, query_pos, query_seg, table, causal
        )
        probs = jnp.where(mask[None], jnp.exp(scores - log_total[..., None]), 0.0)
        grad_probs = jnp.einsum(
            "qhd,khd->hqk", grad_heads, block[:, 1], preferred_element_type=jnp.float32
        )
        grad_scores = probs * (grad_probs - correction[..., None])
        if causal:
            grad_table = grad_table + jnp.dot(
                onehot.T, diagonal_sums(grad_scores).T, precision=highest
            )
        low_scores = grad_scores.astype(jnp.bfloat16)
        grad_query = grad_query + jnp.einsum(
            "hqk,khd->qhd", low_scores, block[:, 0], preferred_element_type=jnp.float32
        )
        stacked = None
        grad_values = jnp.einsum(
            "hqk,qhd->khd",
            probs.astype(jnp.bfloat16),
            grad_heads,
            preferred_element_type=jnp.float32,
        )
        grad_keys = jnp.einsum(
            "hqk,qhd->khd", low_scores, query, preferred_element_type=jnp.float32
        )
        width = block.shape[0]
        stacked = jnp.concatenate(
            [
                grad_keys.reshape(width, heads * HEAD_DIM),
                grad_values.reshape(width, heads * HEAD_DIM),
            ],
            axis=1,
        )
        return ((grad_query, grad_table), stacked)

    start = (
        jnp.zeros((count_rows, heads, HEAD_DIM), jnp.float32),
        jnp.zeros(table.shape, jnp.float32),
    )
    (grad_query, grad_table), grad_pairs = lax.scan(step, start, blocks)
    grad_pairs = grad_pairs.reshape(pairs.shape[0], pairs.shape[1])
    return (grad_query.reshape(count_rows, heads * HEAD_DIM), grad_pairs, grad_table)


BLOCK = 128


def nt(left, right):
    return lax.dot_general(
        left, right, (((1,), (1,)), ((), ())), preferred_element_type=jnp.float32
    )


def tn(left, right):
    return lax.dot_general(
        left, right, (((0,), (0,)), ((), ())), preferred_element_type=jnp.float32
    )


def lane_buckets():
    lane = np.arange(BLOCK)
    distance = (BLOCK - lane) % BLOCK
    bucket = (distance[:, None] >= thresholds()[None, :]).sum(axis=1)
    return (bucket[None, :] == np.arange(BUCKETS)[:, None]).astype(np.float32)


def build_strip(near_ref, far_ref, strip_ref, tiles, heads):
    row = lax.broadcasted_iota(jnp.int32, (BLOCK, BLOCK), 0)
    col = lax.broadcasted_iota(jnp.int32, (BLOCK, BLOCK), 1)
    for h in range(heads):
        near = jnp.broadcast_to(near_ref[h : h + 1, :], (BLOCK, BLOCK))
        near = pltpu.roll(near, 0, 1, stride=1, stride_axis=0)
        far = jnp.broadcast_to(far_ref[h : h + 1, :], (BLOCK, BLOCK))
        for m in range(tiles - 2):
            strip_ref[h, :, m * BLOCK : (m + 1) * BLOCK] = far
        strip_ref[h, :, (tiles - 2) * BLOCK : (tiles - 1) * BLOCK] = jnp.where(
            row < col, near, far
        )
        strip_ref[h, :, (tiles - 1) * BLOCK : tiles * BLOCK] = near
        strip_ref[h, :, tiles * BLOCK :] = jnp.zeros((BLOCK, (tiles - 1) * BLOCK), jnp.float32)


def fold_diagonals(tile):
    rows = BLOCK
    while rows > 8:
        rows //= 2
        tile = tile[:rows] + pltpu.roll(tile[rows:], BLOCK - rows, 1)
    total = tile[0:1]
    for r in range(1, 8):
        total = total + pltpu.roll(tile[r : r + 1], BLOCK - r, 1)
    return total


SELF_Q, SELF_K, SELF_V, SELF_O, CROSS_Q, CROSS_K, CROSS_V, CROSS_O, GATE, UP, DOWN = range(11)
GROUPS = (
    (DOWN,), (GATE,), (UP,), (CROSS_O, CROSS_Q), (CROSS_K, CROSS_V),
    (SELF_O, SELF_Q), (SELF_K, SELF_V),
)
ORDER = (
    SELF_K, SELF_V, SELF_Q, SELF_O, CROSS_K, CROSS_V, CROSS_Q, CROSS_O, GATE, UP, DOWN,
)
WHOLE = (0, 1, 5)
DIRECT = (DOWN,)
CHUNK = 128
BIG = 256
SHARDS = 4
MESH = pl.DeviceIdType.MESH
bf16 = jnp.bfloat16
f32 = jnp.float32


def loop_rows(count, block, step):
    def body(i, carry):
        step(pl.multiple_of(i * block, block))
        return carry

    lax.fori_loop(0, count // block, body, 0)


def layer_kernel(shape, trees, *refs):
    found, at = {}, 0
    for tree in trees:
        found.update(tree.unflatten(refs[at : at + tree.num_leaves]))
        at += tree.num_leaves
    r = types.SimpleNamespace(**found)
    rows, mem_count, dim, width, heads = shape
    keys = 2 * rows
    mem_keys = 2 * mem_count
    half = dim // SHARDS // 2
    z = lax.axis_index(SHARD)
    x = lax.axis_index(CTX)
    t = lax.axis_index(TENSOR)
    core = lax.rem(t, 2)
    to_x = {CTX: 1 - x}
    to_core = {TENSOR: t + 1 - 2 * core}
    to_y = {TENSOR: lax.rem(t + 2, 4)}

    near_z = z + 1 - 2 * lax.rem(z, 2)
    far_z = lax.rem(z + 2, SHARDS)
    last_z = lax.rem(near_z + 2, SHARDS)
    to_near = {SHARD: near_z}
    to_far = {SHARD: far_z}

    send_sem, recv_sem = r.send_sem, r.recv_sem
    used = [0]
    unsent = []

    def copy(src, dst, where):
        i = used[0]
        used[0] += 1
        return pltpu.make_async_remote_copy(
            src_ref=src, dst_ref=dst, send_sem=send_sem.at[i], recv_sem=recv_sem.at[i],
            device_id=where, device_id_type=MESH,
        )

    def start(src, dst, where):
        c = copy(src, dst, where)
        c.start()
        unsent.append(c)
        return c

    barrier = pltpu.get_barrier_semaphore()
    partners = [to_near, to_far, to_x, to_core, to_y]
    for p in partners:
        pl.semaphore_signal(barrier, inc=1, device_id=p, device_id_type=MESH)

    own_copies = {}
    for name in ORDER:
        full, part = r.full[name], r.part[name]
        own_copies[name] = []
        for side in range(2):
            c = pltpu.make_async_copy(
                part.at[pl.ds(side * half, half), :], full.at[z, side],
                r.own_sem.at[2 * name + side],
            )
            c.start()
            own_copies[name].append(c)
    small_own = pltpu.make_async_copy(r.in_small, r.small.at[z], r.own_sem.at[22])
    small_own.start()
    leaving = []

    def leave(src, dst):
        c = pltpu.make_async_copy(src, dst, r.own_sem.at[23 + len(leaving)])
        c.start()
        leaving.append(c)

    seg = r.in_seg[...].astype(f32)
    r.seg[...] = seg
    r.mseg[...] = r.in_mseg[...].astype(f32)
    own_seg = r.seg[:, pl.ds(pl.multiple_of(x * rows, BLOCK), rows)]
    r.seg_col[...] = jnp.broadcast_to(own_seg, (8, rows)).T
    pl.semaphore_wait(barrier, len(partners))

    gathers = {}

    def gather_start(*chosen):
        for name in chosen:
            full, part = r.full[name], r.part[name]
            far, near = [], []
            for side in (0, 1) if name in DIRECT else (x,):
                mine = part.at[pl.ds(side * half, half), :]
                far.append(start(mine, full.at[z, side], to_far))
                near.append(start(mine, full.at[z, side], to_near))
            gathers[name] = ((far, near, []), [])

    def gather_pass(name, source):
        if name not in DIRECT:
            ref = r.full[name].at[source, x]
            gathers[name][1].append(start(ref, ref, to_x))

    def gather_relay(*chosen):
        for name in chosen:
            far, near, relayed = gathers[name][0]
            for k, c in enumerate(far):
                c.wait_recv()
                ref = r.full[name].at[far_z, k if name in DIRECT else x]
                relayed.append(start(ref, ref, to_near))
            gather_pass(name, far_z)

    def gather_pump(*chosen):
        for name in chosen:
            far, near, relayed = gathers[name][0]
            for c in near:
                c.wait_recv()
            gather_pass(name, near_z)
            for c in relayed:
                c.wait_recv()
            gather_pass(name, last_z)

    def gather_wait(*chosen):
        for name in chosen:
            for c in own_copies[name]:
                c.wait()
            for c in gathers[name][1]:
                c.wait_recv()

    def weight(name):
        ref = r.full[name]
        return ref[...].reshape(dim, ref.shape[-1])

    small_sent = [start(r.in_small, r.small.at[z], p) for p in (to_far, to_near)]
    gather_start(SELF_K, SELF_V)
    small_own.wait()
    small_sent[0].wait_recv()
    small_sent.append(start(r.small.at[far_z], r.small.at[far_z], to_near))
    gather_relay(SELF_K, SELF_V)
    gather_start(SELF_Q, SELF_O)
    small_sent[1].wait_recv()
    small_sent[2].wait_recv()
    gathered = [r.small[n].astype(f32) for n in range(SHARDS)]
    for k in range(3):
        r.gains[k : k + 1, :] = jnp.concatenate(
            [g[k : k + 1, : dim // SHARDS] for g in gathered], axis=1
        )
    table = jnp.concatenate([g[8:16, : BUCKETS // SHARDS] for g in gathered], axis=1)
    r.near[...] = forward_mm(table.astype(bf16), r.in_lanes[...].astype(bf16))
    r.far[...] = jnp.broadcast_to(table[:, BUCKETS - 1 : BUCKETS], (8, BLOCK))
    build_strip(r.near, r.far, r.strip, keys // BLOCK, heads)

    def inverse(v):
        return lax.rsqrt(jnp.mean(v * v, axis=1, keepdims=True) + epsilon)

    def norm(v, k):
        return (v * inverse(v) * r.gains[k : k + 1, :]).astype(bf16)

    def input_norm(base):
        here = pl.ds(base, BIG)
        r.h1[here, :] = norm(r.in_dec[here, :].astype(f32), 0)

    loop_rows(rows, BIG, input_norm)

    def head_pairs(dst, here, left, right):
        for h in range(heads):
            lanes = slice(h * HEAD_DIM, (h + 1) * HEAD_DIM)
            dst[h, x, here, :] = jnp.concatenate([left[:, lanes], right[:, lanes]], axis=1).astype(
                bf16
            )

    gather_pump(SELF_K, SELF_V)
    gather_relay(SELF_Q)
    gather_wait(SELF_K, SELF_V)
    gather_pump(SELF_Q)
    gather_relay(SELF_O)
    gather_start(CROSS_K, CROSS_V, CROSS_Q, CROSS_O)

    def project(base):
        here = pl.ds(base, BIG)
        h = r.h1[here, :]
        head_pairs(
            r.kv1, here, forward_mm(h, weight(SELF_K)), forward_mm(h, weight(SELF_V))
        )

    loop_rows(rows, BIG, project)
    kv1_sent = [start(r.kv1.at[h, x], r.kv1.at[h, x], to_x) for h in range(heads)]
    gather_wait(SELF_Q)

    def project_query(base):
        here = pl.ds(base, BIG)
        r.q1[here, :] = forward_mm(r.h1[here, :], weight(SELF_Q)).astype(bf16)

    loop_rows(rows, BIG, project_query)
    gather_pump(SELF_O)

    def attend_block(causal, h, base, q, kv, cols, p_ref, a_ref, total):
        tiles = total // BLOCK
        here = pl.ds(base, BLOCK)
        lanes = slice(h * HEAD_DIM, (h + 1) * HEAD_DIM)
        pair = kv[h].reshape(total, 2 * HEAD_DIM)
        mask = r.seg_col[here, 0:1] == cols[...]
        scores = nt(q[here, lanes], pair[:, :HEAD_DIM])
        if causal:
            first = x * rows + base
            row = lax.broadcasted_iota(jnp.int32, (BLOCK, total), 0) + first
            col = lax.broadcasted_iota(jnp.int32, (BLOCK, total), 1)
            mask = mask & (row >= col)
            begin = pl.multiple_of((tiles - 1) * BLOCK - first, BLOCK)
            scores = scores + r.strip[h, :, pl.ds(begin, total)]
        scores = jnp.where(mask, scores, negative)
        peak = jnp.max(scores, axis=1, keepdims=True)
        weights = jnp.exp(scores - peak)
        probs = (weights / jnp.sum(weights, axis=1, keepdims=True)).astype(bf16)
        p_ref[h, here, :] = probs
        a_ref[here, lanes] = forward_mm(probs, pair[:, HEAD_DIM:]).astype(bf16)

    sums = {}

    def sides(key, j):
        n = r.p_res[key].shape[1]
        return [
            pl.multiple_of(((1 - core) * n + j) * CHUNK, CHUNK),
            pl.multiple_of((core * n + j) * CHUNK, CHUNK),
        ]

    def sum_send(key, j, piece):
        state = sums.setdefault((key, j), {})
        for c in state.values():
            c.wait_send()
            unsent[:] = [u for u in unsent if u is not c]
        other, own = sides(key, j)
        r.ps_out[key][j] = piece(other).astype(bf16)
        state[0] = start(r.ps_out[key].at[j], r.ps_in[key].at[j], to_core)
        mine = piece(own)
        state[0].wait_recv()
        r.py_out[key][j] = (mine + r.ps_in[key][j].astype(f32)).astype(bf16)
        state[1] = start(r.py_out[key].at[j], r.py_in[key].at[j], to_y)

    def sum_send_all(key, piece):
        chunks = range(r.p_res[key].shape[1])
        for j in chunks:
            state = sums.setdefault((key, j), {})
            for c in state.values():
                c.wait_send()
                unsent[:] = [u for u in unsent if u is not c]
            r.ps_out[key][j] = piece(sides(key, j)[0]).astype(bf16)
            state[0] = start(r.ps_out[key].at[j], r.ps_in[key].at[j], to_core)
        mine = [piece(sides(key, j)[1]) for j in chunks]
        for j in chunks:
            state = sums[(key, j)]
            state[0].wait_recv()
            r.py_out[key][j] = (mine[j] + r.ps_in[key][j].astype(f32)).astype(bf16)
            state[1] = start(r.py_out[key].at[j], r.py_in[key].at[j], to_y)

    def sum_recv(key, j, between=None):
        state = sums[(key, j)]
        res = r.p_res[key]
        state[1].wait_recv()
        res[core, j] = (r.py_out[key][j].astype(f32) + r.py_in[key][j].astype(f32)).astype(bf16)
        state[2] = start(res.at[core, j], res.at[core, j], to_core)
        if between is not None:
            between()
        state[2].wait_recv()

    def both_sides(key, j, step):
        other, own = sides(key, j)
        step(other, r.p_res[key][1 - core, j].astype(f32))
        step(own, r.p_res[key][core, j].astype(f32))

    wide = r.p_res[0].shape[1]
    slim = r.p_res[2].shape[1]
    for h in range(heads):
        kv1_sent[h].wait_recv()
        if h == 0:
            gather_relay(CROSS_K, CROSS_V, CROSS_Q, CROSS_O)
            gather_start(GATE)

        def self_rows(base):
            attend_block(True, h, base, r.q1, r.kv1, r.seg, r.p1, r.a1, keys)

        loop_rows(rows, BLOCK, self_rows)
        if h == 1:
            gather_pump(CROSS_K, CROSS_V)
            gather_start(UP)
    gather_relay(GATE)
    gather_start(DOWN)
    gather_wait(SELF_O)
    sum_send_all(0, lambda base: nt(r.a1[pl.ds(base, CHUNK), :], weight(SELF_O)))
    gather_pump(CROSS_Q, CROSS_O)
    gather_wait(CROSS_K, CROSS_V)
    memory = r.in_mem[...]
    head_pairs(
        r.kv2, slice(None), forward_mm(memory, weight(CROSS_K)),
        forward_mm(memory, weight(CROSS_V)),
    )
    kv2_sent = [start(r.kv2.at[h, x], r.kv2.at[h, x], to_x) for h in range(heads)]
    gather_wait(CROSS_Q)
    gather_relay(UP)
    gather_pump(GATE)

    for j in range(wide):
        sum_recv(0, j)

        def second(base, value):
            here = pl.ds(base, CHUNK)
            v = r.in_dec[here, :].astype(f32) + value
            r.x1[here, :] = v
            h = norm(v, 1)
            r.h2[here, :] = h
            r.q2[here, :] = forward_mm(h, weight(CROSS_Q)).astype(bf16)

        both_sides(0, j, second)
        if j == 0:
            for c in kv2_sent:
                c.wait_recv()

        if j == 0:
            gather_wait(CROSS_O)

        def mixed(base):
            for h in range(heads):
                attend_block(False, h, base, r.q2, r.kv2, r.mseg, r.p2, r.a2, mem_keys)
            return nt(r.a2[pl.ds(base, CHUNK), :], weight(CROSS_O))

        sum_send(1, j, mixed)
        if j == 0:
            gather_relay(DOWN)
            gather_pump(UP)
    gather_pump(DOWN)

    def flip(src, dst, count):
        for j in range(dim // BLOCK):
            dst[j * BLOCK : (j + 1) * BLOCK, :count] = src[:, j * BLOCK : (j + 1) * BLOCK].T

    flip(r.in_cot, r.flip, rows)
    gather_wait(DOWN)

    def grad_hidden_block(base):
        here = pl.ds(base, BIG)
        r.gm[here, :] = forward_mm(r.in_cot[here, :], weight(DOWN))

    loop_rows(rows, BIG, grad_hidden_block)
    gather_wait(GATE, UP)

    for j in range(wide):
        sum_recv(1, j)

        def third(base, value):
            here = pl.ds(base, CHUNK)
            v = r.x1[here, :] + value
            r.x2[here, :] = v
            r.h3[here, :] = norm(v, 2)

        both_sides(1, j, third)

        def hidden_piece(base):
            here = pl.ds(base, CHUNK)
            h = r.h3[here, :]
            gate = forward_mm(h, weight(GATE))
            upper = forward_mm(h, weight(UP))
            scale = np.float32(np.sqrt(2.0 / np.pi))
            square = gate * gate
            curve = jnp.tanh(scale * (gate + 0.044715 * (square * gate)))
            lower = 0.5 * (1.0 + curve)
            gelu = gate * lower
            slope = lower + 0.5 * gate * (1.0 - curve * curve) * scale * (
                1.0 + 3 * 0.044715 * square
            )
            grad = r.gm[here, :]
            r.m[here, :] = (gelu * upper).astype(bf16)
            grad_gate = (grad * upper * slope).astype(bf16)
            grad_up = (grad * gelu).astype(bf16)
            r.ggate[here, :] = grad_gate
            r.gup[here, :] = grad_up
            return nt(grad_gate, weight(GATE)) + nt(grad_up, weight(UP))

        sum_send(0, j, hidden_piece)

    shard_rows = dim // SHARDS

    def grad_into(g, at, flipped, right, count):
        stage = r.stage[g]
        cols = right.shape[1]

        def step(d, carry):
            here = pl.ds(pl.multiple_of(d * shard_rows, shard_rows), shard_rows)
            value = forward_mm(flipped[here, :count], right[...]).astype(bf16)
            stage[d, :, :, at : at + cols] = value.reshape(2, half, cols)
            return carry

        lax.fori_loop(0, SHARDS, step, 0)

    reduces = {}

    def reduce_x(g):
        stage = r.stage[g]
        reduces[g] = [start(stage.at[:, 1 - x], r.xr[g], to_x)]

    def reduce_a(g):
        stage, xr, zr = r.stage[g], r.xr[g], r.zr[g]
        reduces[g][0].wait_recv()

        def step(d, carry):
            stage[d, x] = (stage[d, x].astype(f32) + xr[d].astype(f32)).astype(bf16)
            return carry

        lax.fori_loop(0, SHARDS, step, 0)
        reduces[g].append(start(stage.at[last_z, x], zr.at[1], to_near))
        reduces[g].append(start(stage.at[near_z, x], zr.at[0], to_near))

    def reduce_b(g):
        stage, zr = r.stage[g], r.zr[g]
        reduces[g][1].wait_recv()
        stage[far_z, x] = (stage[far_z, x].astype(f32) + zr[1].astype(f32)).astype(bf16)
        reduces[g].append(start(stage.at[far_z, x], zr.at[2], to_far))

    def reduce_f(g):
        stage, zr, both = r.stage[g], r.zr[g], r.fb[g]
        reduces[g][2].wait_recv()
        reduces[g][3].wait_recv()
        total = stage[z, x].astype(f32) + zr[0].astype(f32) + zr[2].astype(f32)
        both[x] = total.astype(bf16)
        reduces[g].append(start(both.at[x], both.at[x], to_x))

    def reduce_o(g):
        reduces[g][4].wait_recv()
        leave(r.fb[g], r.o_fb[g])

    def whole_a(g):
        stage, zr = r.stage[g], r.zr[g]
        reduces[g] = [
            start(stage.at[last_z], zr.at[1], to_near), start(stage.at[near_z], zr.at[0], to_near)
        ]

    def whole_b(g):
        stage, zr = r.stage[g], r.zr[g]
        reduces[g][0].wait_recv()
        stage[far_z] = (stage[far_z].astype(f32) + zr[1].astype(f32)).astype(bf16)
        reduces[g].append(start(stage.at[far_z], zr.at[2], to_far))

    def whole_x(g):
        stage, zr = r.stage[g], r.zr[g]
        reduces[g][1].wait_recv()
        reduces[g][2].wait_recv()
        total = stage[z].astype(f32) + zr[0].astype(f32) + zr[2].astype(f32)
        r.fb[g][...] = total.astype(bf16)
        reduces[g].append(start(r.fb[g], r.xr[g], to_x))

    def whole_o(g):
        reduces[g][3].wait_recv()
        r.zr[g][0] = (r.fb[g][...].astype(f32) + r.xr[g][...].astype(f32)).astype(bf16)
        leave(r.zr[g].at[0], r.o_fb[g])

    grad_into(0, 0, r.flip, r.m, rows)
    whole_a(0)
    flip(r.h3, r.flip, rows)
    grad_into(2, 0, r.flip, r.gup, rows)
    reduce_x(2)
    grad_into(1, 0, r.flip, r.ggate, rows)
    whole_a(1)

    def norm_back(v, grad, k):
        inv = inverse(v)
        unit = v * inv
        scaled = grad * r.gains[k : k + 1, :]
        mean = jnp.mean(scaled * unit, axis=1, keepdims=True)
        return inv * (scaled - unit * mean), jnp.sum(grad * unit, axis=0, keepdims=True)

    def attend_back_block(causal, h, base, q, kv, p_ref, gq, ds, total):
        tiles = total // BLOCK
        here = pl.ds(base, BLOCK)
        lanes = slice(h * HEAD_DIM, (h + 1) * HEAD_DIM)
        pair = kv[h].reshape(total, 2 * HEAD_DIM)
        probs = p_ref[h, here, :].astype(f32)
        grad_probs = nt(r.ga[here, lanes], pair[:, HEAD_DIM:])
        mean = jnp.sum(probs * grad_probs, axis=1, keepdims=True)
        scores = probs * (grad_probs - mean)
        if causal:
            begin = pl.multiple_of((tiles - 1) * BLOCK - x * rows - base, BLOCK)
            window = pl.ds(begin, total)
            r.strip[h, :, window] = r.strip[h, :, window] + scores
        low = scores.astype(bf16)
        ds[here, :] = low
        gq[here, lanes] = forward_mm(low, pair[:, :HEAD_DIM]).astype(bf16)

    def pair_grads(h, q, p_ref, ds, gkv, total):
        lanes = slice(h * HEAD_DIM, (h + 1) * HEAD_DIM)
        r.gkv_t[:HEAD_DIM, :total] = tn(q[:, lanes], ds[...])
        r.gkv_t[HEAD_DIM:, :total] = tn(r.ga[:, lanes], p_ref[h])
        part = total // 2
        for side in range(2):
            gkv[h, side] = r.gkv_t[:, side * part : (side + 1) * part].T.astype(bf16)

    def pairs_sum(gkv, arrived, out):
        left, right = [], []
        for h in range(heads):
            value = gkv[h, x].astype(f32) + arrived[h].astype(f32)
            left.append(value[:, :HEAD_DIM])
            right.append(value[:, HEAD_DIM:])
        out[...] = jnp.concatenate(left + right, axis=1).astype(bf16)

    r.tiny[...] = jnp.zeros_like(r.tiny)
    for j in range(wide):
        sum_recv(0, j)

        def second_grad(base, value):
            here = pl.ds(base, CHUNK)
            back, gain = norm_back(r.x2[here, :], value, 2)
            grad = r.in_cot[here, :].astype(f32) + back
            r.tiny[2:3, :] = r.tiny[2:3, :] + gain
            r.gx[here, :] = grad
            low = grad.astype(bf16)
            r.gxb[here, :] = low
            r.ga[here, :] = forward_mm(low, weight(CROSS_O)).astype(bf16)

        both_sides(0, j, second_grad)

        def query_piece(base):
            for h in range(heads):
                attend_back_block(
                    False, h, base, r.q2, r.kv2, r.p2, r.gq2, r.ds2.at[h], mem_keys
                )
            return nt(r.gq2[pl.ds(base, CHUNK), :], weight(CROSS_Q))

        sum_send(1, j, query_piece)
    gkv2_sent = []
    for h in range(heads):
        pair_grads(h, r.q2, r.p2, r.ds2.at[h], r.gkv2, mem_keys)
        gkv2_sent.append(start(r.gkv2.at[h, 1 - x], r.gkv2_in.at[h], to_x))
    flip(r.gxb, r.flip, rows)
    grad_into(3, 0, r.flip, r.a2, rows)
    flip(r.h2, r.flip, rows)
    grad_into(3, width, r.flip, r.gq2, rows)
    reduce_x(3)
    reduce_a(2)

    for j in range(wide):
        sum_recv(1, j)

        def first_grad(base, value):
            here = pl.ds(base, CHUNK)
            back, gain = norm_back(r.x1[here, :], value, 1)
            grad = r.gx[here, :] + back
            r.tiny[1:2, :] = r.tiny[1:2, :] + gain
            r.gx[here, :] = grad
            low = grad.astype(bf16)
            r.gxb[here, :] = low
            r.ga1[here, :] = forward_mm(low, weight(SELF_O)).astype(bf16)

        both_sides(1, j, first_grad)
    whole_b(0)
    sum_send_all(3, lambda base: nt(r.m[pl.ds(base, CHUNK), :], weight(DOWN)))
    r.ga[...] = r.ga1[...]
    r.strip[...] = jnp.zeros_like(r.strip)
    gkv1_sent = []
    for h in range(heads):

        def self_back_rows(base):
            attend_back_block(True, h, base, r.q1, r.kv1, r.p1, r.gq1, r.ds, keys)

        loop_rows(rows, BLOCK, self_back_rows)
        pair_grads(h, r.q1, r.p1, r.ds, r.gkv1, keys)
        gkv1_sent.append(start(r.gkv1.at[h, 1 - x], r.gkv1_in.at[h], to_x))
        if h == 0:
            for c in gkv2_sent:
                c.wait_recv()
            pairs_sum(r.gkv2, r.gkv2_in, r.gkv2_sum)
            flip(r.in_mem, r.flip, mem_count)
            grad_into(4, 0, r.flip, r.gkv2_sum, mem_count)
            reduce_x(4)
            whole_b(1)
        if h == 1:
            reduce_b(2)
            reduce_a(3)
    whole_x(0)
    tiles = keys // BLOCK
    row = lax.broadcasted_iota(jnp.int32, (BLOCK, BLOCK), 0)
    col = lax.broadcasted_iota(jnp.int32, (BLOCK, BLOCK), 1)
    for h in range(heads):
        own = r.strip[h, :, (tiles - 1) * BLOCK : tiles * BLOCK]
        prior = r.strip[h, :, (tiles - 2) * BLOCK : (tiles - 1) * BLOCK]
        far = jnp.where(row < col, 0.0, prior)
        for j in range(tiles - 2):
            far = far + r.strip[h, :, j * BLOCK : (j + 1) * BLOCK]
        r.tiny[3 + h : 4 + h, :BLOCK] = fold_diagonals(own + jnp.where(row < col, prior, 0.0))
        r.tiny[3 + h : 4 + h, BLOCK : 2 * BLOCK] = jnp.sum(far, axis=0, keepdims=True)
    flip(r.gxb, r.flip, rows)
    grad_into(5, 0, r.flip, r.a1, rows)
    flip(r.h1, r.flip, rows)
    grad_into(5, width, r.flip, r.gq1, rows)
    whole_a(5)
    whole_x(1)
    for c in gkv1_sent:
        c.wait_recv()
    pairs_sum(r.gkv1, r.gkv1_in, r.gkv1_sum)

    def input_piece(base):
        here = pl.ds(base, CHUNK)
        return (
            nt(r.gq1[here, :], weight(SELF_Q))
            + nt(r.gkv1_sum[here, :width], weight(SELF_K))
            + nt(r.gkv1_sum[here, width:], weight(SELF_V))
        )

    sum_send_all(0, input_piece)
    grad_into(6, 0, r.flip, r.gkv1_sum, rows)
    reduce_x(6)
    reduce_b(3)

    def memory_piece(base):
        here = pl.ds(base, CHUNK)
        return nt(r.gkv2_sum[here, :width], weight(CROSS_K)) + nt(
            r.gkv2_sum[here, width:], weight(CROSS_V)
        )

    sum_send_all(2, memory_piece)
    reduce_a(4)
    for j in range(wide):
        sum_recv(3, j)

        def output_rows(base, value):
            here = pl.ds(base, CHUNK)
            r.dec[here, :] = (r.x2[here, :] + value).astype(bf16)

        both_sides(3, j, output_rows)
    leave(r.dec, r.o_dec)
    reduce_f(2)

    def tail():
        whole_b(5)

    for j in range(wide):
        sum_recv(0, j, tail if j == wide - 1 else None)

        def input_grad(base, value):
            here = pl.ds(base, CHUNK)
            back, gain = norm_back(r.in_dec[here, :].astype(f32), value, 0)
            r.tiny[0:1, :] = r.tiny[0:1, :] + gain
            r.gx[here, :] = r.gx[here, :] + back

        both_sides(0, j, input_grad)
    tiny = r.tiny_all
    sent = start(r.tiny, tiny.at[0], to_x)
    leave(r.gx, r.o_input)
    reduce_b(4)
    sent.wait_recv()
    tiny[1] = r.tiny[...] + tiny[0]
    sent = start(tiny.at[1], tiny.at[2], to_near)
    reduce_a(6)
    for j in range(slim):
        sum_recv(2, j)
    leave(r.p_res[2], r.o_mem)
    reduce_f(3)
    sent.wait_recv()
    tiny[3] = tiny[1] + tiny[2]
    sent = start(tiny.at[3], tiny.at[4], to_far)
    whole_x(5)
    reduce_f(4)
    reduce_b(6)
    for g in (0, 1):
        whole_o(g)
    reduce_o(2)
    reduce_f(6)
    sent.wait_recv()
    r.tiny_sum[...] = tiny[3] + tiny[4]
    leave(r.tiny_sum, r.o_tiny)
    reduce_o(3)
    whole_o(5)
    reduce_o(4)
    reduce_o(6)
    for c in unsent:
        c.wait_send()
    for c in leaving:
        c.wait()


def output_kernel(trees, *refs):
    found, at = {}, 0
    for tree in trees:
        found.update(tree.unflatten(refs[at : at + tree.num_leaves]))
        at += tree.num_leaves
    r = types.SimpleNamespace(**found)
    z = lax.axis_index(SHARD)
    r.out_dec[...] = r.o_dec[...]
    r.out_input[...] = r.o_input[...]
    r.out_mem[...] = r.o_mem[...].reshape(r.out_mem.shape).astype(f32)
    for g, group in enumerate(GROUPS):
        at = 0
        for name in group:
            out = r.out_grad[name]
            cols = out.shape[1]
            out[...] = r.o_fb[g][:, :, at : at + cols].reshape(out.shape).astype(f32)
            at += cols
    total = r.o_tiny[...]
    part = r.out_gain[0].shape[1]
    for k in range(3):
        piece = jnp.zeros((1, part), f32)
        for n in range(SHARDS):
            piece = jnp.where(z == n, total[k : k + 1, n * part : (n + 1) * part], piece)
        r.out_gain[k][...] = piece
    lanes = r.in_lanes[...]
    bucket = lax.broadcasted_iota(jnp.int32, (BUCKETS, BLOCK), 0)
    column = lax.broadcasted_iota(jnp.int32, (BUCKETS, BLOCK), 1)
    heads, share = r.out_table.shape
    table = jnp.zeros((BUCKETS, BLOCK), f32)
    for h in range(heads):
        near = jnp.sum(lanes * total[3 + h : 4 + h, :BLOCK], axis=1, keepdims=True)
        far = jnp.sum(total[3 + h : 4 + h, BLOCK : 2 * BLOCK], axis=1, keepdims=True)
        table = jnp.where(
            column == h, near + jnp.where(bucket == BUCKETS - 1, far, 0.0), table
        )
    table = table.T
    piece = jnp.zeros((heads, share), f32)
    for n in range(SHARDS):
        piece = jnp.where(z == n, table[:heads, n * share : (n + 1) * share], piece)
    r.out_table[...] = piece


def local_fast(
    dec_in, memory, dec_segments, mem_segments, gain_self, gain_cross, gain_ffn,
    self_q, self_k, self_v, self_o, cross_q, cross_k, cross_v, cross_o,
    ffn_gate, ffn_up, ffn_down, bias_table, cotangent,
):
    rows, dim = dec_in.shape[1:]
    mem = memory.shape[1]
    width, hidden = self_q.shape[1], ffn_gate.shape[1]
    heads = width // HEAD_DIM
    part = gain_self.shape[0]
    share = bias_table.shape[0]
    keys, mem_keys = 2 * rows, 2 * mem
    half = dim // SHARDS // 2
    line = lax.broadcasted_iota(jnp.int32, (16, part), 0)
    small = jnp.pad(bias_table.T, ((8, 8 - heads), (0, part - share)))
    for k, gain in enumerate((gain_self, gain_cross, gain_ffn)):
        small = jnp.where(line == k, gain[None, :], small)
    weights = [
        self_q, self_k, self_v, self_o, cross_q, cross_k, cross_v, cross_o,
        ffn_gate, ffn_up, ffn_down,
    ]
    widths = [w.shape[1] for w in weights]
    joined = [sum(widths[k] for k in group) for group in GROUPS]
    chunks = [n // 2 // CHUNK for n in (rows, rows, mem, rows)]
    near = dict(
        in_dec=dec_in[0], in_mem=memory[0], in_seg=dec_segments, in_mseg=mem_segments,
        in_lanes=jnp.asarray(lane_buckets()), in_cot=cotangent[0],
    )
    far = dict(in_small=small, part=weights)

    def out(shape, kind):
        return jax.ShapeDtypeStruct(shape, kind)

    outs = dict(
        out_dec=out((rows, dim), bf16), out_input=out((rows, dim), f32),
        out_mem=out((mem, dim), f32), out_gain=[out((1, part), f32)] * 3,
        out_grad=[out((part, c), f32) for c in widths], out_table=out((heads, share), f32),
    )
    passed = dict(
        o_dec=out((rows, dim), bf16), o_input=out((rows, dim), f32),
        o_mem=out((2, chunks[2], CHUNK, dim), bf16), o_tiny=out((8, dim), f32),
        o_fb=[out((2, half, c), bf16) for c in joined],
    )
    vmem = pltpu.VMEM
    held = dict(
        full=[vmem((SHARDS, 2, half, c), bf16) for c in widths],
        small=vmem((SHARDS, 16, part), bf16), seg=vmem((1, keys), f32),
        mseg=vmem((1, mem_keys), f32), seg_col=vmem((rows, 8), f32), gains=vmem((8, dim), f32),
        near=vmem((8, BLOCK), f32), far=vmem((8, BLOCK), f32),
        strip=vmem((heads, BLOCK, (2 * (keys // BLOCK) - 1) * BLOCK), f32),
        h1=vmem((rows, dim), bf16), h2=vmem((rows, dim), bf16), h3=vmem((rows, dim), bf16),
        x1=vmem((rows, dim), f32), x2=vmem((rows, dim), f32),
        q1=vmem((rows, width), bf16), q2=vmem((rows, width), bf16),
        kv1=vmem((heads, 2, rows, 2 * HEAD_DIM), bf16), kv2=vmem((heads, 2, mem, 2 * HEAD_DIM), bf16),
        p1=vmem((heads, rows, keys), bf16), p2=vmem((heads, rows, mem_keys), bf16),
        a1=vmem((rows, width), bf16), a2=vmem((rows, width), bf16),
        gm=vmem((rows, hidden), f32), m=vmem((rows, hidden), bf16),
        ggate=vmem((rows, hidden), bf16), gup=vmem((rows, hidden), bf16),
        flip=vmem((dim, rows), bf16), gx=vmem((rows, dim), f32), gxb=vmem((rows, dim), bf16),
        ga=vmem((rows, width), bf16), ds=vmem((rows, keys), bf16),
        gkv_t=vmem((2 * HEAD_DIM, keys), f32), ds2=vmem((heads, rows, mem_keys), bf16),
        ga1=vmem((rows, width), bf16), dec=vmem((rows, dim), bf16), gq1=vmem((rows, width), bf16),
        gq2=vmem((rows, width), bf16), gkv1=vmem((heads, 2, rows, 2 * HEAD_DIM), bf16),
        gkv2=vmem((heads, 2, mem, 2 * HEAD_DIM), bf16), gkv1_in=vmem((heads, rows, 2 * HEAD_DIM), bf16),
        gkv2_in=vmem((heads, mem, 2 * HEAD_DIM), bf16), gkv1_sum=vmem((rows, 2 * width), bf16),
        gkv2_sum=vmem((mem, 2 * width), bf16), tiny=vmem((8, dim), f32),
        tiny_all=vmem((5, 8, dim), f32), tiny_sum=vmem((8, dim), f32),
        ps_out=[vmem((n, CHUNK, dim), bf16) for n in chunks],
        ps_in=[vmem((n, CHUNK, dim), bf16) for n in chunks],
        py_out=[vmem((n, CHUNK, dim), bf16) for n in chunks],
        py_in=[vmem((n, CHUNK, dim), bf16) for n in chunks],
        p_res=[vmem((2, n, CHUNK, dim), bf16) for n in chunks],
        stage=[vmem((SHARDS, 2, half, c), bf16) for c in joined],
        xr=[
            vmem((2 if g in WHOLE else SHARDS, half, c), bf16) for g, c in enumerate(joined)
        ],
        zr=[
            vmem((3, 2, half, c) if g in WHOLE else (3, half, c), bf16)
            for g, c in enumerate(joined)
        ],
        fb=[vmem((2, half, c), bf16) for c in joined],
        send_sem=pltpu.SemaphoreType.DMA((192,)), recv_sem=pltpu.SemaphoreType.DMA((192,)),
        own_sem=pltpu.SemaphoreType.DMA((40,)),
    )
    in_vmem = pl.BlockSpec(memory_space=pltpu.VMEM)
    anywhere = pl.BlockSpec(memory_space=pl.ANY)
    flat = [jax.tree.flatten(v) for v in (near, far, passed, held)]
    results = pl.pallas_call(
        functools.partial(
            layer_kernel, (rows, mem, dim, width, heads), [tree for _, tree in flat]
        ),
        out_shape=tuple(flat[2][0]),
        in_specs=[in_vmem] * len(flat[0][0]) + [anywhere] * len(flat[1][0]),
        out_specs=tuple([anywhere] * len(flat[2][0])),
        scratch_shapes=flat[3][0],
        compiler_params=pltpu.CompilerParams(
            collective_id=0, has_side_effects=True, vmem_limit_bytes=67043328
        ),
        name="layer",
    )(*flat[0][0], *flat[1][0])
    ready = dict(flat[2][1].unflatten(results), in_lanes=near["in_lanes"])
    flat = [jax.tree.flatten(v) for v in (ready, outs)]
    results = pl.pallas_call(
        functools.partial(output_kernel, [tree for _, tree in flat]),
        out_shape=tuple(flat[1][0]),
        in_specs=[in_vmem] * len(flat[0][0]),
        out_specs=tuple([in_vmem] * len(flat[1][0])),
        compiler_params=pltpu.CompilerParams(vmem_limit_bytes=67043328),
        name="outputs",
    )(*flat[0][0])
    flat = flat[:1] + [None] + flat[1:2]
    got = types.SimpleNamespace(**flat[2][1].unflatten(results))
    return (
        got.out_dec[None], got.out_input[None], got.out_mem[None],
        *[g[0] for g in got.out_gain], *got.out_grad, got.out_table.T,
    )


def shard_part(parts):
    return tuple(
        lax.psum_scatter(p.astype(jnp.bfloat16), SHARD, scatter_dimension=0, tiled=True).astype(
            jnp.float32
        )
        for p in parts
    )


def context_total(parts):
    return tuple(lax.psum(p.astype(jnp.bfloat16), CTX).astype(jnp.float32) for p in parts)


def local(
    dec_in,
    memory,
    dec_segments,
    mem_segments,
    gain_self,
    gain_cross,
    gain_ffn,
    self_q,
    self_k,
    self_v,
    self_o,
    cross_q,
    cross_k,
    cross_v,
    cross_o,
    ffn_gate,
    ffn_up,
    ffn_down,
    bias_table,
    cotangent,
):
    gathered = (
        lax.all_gather(gain_self, SHARD, axis=0, tiled=True),
        lax.all_gather(gain_cross, SHARD, axis=0, tiled=True),
        lax.all_gather(gain_ffn, SHARD, axis=0, tiled=True),
        lax.all_gather(self_q, SHARD, axis=0, tiled=True),
        lax.all_gather(self_k, SHARD, axis=0, tiled=True),
        lax.all_gather(self_v, SHARD, axis=0, tiled=True),
        lax.all_gather(self_o, SHARD, axis=0, tiled=True),
        lax.all_gather(cross_q, SHARD, axis=0, tiled=True),
        lax.all_gather(cross_k, SHARD, axis=0, tiled=True),
        lax.all_gather(cross_v, SHARD, axis=0, tiled=True),
        lax.all_gather(cross_o, SHARD, axis=0, tiled=True),
        lax.all_gather(ffn_gate, SHARD, axis=0, tiled=True),
        lax.all_gather(ffn_up, SHARD, axis=0, tiled=True),
        lax.all_gather(ffn_down, SHARD, axis=0, tiled=True),
        lax.all_gather(bias_table, SHARD, axis=0, tiled=True),
    )
    (
        norm_one,
        norm_two,
        norm_three,
        query_self,
        key_self,
        value_self,
        out_self,
        query_cross,
        key_cross,
        value_cross,
        out_cross,
        gate_full,
        up_full,
        down_full,
        table_full,
    ) = gathered
    gain_one = norm_one.astype(jnp.float32)
    gain_two = norm_two.astype(jnp.float32)
    gain_three = norm_three.astype(jnp.float32)
    table = table_full.astype(jnp.float32)
    width = query_self.shape[1]
    hidden_in = dec_in[0].astype(jnp.float32)
    mem_rows = memory[0]
    grad_out = cotangent[0].astype(jnp.float32)
    count_rows = hidden_in.shape[0]
    place = lax.axis_index(CTX)
    dec_ids = dec_segments[0]
    mem_ids = mem_segments[0]
    query_ids = lax.dynamic_slice_in_dim(dec_ids, place * count_rows, count_rows)
    query_pos = place * count_rows + jnp.arange(count_rows, dtype=jnp.int32)
    key_pos = jnp.arange(dec_ids.shape[0], dtype=jnp.int32)
    mem_pos = jnp.arange(mem_ids.shape[0], dtype=jnp.int32)
    normed_one = rms_norm(hidden_in, gain_one).astype(jnp.bfloat16)
    query_one = forward_mm(normed_one, query_self).astype(jnp.bfloat16)
    pairs_own = jnp.concatenate(
        [forward_mm(normed_one, key_self), forward_mm(normed_one, value_self)], axis=1
    ).astype(jnp.bfloat16)
    pairs_one = lax.all_gather(pairs_own, CTX, axis=0, tiled=True)
    mixed_one, lse_one = attend(
        query_one, pairs_one, key_pos, dec_ids, query_pos, query_ids, table, True
    )
    context_one = mixed_one.astype(jnp.bfloat16)
    first = hidden_in + lax.psum(
        backward_mm(context_one, out_self).astype(jnp.bfloat16), TENSOR
    ).astype(jnp.float32)
    normed_two = rms_norm(first, gain_two).astype(jnp.bfloat16)
    query_two = forward_mm(normed_two, query_cross).astype(jnp.bfloat16)
    pairs_mem = jnp.concatenate(
        [forward_mm(mem_rows, key_cross), forward_mm(mem_rows, value_cross)], axis=1
    ).astype(jnp.bfloat16)
    pairs_two = lax.all_gather(pairs_mem, CTX, axis=0, tiled=True)
    mixed_two, lse_two = attend(
        query_two, pairs_two, mem_pos, mem_ids, query_pos, query_ids, table, False
    )
    context_two = mixed_two.astype(jnp.bfloat16)
    second = first + lax.psum(
        backward_mm(context_two, out_cross).astype(jnp.bfloat16), TENSOR
    ).astype(jnp.float32)
    normed_three = rms_norm(second, gain_three).astype(jnp.bfloat16)
    gate = forward_mm(normed_three, gate_full)
    upper = forward_mm(normed_three, up_full)
    activated = gated(gate, upper).astype(jnp.bfloat16)
    result = second + lax.psum(
        backward_mm(activated, down_full).astype(jnp.bfloat16), TENSOR
    ).astype(jnp.float32)
    dec_out = result.astype(jnp.bfloat16)
    grad_low = cotangent[0]
    grad_down_w = weight_mm(grad_low, activated)
    grad_hidden = forward_mm(grad_low, down_full)
    _, pull_gate = jax.vjp(gated, gate, upper)
    grad_gate, grad_upper = pull_gate(grad_hidden)
    gate_low = grad_gate.astype(jnp.bfloat16)
    upper_low = grad_upper.astype(jnp.bfloat16)
    grad_gate_w = weight_mm(normed_three, gate_low)
    grad_up_w = weight_mm(normed_three, upper_low)
    grad_normed_three = backward_mm(gate_low, gate_full) + backward_mm(upper_low, up_full)
    grad_normed_three = lax.psum(grad_normed_three.astype(jnp.bfloat16), TENSOR).astype(
        jnp.float32
    )
    _, pull_three = jax.vjp(rms_norm, second, gain_three)
    grad_second, grad_gain_three = pull_three(grad_normed_three)
    grad_second = grad_out + grad_second
    second_low = grad_second.astype(jnp.bfloat16)
    grad_out_cross = weight_mm(second_low, context_two)
    grad_context_two = forward_mm(second_low, out_cross).astype(jnp.bfloat16)
    grad_query_two, grad_pairs_two, _ = attend_back(
        query_two,
        pairs_two,
        mem_pos,
        mem_ids,
        query_pos,
        query_ids,
        table,
        False,
        mixed_two,
        lse_two,
        grad_context_two,
    )
    pairs_grad_mem = lax.psum_scatter(
        grad_pairs_two.astype(jnp.bfloat16), CTX, scatter_dimension=0, tiled=True
    )
    query_two_low = grad_query_two.astype(jnp.bfloat16)
    grad_mem_keys = pairs_grad_mem[:, :width]
    grad_mem_values = pairs_grad_mem[:, width:]
    grad_query_cross = weight_mm(normed_two, query_two_low)
    grad_key_cross = weight_mm(mem_rows, grad_mem_keys)
    grad_value_cross = weight_mm(mem_rows, grad_mem_values)
    grad_normed_two = backward_mm(query_two_low, query_cross)
    grad_memory = backward_mm(grad_mem_keys, key_cross) + backward_mm(grad_mem_values, value_cross)
    grad_normed_two, grad_memory = (
        lax.psum(grad_normed_two.astype(jnp.bfloat16), TENSOR).astype(jnp.float32),
        lax.psum(grad_memory.astype(jnp.bfloat16), TENSOR).astype(jnp.float32),
    )
    _, pull_two = jax.vjp(rms_norm, first, gain_two)
    grad_first, grad_gain_two = pull_two(grad_normed_two)
    grad_first = grad_second + grad_first
    first_low = grad_first.astype(jnp.bfloat16)
    grad_out_self = weight_mm(first_low, context_one)
    grad_context_one = forward_mm(first_low, out_self).astype(jnp.bfloat16)
    grad_query_one, grad_pairs_one, grad_table = attend_back(
        query_one,
        pairs_one,
        key_pos,
        dec_ids,
        query_pos,
        query_ids,
        table,
        True,
        mixed_one,
        lse_one,
        grad_context_one,
    )
    pairs_grad_own = lax.psum_scatter(
        grad_pairs_one.astype(jnp.bfloat16), CTX, scatter_dimension=0, tiled=True
    )
    query_one_low = grad_query_one.astype(jnp.bfloat16)
    grad_keys_own = pairs_grad_own[:, :width]
    grad_values_own = pairs_grad_own[:, width:]
    grad_query_self = weight_mm(normed_one, query_one_low)
    grad_key_self = weight_mm(normed_one, grad_keys_own)
    grad_value_self = weight_mm(normed_one, grad_values_own)
    grad_normed_one = (
        backward_mm(query_one_low, query_self)
        + backward_mm(grad_keys_own, key_self)
        + backward_mm(grad_values_own, value_self)
    )
    grad_normed_one = lax.psum(grad_normed_one.astype(jnp.bfloat16), TENSOR).astype(jnp.float32)
    _, pull_one = jax.vjp(rms_norm, hidden_in, gain_one)
    grad_input, grad_gain_one = pull_one(grad_normed_one)
    grad_input = grad_first + grad_input
    local_grads = (
        grad_gain_one,
        grad_gain_two,
        grad_gain_three,
        grad_query_self,
        grad_key_self,
        grad_value_self,
        grad_out_self,
        grad_query_cross,
        grad_key_cross,
        grad_value_cross,
        grad_out_cross,
        grad_gate_w,
        grad_up_w,
        grad_down_w,
        grad_table,
    )
    summed = shard_part(context_total(local_grads))
    return (
        dec_out[None],
        grad_input[None],
        grad_memory[None],
        summed[0],
        summed[1],
        summed[2],
        summed[3],
        summed[4],
        summed[5],
        summed[6],
        summed[7],
        summed[8],
        summed[9],
        summed[10],
        summed[11],
        summed[12],
        summed[13],
        summed[14],
    )


def solution(mesh):
    in_specs = (
        P(SHARD, CTX, None),
        P(SHARD, CTX, None),
        P(SHARD, None),
        P(SHARD, None),
        P(SHARD),
        P(SHARD),
        P(SHARD),
        P(SHARD, TENSOR),
        P(SHARD, TENSOR),
        P(SHARD, TENSOR),
        P(SHARD, TENSOR),
        P(SHARD, TENSOR),
        P(SHARD, TENSOR),
        P(SHARD, TENSOR),
        P(SHARD, TENSOR),
        P(SHARD, TENSOR),
        P(SHARD, TENSOR),
        P(SHARD, TENSOR),
        P(SHARD, TENSOR),
        P(SHARD, CTX, None),
    )
    out_specs = (
        P(SHARD, CTX, None),
        P(SHARD, CTX, None),
        P(SHARD, CTX, None),
        P(SHARD),
        P(SHARD),
        P(SHARD),
        P(SHARD, TENSOR),
        P(SHARD, TENSOR),
        P(SHARD, TENSOR),
        P(SHARD, TENSOR),
        P(SHARD, TENSOR),
        P(SHARD, TENSOR),
        P(SHARD, TENSOR),
        P(SHARD, TENSOR),
        P(SHARD, TENSOR),
        P(SHARD, TENSOR),
        P(SHARD, TENSOR),
        P(SHARD, TENSOR),
    )
    fast = (mesh.shape[SHARD], mesh.shape[CTX], mesh.shape[TENSOR]) == (SHARDS, 2, 4)
    body = local_fast if fast else local
    return jax.shard_map(body, mesh=mesh, in_specs=in_specs, out_specs=out_specs, check_vma=False)
```
